128 devices in a mesh: gx: 8 (over y, core), gy: 16 (over z, x).
Axes of the slice: x: 4, y: 4, z: 4, core: 2. Of those that a mesh axis runs over, the one named last changes fastest.
Arguments:
- wavefield: float32 [16, 32, 3, 125, 256], P('gx', 'gy'), may hold values from -0.6 to 0.6
- moduli: float32 [16, 32, 2, 256], P('gx', 'gy'), may hold values from 0.5 to 4
- residuals: float32 [128, 128, 128], P(('gx', 'gy')), may hold values from -6 to 6
- coords: float32 [128, 128, 3, 128], P(('gx', 'gy')), may hold values from -1 to 1
- angles: float32 [128, 128, 2, 128], P(('gx', 'gy')), may hold values from -3.140625 to 3.140625
- element_ids: int32 [128, 128, 128], P(('gx', 'gy')), may hold values from 0 to 1023
- counts: int32 [128, 128], P(('gx', 'gy')), may hold values from 0 to 128, as said below
Outputs:
- force: float32 [16, 32, 3, 125, 256], P('gx', 'gy')
The draws below stay inside these ranges and needn't reach their ends.
Inputs may be any that keep to these rules, and one draw needn't show every extreme that they name: `counts`: each sending device has at least one tile with exactly 128 live slots; in every draw one owner receives 128 live slots from every sender. The lightest owners receive on average about a sixth of 128 a sender, the others lie between.
All inputs are finite; a program needn't handle non-finite values.
Results may differ from the reference program's by a relative error of at most 0.0003.
Values sent between devices are 32-bit elements; how exact they have to be, the bound alone decides.
A program may use at most 64 MiB of HBM per device.

```python
import math
import jax
import jax.numpy as jnp
import numpy as np
from jax import lax

CX = 2
CY = 2
EZ = 256
CAP = 128
OWNERS = 128
NXE = 16
NYE = 32
N_GX = 8
N_GY = 16


def draw_counts(key, part):
    base_key = jax.random.fold_in(key, 11)
    key_heavy, key_base, key_full = jax.random.split(base_key, 3)
    heavy = jax.random.randint(key_heavy, (OWNERS,), 1, 5)
    base = jax.random.randint(key_base, (OWNERS, OWNERS), 0, CAP // 3 + 1)
    filled = jnp.minimum(base * heavy[None, :], CAP)
    full_owner = jax.random.randint(key_full, (), 0, OWNERS)
    column = jnp.arange(OWNERS, dtype=jnp.int32)[None, :]
    return jnp.where(column == full_owner, CAP, filled).astype(jnp.int32)


def set_ends(values, stream_key, least, high):
    spot = [jax.random.randint(jax.random.fold_in(stream_key, axis), (), 0, length) for axis, length in enumerate(values.shape)]
    longest = values.shape.index(max(values.shape))
    neighbour = spot[:longest] + [(spot[longest] + 1) % values.shape[longest]] + spot[longest + 1:]
    return values.at[tuple(spot)].set(least).at[tuple(neighbour)].set(high)


def steps_of(own_key, shape, cuts, least, largest):
    factor_of, own = 1.0, jax.random.fold_in(own_key, 6)
    for axis_at, blocks in cuts:
        heights = jnp.exp(jax.random.uniform(jax.random.fold_in(own, axis_at), (blocks,), jnp.float32, least / len(cuts), largest / len(cuts)))
        factor_of = factor_of * jnp.repeat(heights, shape[axis_at] // blocks).reshape([-1 if axis == axis_at else 1 for axis in range(len(shape))])
    return factor_of


def normal_values(own_key, dims, deviation, most, pieces=(), kind=jnp.bfloat16):
    level = steps_of(own_key, dims, pieces, -0.22, 0.18) if pieces else 1.0
    drawn = jax.random.normal(own_key, dims, jnp.float32) * deviation * level
    return jnp.minimum(jnp.maximum(drawn, -most), most).astype(kind)


def setup_inputs(seed: int = 0) -> dict:
    key_of = jax.random.split(jax.random.key(seed), 8)
    wavefield = normal_values(key_of[0], (NXE, NYE, 3, 125, EZ), 0.1, 0.6, ((0, 8), (1, 16)), jnp.float32)
    moduli = jnp.clip(jnp.exp(math.log(4.0) - 2.0794415 * jax.random.uniform(key_of[1], (NXE, NYE, 2, EZ), jnp.float32) ** steps_of(key_of[1], (NXE, NYE, 2, EZ), ((0, 8), (1, 16)), -0.2, 0.2)), 0.5, 4.0)
    residuals = normal_values(key_of[2], (OWNERS, OWNERS, CAP), 1.0, 6.0, ((0, 128),), jnp.float32)
    coords = jnp.clip(jax.random.uniform(key_of[3], (OWNERS, OWNERS, 3, CAP), jnp.float32, -1.0, 1.0) * steps_of(key_of[3], (OWNERS, OWNERS, 3, CAP), ((0, 128),), -0.4, 0.0), -1.0, 1.0)
    angles = jnp.clip(jax.random.uniform(key_of[4], (OWNERS, OWNERS, 2, CAP), jnp.float32, -3.140625, 3.140625), -3.140625, 3.140625)
    element_ids = set_ends(jax.random.randint(key_of[5], (OWNERS, OWNERS, CAP), 0, CX * CY * EZ), jax.random.fold_in(key_of[5], 1), 0, (CX * CY * EZ) - 1).astype(jnp.int32)
    counts = draw_counts(jax.random.fold_in(key_of[7], 71), 0)
    return dict(wavefield=wavefield, moduli=moduli, residuals=residuals, coords=coords, angles=angles, element_ids=element_ids, counts=counts)


def gll_points():
    return np.array([-1.0, -math.sqrt(3.0 / 7.0), 0.0, math.sqrt(3.0 / 7.0), 1.0])

def gll_weights():
    return np.array([0.1, 49.0 / 90.0, 32.0 / 45.0, 49.0 / 90.0, 0.1])

def derivative_table():
    points = gll_points()
    table = np.zeros((5, 5))
    for row in range(5):
        for col in range(5):
            if row == col:
                table[row, col] = sum((1.0 / (points[col] - points[other]) for other in range(5) if other != col))
            else:
                value = 1.0 / (points[col] - points[row])
                for other in range(5):
                    if other != col and other != row:
                        value = value * (points[row] - points[other]) / (points[col] - points[other])
                table[row, col] = value
    return table

def basis(where):
    points = gll_points()
    values = []
    slopes = []
    for node in range(5):
        value = jnp.ones_like(where)
        slope = jnp.zeros_like(where)
        for other in range(5):
            if other != node:
                scale = 1.0 / (points[node] - points[other])
                factor = (where - points[other]) * scale
                slope = slope * factor + value * scale
                value = value * factor
        values.append(value)
        slopes.append(slope)
    return (jnp.stack(values), jnp.stack(slopes))

def inject(total, resid, coord, angle, ids, live_count):
    slots = resid.shape[-1]
    live = jnp.arange(slots, dtype=jnp.int32)[None, :] < live_count[:, None]
    value = jnp.where(live, resid, 0.0).reshape(-1)
    first = coord[:, 0, :].reshape(-1)
    second = coord[:, 1, :].reshape(-1)
    third = coord[:, 2, :].reshape(-1)
    azimuth = angle[:, 0, :].reshape(-1)
    dip = angle[:, 1, :].reshape(-1)
    tang_x = jnp.cos(azimuth) * jnp.cos(dip)
    tang_y = jnp.sin(azimuth) * jnp.cos(dip)
    tang_z = jnp.sin(dip)
    val_x, der_x = basis(first)
    val_y, der_y = basis(second)
    val_z, der_z = basis(third)
    shape = tang_x * der_x[:, None, None, :] * val_y[None, :, None, :] * val_z[None, None, :, :] + tang_y * val_x[:, None, None, :] * der_y[None, :, None, :] * val_z[None, None, :, :] + tang_z * val_x[:, None, None, :] * val_y[None, :, None, :] * der_z[None, None, :, :]
    direction = jnp.stack([tang_x, tang_y, tang_z]) * value[None, :]
    contrib = (direction[:, None, None, None, :] * shape[None]).reshape(375, -1)
    return total.at[:, ids.reshape(-1)].add(contrib)

def along(field, table, dim):
    if dim == 0:
        return jnp.einsum('pa,...aqsz->...pqsz', table, field, precision=lax.Precision.HIGHEST)
    if dim == 1:
        return jnp.einsum('qb,...pbsz->...pqsz', table, field, precision=lax.Precision.HIGHEST)
    return jnp.einsum('sc,...pqcz->...pqsz', table, field, precision=lax.Precision.HIGHEST)

def back(field, table, dim):
    if dim == 0:
        return jnp.einsum('pa,...pqsz->...aqsz', table, field, precision=lax.Precision.HIGHEST)
    if dim == 1:
        return jnp.einsum('qb,...pqsz->...pbsz', table, field, precision=lax.Precision.HIGHEST)
    return jnp.einsum('sc,...pqsz->...pqcz', table, field, precision=lax.Precision.HIGHEST)

def stiffness(field, moduli):
    table = jnp.asarray(derivative_table(), jnp.float32)
    weight = jnp.asarray(gll_weights(), jnp.float32)
    wgrid = (weight[:, None, None] * weight[None, :, None] * weight[None, None, :])[:, :, :, None]
    grads = [along(field, table, dim) for dim in range(3)]
    lame = moduli[..., 0, :][..., None, None, None, :]
    shear = moduli[..., 1, :][..., None, None, None, :]
    diverge = grads[0][..., 0, :, :, :, :] + grads[1][..., 1, :, :, :, :] + grads[2][..., 2, :, :, :, :]
    result = jnp.zeros_like(field)
    for col in range(3):
        parts = []
        for row in range(3):
            stress = shear * (grads[col][..., row, :, :, :, :] + grads[row][..., col, :, :, :, :])
            if row == col:
                stress = stress + lame * diverge
            parts.append(stress * wgrid)
        result = result + back(jnp.stack(parts, axis=-5), table, col)
    return result

def assemble_dim(field, e_dim, n_dim, fetch):
    count = field.shape[e_dim]
    low = lax.slice_in_dim(field, 0, 1, axis=n_dim)
    high = lax.slice_in_dim(field, 4, 5, axis=n_dim)
    middle = lax.slice_in_dim(field, 1, 4, axis=n_dim)
    first = lax.slice_in_dim(low, 0, 1, axis=e_dim)
    last = lax.slice_in_dim(high, count - 1, count, axis=e_dim)
    below, above = fetch(first, last)
    low_next = jnp.concatenate([lax.slice_in_dim(low, 1, count, axis=e_dim), above], axis=e_dim)
    high_prev = jnp.concatenate([below, lax.slice_in_dim(high, 0, count - 1, axis=e_dim)], axis=e_dim)
    return jnp.concatenate([low + high_prev, middle, high + low_next], axis=n_dim)

def fetch_none(first, last):
    return (jnp.zeros_like(last), jnp.zeros_like(first))

def reference(wavefield, moduli, residuals, coords, angles, element_ids, counts):
    owners = N_GX * N_GY
    nxe = CX * N_GX
    nye = CY * N_GY
    index = jnp.arange(owners, dtype=jnp.int32)
    owner_x = (index // N_GY)[:, None]
    owner_y = (index % N_GY)[:, None]

    def per_source(total, items):
        resid, coord, angle, ids, live_count = items
        cell_x = ids // (CY * EZ)
        cell_y = ids // EZ % CY
        cell_z = ids % EZ
        global_ids = (((owner_x * CX + cell_x) * nye + owner_y * CY + cell_y) * EZ + cell_z).astype(jnp.int32)
        return (inject(total, resid, coord, angle, global_ids, live_count), None)
    start = jnp.zeros((375, nxe * nye * EZ), jnp.float32)
    total, unused = lax.scan(per_source, start, (residuals, coords, angles, element_ids, counts))
    injected = total.reshape(3, 5, 5, 5, nxe, nye, EZ).transpose(4, 5, 0, 1, 2, 3, 6)
    field = wavefield.reshape(nxe, nye, 3, 5, 5, 5, EZ)
    internal = lax.map(lambda pair: stiffness(pair[0], pair[1]), (field, moduli))
    force = injected - internal
    force = assemble_dim(force, 0, 3, fetch_none)
    force = assemble_dim(force, 1, 4, fetch_none)
    force = assemble_dim(force, 6, 5, fetch_none)
    return force.reshape(nxe, nye, 3, 125, EZ)
```

```python
import functools
import math

import jax
import jax.numpy as jnp
import numpy as np
from jax import lax
from jax.experimental import pallas as pl
from jax.experimental.pallas import tpu as pltpu
from jax.sharding import PartitionSpec as P

MESH = pl.DeviceIdType.MESH
F32 = jnp.float32
BF16 = jnp.bfloat16
NGX = 8
NGY = 16
NDEV = 128
NT = (((1,), (1,)), ((), ()))
NN = (((1,), (0,)), ((), ()))


def gll_points():
    return np.array([-1.0, -math.sqrt(3.0 / 7.0), 0.0, math.sqrt(3.0 / 7.0), 1.0])


def gll_weights():
    return np.array([0.1, 49.0 / 90.0, 32.0 / 45.0, 49.0 / 90.0, 0.1])


def derivative_table():
    points = gll_points()
    table = np.zeros((5, 5))
    for row in range(5):
        for col in range(5):
            if row == col:
                table[row, col] = sum(
                    (1.0 / (points[col] - points[other]) for other in range(5) if other != col)
                )
            else:
                value = 1.0 / (points[col] - points[row])
                for other in range(5):
                    if other != col and other != row:
                        value = (
                            value * (points[row] - points[other]) / (points[col] - points[other])
                        )
                table[row, col] = value
    return table


def split_np(a):
    hi = np.asarray(a, np.float32).astype(jnp.bfloat16)
    lo = (np.asarray(a, np.float64) - hi.astype(np.float64)).astype(jnp.bfloat16)
    return hi, lo


def row_of(p, q, r):
    pq = 5 * p + q
    return 120 + r if pq == 24 else 24 * r + pq


def operators():
    table = np.asarray(derivative_table(), np.float32).astype(np.float64)
    weight = np.asarray(gll_weights(), np.float32).astype(np.float64)
    grad = np.zeros((3, 128, 128))
    back = np.zeros((3, 128, 128))
    for p in range(5):
        for q in range(5):
            for r in range(5):
                n = 25 * p + 5 * q + r
                for k in range(5):
                    grad[0, n, 25 * k + 5 * q + r] = table[p, k]
                    grad[1, n, 25 * p + 5 * k + r] = table[q, k]
                    grad[2, n, 25 * p + 5 * q + k] = table[r, k]
                w = weight[p] * weight[q] * weight[r]
                for k in range(5):
                    back[0, row_of(k, q, r), n] = -w * table[p, k]
                    back[1, row_of(p, k, r), n] = -w * table[q, k]
                    back[2, row_of(p, q, k), n] = -w * table[r, k]
    ghi, glo = split_np(grad.reshape(384, 128))
    flat = np.concatenate([back[0], back[1], back[2]], axis=1)
    bhi, blo = split_np(flat)
    return np.concatenate([ghi, glo, ghi], axis=1), np.concatenate([bhi, blo, bhi], axis=1)


def basis_table():
    points = gll_points()
    out = np.zeros((8, 128))
    for node in range(5):
        poly = np.array([1.0])
        for other in range(5):
            if other != node:
                poly = np.convolve(poly, np.array([-points[other], 1.0])) / (
                    points[node] - points[other]
                )
        out[node, :5] = poly
    return out


def split(x):
    hi = x.astype(BF16)
    return hi, (x - hi.astype(F32)).astype(BF16)


def exchange_kernel(
    packed, wave, moduli, grad, back, recv, nst, wbuf, obuf, wsem, osem, lsem, ssem, rsem
):
    gx = lax.axis_index("gx")
    gy = lax.axis_index("gy")
    me = gx * NGY + gy
    fetch = pltpu.make_async_copy(wave, wbuf, wsem)
    fetch.start()
    own = pltpu.make_async_copy(packed.at[me], recv.at[me], lsem)
    own.start()
    bar = pltpu.get_barrier_semaphore()

    def greet(k, carry):
        t = (me + k) % NDEV
        pl.semaphore_signal(bar, inc=1, device_id=(t // NGY, t % NGY), device_id_type=MESH)
        return carry

    lax.fori_loop(1, NDEV, greet, 0)
    pl.semaphore_wait(bar, NDEV - 1)

    def send(k, carry):
        t = (me + k) % NDEV
        pltpu.make_async_remote_copy(
            src_ref=packed.at[t],
            dst_ref=recv.at[me],
            send_sem=ssem,
            recv_sem=rsem,
            device_id=(t // NGY, t % NGY),
            device_id_type=MESH,
        ).start()
        return carry

    lax.fori_loop(1, NDEV, send, 0)
    fetch.wait()

    def column(w, carry):
        cx = w // 2
        cy = w % 2
        lam = moduli[w, 0:1, :]
        mu = moduli[w, 1:2, :]
        grads = []
        for i in range(3):
            start = (cx * 3 + i) * 500 + cy
            u = jnp.concatenate(
                [wbuf[pl.ds(start + 2 * h, 125, stride=4), :] for h in range(2)], axis=1
            )
            u = jnp.concatenate([u, jnp.zeros((3, 256), F32)], axis=0)
            hi, lo = split(u)
            grads.append(
                lax.dot_general(
                    grad[...],
                    jnp.concatenate([hi, hi, lo], axis=0),
                    NN,
                    preferred_element_type=F32,
                )
            )
        g = [[grads[i][128 * j : 128 * j + 128] for j in range(3)] for i in range(3)]
        ldiv = lam * (g[0][0] + g[1][1] + g[2][2])
        parts = {}
        for i in range(3):
            for j in range(i, 3):
                s = mu * (g[i][j] + g[j][i])
                if i == j:
                    s = s + ldiv
                parts[(i, j)] = parts[(j, i)] = split(s)
        for i in range(3):
            hi = [parts[(i, j)][0] for j in range(3)]
            lo = [parts[(i, j)][1] for j in range(3)]
            obuf[w, 128 * i : 128 * i + 128, :] = lax.dot_general(
                back[...],
                jnp.concatenate(hi + hi + lo, axis=0),
                NN,
                preferred_element_type=F32,
            )
        return carry

    lax.fori_loop(0, 4, column, 0)
    put = pltpu.make_async_copy(obuf, nst, osem)
    put.start()
    own.wait()
    drain = pltpu.make_async_remote_copy(
        src_ref=packed.at[pl.ds(0, NDEV - 1)],
        dst_ref=recv.at[pl.ds(0, NDEV - 1)],
        send_sem=ssem,
        recv_sem=rsem,
        device_id=(gx, (gy + 1) % NGY),
        device_id_type=MESH,
    )
    drain.wait_send()
    drain.wait_recv()
    put.wait()


def exchange(packed, wave, moduli):
    grad, back = operators()
    vm = pl.BlockSpec(memory_space=pltpu.VMEM)
    anyspec = pl.BlockSpec(memory_space=pl.ANY)
    return pl.pallas_call(
        exchange_kernel,
        name="exchange",
        out_shape=(
            jax.ShapeDtypeStruct((NDEV, 7, 128), F32),
            jax.ShapeDtypeStruct((4, 384, 256), F32),
        ),
        in_specs=[anyspec, anyspec, vm, vm, vm],
        out_specs=(anyspec, anyspec),
        scratch_shapes=[
            pltpu.VMEM((3000, 128), F32),
            pltpu.VMEM((4, 384, 256), F32),
            pltpu.SemaphoreType.DMA(()),
            pltpu.SemaphoreType.DMA(()),
            pltpu.SemaphoreType.DMA(()),
            pltpu.SemaphoreType.DMA(()),
            pltpu.SemaphoreType.DMA(()),
        ],
        compiler_params=pltpu.CompilerParams(collective_id=0, has_side_effects=True),
    )(packed, wave, moduli, jnp.asarray(grad), jnp.asarray(back))


def sin_cos(x):
    y = 0.5 * x
    z = y * y
    s = y * (
        1.0
        + z * (-1.0 / 6 + z * (1.0 / 120 + z * (-1.0 / 5040 + z * (1.0 / 362880 + z * (-1.0 / 39916800)))))
    )
    c = 1.0 + z * (
        -0.5
        + z
        * (1.0 / 24 + z * (-1.0 / 720 + z * (1.0 / 40320 + z * (-1.0 / 3628800 + z * (1.0 / 479001600)))))
    )
    return 2.0 * s * c, 1.0 - 2.0 * s * s


def spread(x, first):
    row = lambda k: x[k : k + 1, :]
    shape = (8, x.shape[1])
    sub = lax.broadcasted_iota(jnp.int32, shape, 0)
    tiles = []
    for t in range(3):
        ks = [(8 * t + s) // 5 if first else (8 * t + s) % 5 for s in range(8)]
        if first:
            order = sorted(set(ks))
            tile = jnp.broadcast_to(row(order[0]), shape)
            for k in order[1:]:
                tile = jnp.where(sub >= ks.index(k), jnp.broadcast_to(row(k), shape), tile)
        else:
            q = (sub + 8 * t) % 5
            tile = jnp.broadcast_to(row(4), shape)
            for k in range(4):
                tile = jnp.where(q == k, jnp.broadcast_to(row(k), shape), tile)
        tiles.append(tile)
    return jnp.concatenate(tiles, axis=0)


def contributions(f, coef):
    def basis(k):
        x = jnp.broadcast_to(f[k : k + 1, :], (8, 256))
        a = [coef[:, m : m + 1] for m in range(5)]
        val = (((a[4] * x + a[3]) * x + a[2]) * x + a[1]) * x + a[0]
        der = ((4.0 * a[4] * x + 3.0 * a[3]) * x + 2.0 * a[2]) * x + a[1]
        return val, der

    vx, dx = basis(1)
    vy, dy = basis(2)
    vz, dz = basis(3)
    t = [f[4 + i : 5 + i, :] for i in range(3)]
    d = [f[0:1, :] * t[i] for i in range(3)]
    x1, x2, x3 = dx * t[0], vx * t[1], vx * t[2]
    ey, ed = spread(vy, False), spread(dy, False)
    a = spread(x1, True) * ey + spread(x2, True) * ed
    b = spread(x3, True) * ey
    shapes = [a * vz[r : r + 1, :] + b * dz[r : r + 1, :] for r in range(5)]
    a4 = x1[4:5, :] * vy[4:5, :] + x2[4:5, :] * dy[4:5, :]
    b4 = x3[4:5, :] * vy[4:5, :]
    shapes.append(a4 * vz + b4 * dz)
    shape = jnp.concatenate(shapes, axis=0)
    return jnp.concatenate([shape * d[i] for i in range(3)], axis=0)


def inject_kernel(
    recv, nst, coef_ref, upper, out, xlo, xhi, ylo, yhi, corner,
    acc, flds, pos_s, srt, win, tabv, tabs, nsem, tsem,
):
    load = pltpu.make_async_copy(nst, acc, nsem)
    load.start()
    ids = recv[:, 6, :]
    sin_a, cos_a = sin_cos(recv[:, 4, :])
    sin_d, cos_d = sin_cos(recv[:, 5, :])
    colf = jnp.floor(ids * (1.0 / 256.0))
    for k in range(4):
        flds[:, k, :] = recv[:, k, :]
    flds[:, 4, :] = cos_a * cos_d
    flds[:, 5, :] = sin_a * cos_d
    flds[:, 6, :] = sin_d
    flds[:, 7, :] = ids - 256.0 * colf
    masks = [(colf == float(w)).astype(F32).astype(BF16) for w in range(4)]
    stacked = jnp.concatenate(masks, axis=0)
    up = upper[...]
    ones = jnp.ones((128, 128), BF16)
    prefix = lax.dot_general(stacked, up, NN, preferred_element_type=F32)
    total = lax.dot_general(stacked, ones, NN, preferred_element_type=F32)
    start = jnp.zeros((128, 128), F32)
    pos = jnp.full((128, 128), -1.0, F32)
    for w in range(4):
        pos = jnp.where(colf == float(w), prefix[128 * w : 128 * w + 128] + start, pos)
        start = start + total[128 * w : 128 * w + 128]
    pos_s[...] = pos
    sub = lax.broadcasted_iota(jnp.int32, (16, 128), 0)
    table = jnp.zeros((16, 128), F32)
    first = jnp.zeros((16, 128), F32)
    for w in range(4):
        tot = lax.dot_general(jnp.ones((16, 128), BF16), masks[w], NT, preferred_element_type=F32)
        fill = lax.dot_general(tot.astype(BF16), up, NN, preferred_element_type=F32)
        table = jnp.where(sub == w, tot, table)
        table = jnp.where(sub == 4 + w, first, table)
        table = jnp.where(sub == 8 + w, fill, table)
        first = first + tot
    tabv[...] = table.astype(jnp.int32)
    totab = pltpu.make_async_copy(tabv, tabs, tsem)
    totab.start()

    lane_row = lax.broadcasted_iota(jnp.int32, (128, 128), 0).astype(F32)

    def sort_group(g, carry):
        for k in range(8):
            t = g * 8 + k
            f = flds[t]
            hi = f.astype(BF16).astype(F32)
            mid = (f - hi).astype(BF16).astype(F32)
            lo = f - hi - mid
            perm = jnp.where(lane_row == pos_s[pl.ds(t, 1), :], 1.0, 0.0).astype(BF16)
            got = lax.dot_general(
                jnp.concatenate([hi, mid, lo], axis=0).astype(BF16),
                perm,
                NT,
                preferred_element_type=F32,
            )
            srt[t] = got[0:8] + got[8:16] + got[16:24]
        return carry

    lax.fori_loop(0, 16, sort_group, 0)
    totab.wait()

    lane = lax.broadcasted_iota(jnp.int32, (8, 128), 1)
    zero = jnp.zeros((8, 128), F32)

    def place(t, cur):
        tile = srt[t]
        new = []
        for w in range(4):
            n = tabs[w, t]
            st = tabs[4 + w, t]
            fl = tabs[8 + w, t]
            c0 = fl // 128
            o = fl % 128
            rolled = pltpu.roll(tile, (o - st + 128) % 128, axis=1)
            low = jnp.where(lane < o, cur[w], jnp.where(lane < o + n, rolled, zero))
            high = jnp.where(lane < o + n - 128, rolled, zero)
            win[w, c0] = low
            win[w, c0 + 1] = high
            new.append(jnp.where(o + n >= 128, high, low))
        return tuple(new)

    lax.fori_loop(0, 128, place, (zero,) * 4)
    load.wait()
    coef = coef_ref[...]
    row = lax.broadcasted_iota(jnp.int32, (256, 256), 0).astype(F32)
    for w in range(4):
        count = tabs[8 + w, 127] + tabs[w, 127]
        win[w, (count + 127) // 128] = zero

        def block(b, carry, w=w):
            f = jnp.concatenate([win[w, 2 * b], win[w, 2 * b + 1]], axis=1)
            hi, lo = split(contributions(f, coef))
            onehot = jnp.where(row == f[7:8, :], 1.0, 0.0).astype(BF16)
            acc[w] += lax.dot_general(
                jnp.concatenate([hi, lo], axis=1),
                jnp.concatenate([onehot, onehot], axis=1),
                NT,
                preferred_element_type=F32,
            )
            return carry

        lax.fori_loop(0, (count + 255) // 256, block, 0)

    lane2 = lax.broadcasted_iota(jnp.int32, (8, 256), 1)
    for w in range(4):
        cx, cy = w // 2, w % 2
        for i in range(3):
            base = 128 * i
            g = [acc[w, base + 24 * r : base + 24 * r + 24, :] for r in range(5)]
            tail = acc[w, base + 120 : base + 128, :]
            groups = [g[0], tail[0:1, :]], [g[4], tail[4:5, :]]
            lows, highs = [], []
            for a, b in zip(*groups):
                ln = lax.broadcasted_iota(jnp.int32, a.shape, 1)
                lows.append(a + jnp.where(ln == 0, 0.0, pltpu.roll(b, 1, axis=1)))
                highs.append(b + jnp.where(ln == 255, 0.0, pltpu.roll(a, 255, axis=1)))
            main = [lows[0], g[1], g[2], g[3], highs[0]]
            last = [lows[1], tail[1:2, :], tail[2:3, :], tail[3:4, :], highs[1]]
            origin = (cx * 3 + i) * 500 + cy
            for r in range(5):
                for h in range(2):
                    cols = slice(128 * h, 128 * h + 128)
                    at = origin + 4 * r + 2 * h
                    out[pl.ds(at, 24, stride=20), :] = main[r][:, cols]
                    out[pl.ds(at + 480, 1), :] = last[r][:, cols]
    for i in range(3):
        a = out[i * 500 + 400 : i * 500 + 500, :]
        b = out[(3 + i) * 500 : (3 + i) * 500 + 100, :]
        out[i * 500 + 400 : i * 500 + 500, :] = a + b
        out[(3 + i) * 500 : (3 + i) * 500 + 100, :] = a + b
    for c in range(6):
        for p in range(5):
            high = pl.ds(c * 500 + 100 * p + 80, 10, stride=2)
            low = pl.ds(c * 500 + 100 * p + 1, 10, stride=2)
            both = out[high, :] + out[low, :]
            out[high, :] = both
            out[low, :] = both
    for i in range(3):
        xlo[100 * i : 100 * i + 100, :] = out[i * 500 : i * 500 + 100, :]
        xhi[100 * i : 100 * i + 100, :] = out[(3 + i) * 500 + 400 : (3 + i) * 500 + 500, :]
    for c in range(6):
        for p in range(5):
            at = 50 * c + 10 * p
            ylo[at : at + 10, :] = out[pl.ds(c * 500 + 100 * p, 10, stride=2), :]
            yhi[at : at + 10, :] = out[pl.ds(c * 500 + 100 * p + 81, 10, stride=2), :]
    for cx in range(2):
        for cy in range(2):
            for i in range(3):
                start = (cx * 3 + i) * 500 + 400 * cx + 80 * cy + cy
                corner[2 * cx + cy, 10 * i : 10 * i + 10, :] = out[pl.ds(start, 10, stride=2), :]


def inject(recv, nst):
    vm = pl.BlockSpec(memory_space=pltpu.VMEM)
    anyspec = pl.BlockSpec(memory_space=pl.ANY)
    face = jax.ShapeDtypeStruct((304, 128), F32)
    upper = np.triu(np.ones((128, 128), np.float32), 1)
    return pl.pallas_call(
        inject_kernel,
        name="inject",
        out_shape=(
            jax.ShapeDtypeStruct((3000, 128), F32),
            face, face, face, face,
            jax.ShapeDtypeStruct((4, 32, 128), F32),
        ),
        in_specs=[vm, anyspec, vm, vm],
        out_specs=(vm,) * 6,
        scratch_shapes=[
            pltpu.VMEM((4, 384, 256), F32),
            pltpu.VMEM((128, 8, 128), F32),
            pltpu.VMEM((128, 128), F32),
            pltpu.VMEM((128, 8, 128), F32),
            pltpu.VMEM((4, 132, 8, 128), F32),
            pltpu.VMEM((16, 128), jnp.int32),
            pltpu.SMEM((16, 128), jnp.int32),
            pltpu.SemaphoreType.DMA(()),
            pltpu.SemaphoreType.DMA(()),
        ],
        compiler_params=pltpu.CompilerParams(vmem_limit_bytes=48 * 2**20),
    )(recv, nst, jnp.asarray(basis_table(), F32), jnp.asarray(upper, BF16))


SIDES = [(-1, 0), (1, 0), (0, -1), (0, 1), (-1, -1), (-1, 1), (1, -1), (1, 1)]


def halo_kernel(xlo, xhi, ylo, yhi, corner, gxlo, gxhi, gylo, gyhi, gcorner, ssem, rsem):
    gx = lax.axis_index("gx")
    gy = lax.axis_index("gy")
    bar = pltpu.get_barrier_semaphore()

    def there(side):
        dx, dy = side
        ok = None
        for d, g, n in ((dx, gx, NGX), (dy, gy, NGY)):
            if d:
                c = (g + d >= 0) & (g + d < n)
                ok = c if ok is None else ok & c
        return ok

    for side in SIDES:
        @pl.when(there(side))
        def _(side=side):
            pl.semaphore_signal(
                bar, inc=1, device_id=(gx + side[0], gy + side[1]), device_id_type=MESH
            )
    nx = (gx > 0).astype(jnp.int32) + (gx < NGX - 1).astype(jnp.int32)
    ny = (gy > 0).astype(jnp.int32) + (gy < NGY - 1).astype(jnp.int32)
    pl.semaphore_wait(bar, (nx + 1) * (ny + 1) - 1)

    src = [xlo, xhi, ylo, yhi] + [corner.at[k] for k in range(4)]
    dst = [gxhi, gxlo, gyhi, gylo] + [gcorner.at[3 - k] for k in range(4)]

    def copy(k):
        side = SIDES[k]
        return pltpu.make_async_remote_copy(
            src_ref=src[k],
            dst_ref=dst[k],
            send_sem=ssem.at[k],
            recv_sem=rsem.at[k],
            device_id=(gx + side[0], gy + side[1]),
            device_id_type=MESH,
        )

    opposite = [1, 0, 3, 2, 7, 6, 5, 4]
    for k in range(8):
        @pl.when(there(SIDES[k]))
        def _(k=k):
            copy(k).start()
    for k in range(8):
        @pl.when(there(SIDES[k]))
        def _(k=k):
            copy(k).wait_send()
            copy(opposite[k]).wait_recv()


def halo(xlo, xhi, ylo, yhi, corner):
    anyspec = pl.BlockSpec(memory_space=pl.ANY)
    face = jax.ShapeDtypeStruct((304, 128), F32)
    return pl.pallas_call(
        halo_kernel,
        name="halo",
        out_shape=(face, face, face, face, jax.ShapeDtypeStruct((4, 32, 128), F32)),
        in_specs=[anyspec] * 5,
        out_specs=(anyspec,) * 5,
        scratch_shapes=[pltpu.SemaphoreType.DMA((8,)), pltpu.SemaphoreType.DMA((8,))],
        compiler_params=pltpu.CompilerParams(collective_id=1, has_side_effects=True),
    )(xlo, xhi, ylo, yhi, corner)


def finish_kernel(at, local, gxlo, gxhi, gylo, gyhi, gcorner, out):
    gx = at[0]
    gy = at[1]
    out[...] = local[...]

    @pl.when(gx > 0)
    def _():
        for i in range(3):
            out[i * 500 : i * 500 + 100, :] += gxlo[100 * i : 100 * i + 100, :]

    @pl.when(gx < NGX - 1)
    def _():
        for i in range(3):
            out[(3 + i) * 500 + 400 : (3 + i) * 500 + 500, :] += gxhi[100 * i : 100 * i + 100, :]

    @pl.when(gy > 0)
    def _():
        for c in range(6):
            for p in range(5):
                k = 50 * c + 10 * p
                out[pl.ds(c * 500 + 100 * p, 10, stride=2), :] += gylo[k : k + 10, :]

    @pl.when(gy < NGY - 1)
    def _():
        for c in range(6):
            for p in range(5):
                k = 50 * c + 10 * p
                out[pl.ds(c * 500 + 100 * p + 81, 10, stride=2), :] += gyhi[k : k + 10, :]

    for cx in range(2):
        for cy in range(2):
            okx = (gx < NGX - 1) if cx else (gx > 0)
            oky = (gy < NGY - 1) if cy else (gy > 0)

            @pl.when(okx & oky)
            def _(cx=cx, cy=cy):
                for i in range(3):
                    start = (cx * 3 + i) * 500 + 400 * cx + 80 * cy + cy
                    rows = pl.ds(start, 10, stride=2)
                    out[rows, :] += gcorner[2 * cx + cy, 10 * i : 10 * i + 10, :]


def finish(local, got):
    at = jnp.stack([lax.axis_index("gx"), lax.axis_index("gy")]).astype(jnp.int32)
    vm = pl.BlockSpec(memory_space=pltpu.VMEM)
    return pl.pallas_call(
        finish_kernel,
        name="finish",
        out_shape=jax.ShapeDtypeStruct((3000, 128), F32),
        in_specs=[pl.BlockSpec(memory_space=pltpu.SMEM)] + [vm] * 6,
        out_specs=vm,
    )(at, local, *got)


def body(wavefield, moduli, residuals, coords, angles, element_ids, counts):
    live = jnp.arange(128, dtype=jnp.int32)[None, :] < counts[0][:, None]
    ids = jnp.where(live, element_ids[0], -1).astype(F32)
    packed = jnp.concatenate(
        [residuals[0][:, None, :], coords[0], angles[0], ids[:, None, :]], axis=1
    )
    wave = wavefield.reshape(2, 2, 3, 125, 2, 128).transpose(0, 2, 3, 4, 1, 5).reshape(3000, 128)
    recv, nst = exchange(packed, wave, moduli.reshape(4, 2, 256))
    local, xlo, xhi, ylo, yhi, corner = inject(recv, nst)
    got = halo(xlo, xhi, ylo, yhi, corner)
    out = finish(local, got)
    out = out.reshape(2, 3, 125, 2, 2, 128).transpose(0, 4, 1, 2, 3, 5)
    return out.reshape(2, 2, 3, 125, 256)


def solution(mesh):
    in_specs = (
        P("gx", "gy", None, None, None),
        P("gx", "gy", None, None),
        P(("gx", "gy"), None, None),
        P(("gx", "gy"), None, None, None),
        P(("gx", "gy"), None, None, None),
        P(("gx", "gy"), None, None),
        P(("gx", "gy"), None),
    )
    out_specs = P("gx", "gy", None, None, None)
    return jax.shard_map(body, mesh=mesh, in_specs=in_specs, out_specs=out_specs, check_vma=False)
```

```python
import functools
import math

import jax
import jax.numpy as jnp
import numpy as np
from jax import lax
from jax.experimental import pallas as pl
from jax.experimental.pallas import tpu as pltpu
from jax.sharding import PartitionSpec as P

MESH = pl.DeviceIdType.MESH
F32 = jnp.float32
BF16 = jnp.bfloat16
NGX = 8
NGY = 16
NDEV = 128
CHUNKS = 136
TOT = 128
NST = 192
NT = (((1,), (1,)), ((), ()))
NN = (((1,), (0,)), ((), ()))


def gll_points():
    return np.array([-1.0, -math.sqrt(3.0 / 7.0), 0.0, math.sqrt(3.0 / 7.0), 1.0])


def gll_weights():
    return np.array([0.1, 49.0 / 90.0, 32.0 / 45.0, 49.0 / 90.0, 0.1])


def derivative_table():
    points = gll_points()
    table = np.zeros((5, 5))
    for row in range(5):
        for col in range(5):
            if row == col:
                table[row, col] = sum(
                    (1.0 / (points[col] - points[other]) for other in range(5) if other != col)
                )
            else:
                value = 1.0 / (points[col] - points[row])
                for other in range(5):
                    if other != col and other != row:
                        value = (
                            value * (points[row] - points[other]) / (points[col] - points[other])
                        )
                table[row, col] = value
    return table


def split_np(a):
    hi = np.asarray(a, np.float32).astype(jnp.bfloat16)
    lo = (np.asarray(a, np.float64) - hi.astype(np.float64)).astype(jnp.bfloat16)
    return hi, lo


def row_of(p, q, r):
    pq = 5 * p + q
    return 120 + r if pq == 24 else 24 * r + pq


def operators():
    table = np.asarray(derivative_table(), np.float32).astype(np.float64)
    weight = np.asarray(gll_weights(), np.float32).astype(np.float64)
    grad = np.zeros((3, 128, 128))
    back = np.zeros((3, 128, 128))
    for p in range(5):
        for q in range(5):
            for r in range(5):
                n = 25 * p + 5 * q + r
                for k in range(5):
                    grad[0, n, 25 * k + 5 * q + r] = table[p, k]
                    grad[1, n, 25 * p + 5 * k + r] = table[q, k]
                    grad[2, n, 25 * p + 5 * q + k] = table[r, k]
                w = weight[p] * weight[q] * weight[r]
                for k in range(5):
                    back[0, row_of(k, q, r), n] = -w * table[p, k]
                    back[1, row_of(p, k, r), n] = -w * table[q, k]
                    back[2, row_of(p, q, k), n] = -w * table[r, k]
    ghi, glo = split_np(grad.reshape(384, 128))
    flat = np.concatenate([back[0], back[1], back[2]], axis=1)
    bhi, blo = split_np(flat)
    return np.concatenate([ghi, glo, ghi], axis=1), np.concatenate([bhi, blo, bhi], axis=1)


def basis_table():
    points = gll_points()
    out = np.zeros((8, 128))
    for node in range(5):
        poly = np.array([1.0])
        for other in range(5):
            if other != node:
                poly = np.convolve(poly, np.array([-points[other], 1.0])) / (
                    points[node] - points[other]
                )
        out[node, :5] = poly
    return out


def split(x):
    hi = x.astype(BF16)
    return hi, (x - hi.astype(F32)).astype(BF16)


def sin_cos(x):
    y = 0.5 * x
    z = y * y
    s = y * (
        1.0
        + z * (-1.0 / 6 + z * (1.0 / 120 + z * (-1.0 / 5040 + z * (1.0 / 362880 + z * (-1.0 / 39916800)))))
    )
    c = 1.0 + z * (
        -0.5
        + z
        * (1.0 / 24 + z * (-1.0 / 720 + z * (1.0 / 40320 + z * (-1.0 / 3628800 + z * (1.0 / 479001600)))))
    )
    return 2.0 * s * c, 1.0 - 2.0 * s * s


def far_first(j):
    return 2 + ((j + 1) // 2) * (1 - 2 * (j % 2))


def exchange_kernel(
    resid, coords, angles, ids, counts, wave, moduli, grad, back, upper,
    big,
    stage, fm, abuf, ibuf, cbuf, wbuf, mbuf, gbuf, bbuf, ubuf, recv, fl, pos_s,
    isem, wsem, bsem, ssem, rsem, osem,
):
    gx = lax.axis_index("gx")
    gy = lax.axis_index("gy")
    me = gx * NGY + gy
    y, core, z, x = gx // 2, gx % 2, gy // 4, gy % 4
    loads = [
        pltpu.make_async_copy(resid, fm.at[0], isem.at[0]),
        pltpu.make_async_copy(coords, fm.at[pl.ds(1, 3)], isem.at[1]),
        pltpu.make_async_copy(angles, abuf, isem.at[2]),
        pltpu.make_async_copy(ids, ibuf, isem.at[3]),
        pltpu.make_async_copy(counts, cbuf, isem.at[4]),
    ]
    fetches = [
        pltpu.make_async_copy(a, b, wsem.at[k])
        for k, (a, b) in enumerate(
            ((wave, wbuf), (moduli, mbuf), (grad, gbuf), (back, bbuf), (upper, ubuf))
        )
    ]
    for load in loads + fetches:
        load.start()
    bar = pltpu.get_barrier_semaphore()
    for k in range(1, NGY):
        pl.semaphore_signal(bar, inc=1, device_id=(gx, (gy + k) % NGY), device_id_type=MESH)
    for k in range(1, NGX):
        pl.semaphore_signal(bar, inc=1, device_id=((gx + k) % NGX, gy), device_id_type=MESH)
    for load in loads:
        load.wait()
    fm[4] = abuf[pl.ds(0, 128, stride=2), :]
    fm[5] = abuf[pl.ds(1, 128, stride=2), :]
    limit = jnp.transpose(jnp.broadcast_to(cbuf[...].astype(F32), (128, 128)))
    slot = lax.broadcasted_iota(jnp.int32, (128, 128), 1).astype(F32)
    fm[6] = jnp.where(slot < limit, ibuf[...].astype(F32), -1.0)
    pl.semaphore_wait(bar, NGX + NGY - 2)
    for k in range(1, NGX):
        pl.semaphore_signal(bsem, inc=1, device_id=((gx + k) % NGX, gy), device_id_type=MESH)
    for f in range(7):
        recv[3, f, 31:32, :] = fm[f, pl.ds(me, 1), :]
    pl.semaphore_wait(bsem, NGX - 1)

    def send(j, last):
        ty = (y + far_first(j // 4)) % 4
        tz = (z + far_first(j % 4)) % 4
        for m in range(7 if last else 8):
            tx = (x + far_first(m // 2)) % 4
            tc = (core + 1 - m % 2) % 2
            t = (2 * ty + tc) * NGY + 4 * tz + tx
            pltpu.make_async_remote_copy(
                src_ref=fm.at[:, t, :],
                dst_ref=recv.at[j // 4, :, (j % 4) * 8 + m, :],
                send_sem=ssem,
                recv_sem=rsem.at[j // 4],
                device_id=(2 * ty + tc, 4 * tz + tx),
                device_id_type=MESH,
            ).start()

    def send_eight(j, carry):
        send(j, False)
        return carry

    lax.fori_loop(0, 15, send_eight, 0)
    send(15, True)
    for fetch in fetches:
        fetch.wait()

    def column(w, carry):
        cx = w // 2
        cy = w % 2
        lam = mbuf[w, 0:1, :]
        mu = mbuf[w, 1:2, :]
        grads = []
        for i in range(3):
            start = (cx * 3 + i) * 500 + cy
            u = jnp.concatenate(
                [wbuf[pl.ds(start + 2 * h, 125, stride=4), :] for h in range(2)], axis=1
            )
            u = jnp.concatenate([u, jnp.zeros((3, 256), F32)], axis=0)
            hi, lo = split(u)
            grads.append(
                lax.dot_general(
                    gbuf[...],
                    jnp.concatenate([hi, hi, lo], axis=0),
                    NN,
                    preferred_element_type=F32,
                )
            )
        g = [[grads[i][128 * j : 128 * j + 128] for j in range(3)] for i in range(3)]
        ldiv = lam * (g[0][0] + g[1][1] + g[2][2])
        parts = {}
        for i in range(3):
            for j in range(i, 3):
                s = mu * (g[i][j] + g[j][i])
                if i == j:
                    s = s + ldiv
                parts[(i, j)] = parts[(j, i)] = split(s)
        for i in range(3):
            hi = [parts[(i, j)][0] for j in range(3)]
            lo = [parts[(i, j)][1] for j in range(3)]
            got = lax.dot_general(
                bbuf[...],
                jnp.concatenate(hi + hi + lo, axis=0),
                NN,
                preferred_element_type=F32,
            )
            for h in range(2):
                at = NST + 192 * h + 48 * w + 16 * i
                stage[pl.ds(at, 16)] = got[:, 128 * h : 128 * h + 128].reshape(16, 8, 128)
        return carry

    lax.fori_loop(0, 4, column, 0)

    def put(lo, n, k):
        return pltpu.make_async_copy(stage.at[pl.ds(lo, n)], big.at[pl.ds(lo, n)], osem.at[k])

    put(NST, 384, 0).start()
    up = ubuf[...]
    ones = jnp.ones((128, 128), BF16)
    lane_row = lax.broadcasted_iota(jnp.int32, (128, 128), 0).astype(F32)

    def waiter(ref, group):
        return pltpu.make_async_remote_copy(
            src_ref=ref,
            dst_ref=ref,
            send_sem=ssem,
            recv_sem=rsem.at[group],
            device_id=(gx, (gy + 1) % NGY),
            device_id_type=MESH,
        )

    def prepare(g):
        sin_a, cos_a = sin_cos(recv[g, 4])
        sin_d, cos_d = sin_cos(recv[g, 5])
        num = recv[g, 6]
        colf = jnp.floor(num * (1.0 / 256.0))
        for k in range(4):
            fl[32 * k : 32 * k + 32, :] = recv[g, k]
        fl[128:160, :] = cos_a * cos_d
        fl[160:192, :] = sin_a * cos_d
        fl[192:224, :] = sin_d
        fl[224:256, :] = num - 256.0 * colf
        stacked = jnp.concatenate(
            [(colf == float(w)).astype(F32).astype(BF16) for w in range(4)], axis=0
        )
        prefix = lax.dot_general(stacked, up, NN, preferred_element_type=F32)
        total = lax.dot_general(stacked, ones, NN, preferred_element_type=F32)
        start = jnp.zeros((32, 128), F32)
        pos = jnp.full((32, 128), -1.0, F32)
        for w in range(4):
            n = total[32 * w : 32 * w + 32]
            stage[pl.ds(TOT + 16 * w + 4 * g, 4)] = n.reshape(4, 8, 128)
            pos = jnp.where(colf == float(w), prefix[32 * w : 32 * w + 32] + start, pos)
            start = start + n
        pos_s[...] = pos

        def sort_some(h, carry):
            for k in range(16):
                t = h * 16 + k
                f = fl[pl.ds(t, 8, stride=32), :]
                hi = f.astype(BF16).astype(F32)
                mid = (f - hi).astype(BF16).astype(F32)
                lo = f - hi - mid
                perm = jnp.where(lane_row == pos_s[pl.ds(t, 1), :], 1.0, 0.0).astype(BF16)
                got = lax.dot_general(
                    jnp.concatenate([hi, mid, lo], axis=0).astype(BF16),
                    perm,
                    NT,
                    preferred_element_type=F32,
                )
                stage[g * 32 + t] = got[0:8] + got[8:16] + got[16:24]
            return carry

        lax.fori_loop(0, 2, sort_some, 0)

    def group(g, carry):
        waiter(recv.at[g], g).wait_recv()
        prepare(g)
        return carry

    lax.fori_loop(0, 3, group, 0)
    waiter(recv.at[3, :, pl.ds(0, 31), :], 3).wait_recv()
    prepare(3)
    put(0, 192, 1).start()
    waiter(fm.at[:, pl.ds(0, 127), :], 0).wait_send()
    put(NST, 384, 0).wait()
    put(0, 192, 1).wait()


def exchange(resid, coords, angles, ids, counts, wave, moduli):
    grad, back = operators()
    upper = np.triu(np.ones((128, 128), np.float32), 1)
    return pl.pallas_call(
        exchange_kernel,
        name="exchange",
        out_shape=jax.ShapeDtypeStruct((576, 8, 128), F32),
        in_specs=[pl.BlockSpec(memory_space=pltpu.HBM)] * 10,
        out_specs=pl.BlockSpec(memory_space=pltpu.HBM),
        scratch_shapes=[
            pltpu.VMEM((576, 8, 128), F32),
            pltpu.VMEM((7, 128, 128), F32),
            pltpu.VMEM((256, 128), F32),
            pltpu.VMEM((128, 128), jnp.int32),
            pltpu.VMEM((1, 128), jnp.int32),
            pltpu.VMEM((3000, 128), F32),
            pltpu.VMEM((4, 2, 256), F32),
            pltpu.VMEM((384, 384), BF16),
            pltpu.VMEM((128, 1152), BF16),
            pltpu.VMEM((128, 128), BF16),
            pltpu.VMEM((4, 7, 32, 128), F32),
            pltpu.VMEM((256, 128), F32),
            pltpu.VMEM((32, 128), F32),
            pltpu.SemaphoreType.DMA((5,)),
            pltpu.SemaphoreType.DMA((5,)),
            pltpu.SemaphoreType.REGULAR,
            pltpu.SemaphoreType.DMA(()),
            pltpu.SemaphoreType.DMA((4,)),
            pltpu.SemaphoreType.DMA((2,)),
        ],
        compiler_params=pltpu.CompilerParams(
            collective_id=0, has_side_effects=True, vmem_limit_bytes=60 * 2**20
        ),
    )(
        resid, coords, angles, ids, counts, wave, moduli,
        jnp.asarray(grad), jnp.asarray(back), jnp.asarray(upper, BF16),
    )


def spread(x, first):
    row = lambda k: x[k : k + 1, :]
    shape = (8, x.shape[1])
    sub = lax.broadcasted_iota(jnp.int32, shape, 0)
    tiles = []
    for t in range(3):
        ks = [(8 * t + s) // 5 if first else (8 * t + s) % 5 for s in range(8)]
        if first:
            order = sorted(set(ks))
            tile = jnp.broadcast_to(row(order[0]), shape)
            for k in order[1:]:
                tile = jnp.where(sub >= ks.index(k), jnp.broadcast_to(row(k), shape), tile)
        else:
            q = (sub + 8 * t) % 5
            tile = jnp.broadcast_to(row(4), shape)
            for k in range(4):
                tile = jnp.where(q == k, jnp.broadcast_to(row(k), shape), tile)
        tiles.append(tile)
    return jnp.concatenate(tiles, axis=0)


def contributions(f, coef):
    def basis(k):
        x = jnp.broadcast_to(f[k : k + 1, :], (8, 256))
        a = [coef[:, m : m + 1] for m in range(5)]
        val = (((a[4] * x + a[3]) * x + a[2]) * x + a[1]) * x + a[0]
        der = ((4.0 * a[4] * x + 3.0 * a[3]) * x + 2.0 * a[2]) * x + a[1]
        return val, der

    vx, dx = basis(1)
    vy, dy = basis(2)
    vz, dz = basis(3)
    t = [f[4 + i : 5 + i, :] for i in range(3)]
    d = [f[0:1, :] * t[i] for i in range(3)]
    x1, x2, x3 = dx * t[0], vx * t[1], vx * t[2]
    ey, ed = spread(vy, False), spread(dy, False)
    a = spread(x1, True) * ey + spread(x2, True) * ed
    b = spread(x3, True) * ey
    shapes = [a * vz[r : r + 1, :] + b * dz[r : r + 1, :] for r in range(5)]
    a4 = x1[4:5, :] * vy[4:5, :] + x2[4:5, :] * dy[4:5, :]
    b4 = x3[4:5, :] * vy[4:5, :]
    shapes.append(a4 * vz + b4 * dz)
    shape = jnp.concatenate(shapes, axis=0)
    return jnp.concatenate([shape * d[i] for i in range(3)], axis=0)


def inject_kernel(
    big, coef_ref, upper, lower, out, xlo, xhi, ylo, yhi, corner,
    acc, win, tabv, tabs, begin, end, lhs_a, lhs_b, num_a, num_b, tsem,
):
    up = upper[...]
    down = lower[...]
    sub = lax.broadcasted_iota(jnp.int32, (16, 128), 0)
    lane16 = lax.broadcasted_iota(jnp.int32, (16, 128), 1)
    pick = jnp.where(lane16 == 0, 1.0, 0.0).astype(BF16)
    table = jnp.zeros((16, 128), jnp.int32)
    first = jnp.zeros((16, 128), jnp.int32)
    for w in range(4):
        n_rows = big[TOT + 16 * w : TOT + 16 * w + 16].reshape(128, 128)
        n_bf = n_rows.astype(BF16)
        n = lax.dot_general(pick, n_bf, NT, preferred_element_type=F32)
        fill = lax.dot_general(n.astype(BF16), up, NN, preferred_element_type=F32)
        n = n.astype(jnp.int32)
        fill = fill.astype(jnp.int32)
        word = ((fill >> 7) + CHUNKS * w) * 128 + ((fill - first) & 127)
        table = jnp.where(sub == w, word, table)
        table = jnp.where(sub == 4 + w, fill + n, table)
        first = first + n
        at = lax.dot_general(down, n_bf, NN, preferred_element_type=F32).astype(jnp.int32) & 127
        begin[w] = at
        end[w] = at + n_rows.astype(jnp.int32)
    tabv[...] = table
    totab = pltpu.make_async_copy(tabv, tabs, tsem)
    totab.start()
    totab.wait()

    lane = lax.broadcasted_iota(jnp.int32, (8, 128), 1)
    zero = jnp.zeros((8, 128), F32)

    def place(step, cur):
        for h in range(2):
            part = big[pl.ds(NST + 192 * h + 6 * step, 6)].reshape(48, 128)
            acc[pl.ds(step * 48, 48), 128 * h : 128 * h + 128] = part
        for k in range(4):
            t = step * 4 + k
            tile = big[t]
            new = []
            for w in range(4):
                b = jnp.broadcast_to(begin[w, pl.ds(t, 1), :], (8, 128))
                e = jnp.broadcast_to(end[w, pl.ds(t, 1), :], (8, 128))
                word = tabs[w, t]
                chunk = word >> 7
                rolled = pltpu.roll(tile, word & 127, axis=1)
                low = jnp.where(lane < b, cur[w], jnp.where(lane < e, rolled, zero))
                high = jnp.where(lane + 128 < e, rolled, zero)
                win[chunk] = low
                win[chunk + 1] = high
                new.append(jnp.where(e >= 128, high, low))
            cur = tuple(new)
        return cur

    lax.fori_loop(0, 32, place, (zero,) * 4)
    coef = coef_ref[...]
    row = lax.broadcasted_iota(jnp.int32, (256, 256), 0).astype(F32)
    upto = [0]
    for w in range(4):
        count = tabs[4 + w, 127]
        for k in range(3):
            win[CHUNKS * w + (count + 127) // 128 + k] = zero
        upto.append(upto[-1] + (count + 511) // 512)
    for k in range(4):
        win[4 * CHUNKS + k] = zero

    def which(u):
        w = jnp.int32(0)
        at = u * 4
        for k in range(1, 4):
            past = u >= upto[k]
            w = jnp.where(past, k, w)
            at = jnp.where(past, CHUNKS * k + (u - upto[k]) * 4, at)
        done = u >= upto[4]
        return jnp.where(done, 0, w), jnp.where(done, 4 * CHUNKS, at)

    def fill_unit(u, lhs, num):
        _, at = which(u)
        for k in range(2):
            f = jnp.concatenate([win[at + 2 * k], win[at + 2 * k + 1]], axis=1)
            hi, lo = split(contributions(f, coef))
            lhs[k, :, 0:256] = hi
            lhs[k, :, 256:512] = lo
            num[:, 256 * k : 256 * k + 256] = jnp.broadcast_to(f[7:8, :], (8, 256))

    def use_unit(u, lhs, num):
        w, _ = which(u)
        part = pl.ds(pl.multiple_of(w * 384, 384), 384)
        total = None
        for k in range(2):
            onehot = jnp.where(row == num[0:1, 256 * k : 256 * k + 256], 1.0, 0.0).astype(BF16)
            got = lax.dot_general(
                lhs[k],
                jnp.concatenate([onehot, onehot], axis=1),
                NT,
                preferred_element_type=F32,
            )
            total = got if total is None else total + got
        acc[part, :] += total

    fill_unit(0, lhs_a, num_a)

    def two_units(step, carry):
        u = 2 * step
        fill_unit(u + 1, lhs_b, num_b)
        use_unit(u, lhs_a, num_a)
        fill_unit(u + 2, lhs_a, num_a)
        use_unit(u + 1, lhs_b, num_b)
        return carry

    lax.fori_loop(0, (upto[4] + 1) // 2, two_units, 0)

    lane2 = lax.broadcasted_iota(jnp.int32, (8, 256), 1)
    for w in range(4):
        cx, cy = w // 2, w % 2
        for i in range(3):
            base = 384 * w + 128 * i
            g = [acc[base + 24 * r : base + 24 * r + 24, :] for r in range(5)]
            tail = acc[base + 120 : base + 128, :]
            groups = [g[0], tail[0:1, :]], [g[4], tail[4:5, :]]
            lows, highs = [], []
            for a, b in zip(*groups):
                ln = lax.broadcasted_iota(jnp.int32, a.shape, 1)
                lows.append(a + jnp.where(ln == 0, 0.0, pltpu.roll(b, 1, axis=1)))
                highs.append(b + jnp.where(ln == 255, 0.0, pltpu.roll(a, 255, axis=1)))
            main = [lows[0], g[1], g[2], g[3], highs[0]]
            last = [lows[1], tail[1:2, :], tail[2:3, :], tail[3:4, :], highs[1]]
            origin = (cx * 3 + i) * 500 + cy
            for r in range(5):
                for h in range(2):
                    cols = slice(128 * h, 128 * h + 128)
                    at = origin + 4 * r + 2 * h
                    out[pl.ds(at, 24, stride=20), :] = main[r][:, cols]
                    out[pl.ds(at + 480, 1), :] = last[r][:, cols]
    for i in range(3):
        a = out[i * 500 + 400 : i * 500 + 500, :]
        b = out[(3 + i) * 500 : (3 + i) * 500 + 100, :]
        out[i * 500 + 400 : i * 500 + 500, :] = a + b
        out[(3 + i) * 500 : (3 + i) * 500 + 100, :] = a + b
    for c in range(6):
        for p in range(5):
            high = pl.ds(c * 500 + 100 * p + 80, 10, stride=2)
            low = pl.ds(c * 500 + 100 * p + 1, 10, stride=2)
            both = out[high, :] + out[low, :]
            out[high, :] = both
            out[low, :] = both
    for i in range(3):
        xlo[100 * i : 100 * i + 100, :] = out[i * 500 : i * 500 + 100, :]
        xhi[100 * i : 100 * i + 100, :] = out[(3 + i) * 500 + 400 : (3 + i) * 500 + 500, :]
    for c in range(6):
        for p in range(5):
            at = 50 * c + 10 * p
            ylo[at : at + 10, :] = out[pl.ds(c * 500 + 100 * p, 10, stride=2), :]
            yhi[at : at + 10, :] = out[pl.ds(c * 500 + 100 * p + 81, 10, stride=2), :]
    for cx in range(2):
        for cy in range(2):
            for i in range(3):
                start = (cx * 3 + i) * 500 + 400 * cx + 80 * cy + cy
                corner[2 * cx + cy, 10 * i : 10 * i + 10, :] = out[pl.ds(start, 10, stride=2), :]


def inject(big):
    vm = pl.BlockSpec(memory_space=pltpu.VMEM)
    face = jax.ShapeDtypeStruct((304, 128), F32)
    upper = np.triu(np.ones((128, 128), np.float32), 1)
    return pl.pallas_call(
        inject_kernel,
        name="inject",
        out_shape=(
            jax.ShapeDtypeStruct((3000, 128), F32),
            face, face, face, face,
            jax.ShapeDtypeStruct((4, 32, 128), F32),
        ),
        in_specs=[vm] * 4,
        out_specs=(vm,) * 6,
        scratch_shapes=[
            pltpu.VMEM((1536, 256), F32),
            pltpu.VMEM((4 * CHUNKS + 4, 8, 128), F32),
            pltpu.VMEM((16, 128), jnp.int32),
            pltpu.SMEM((16, 128), jnp.int32),
            pltpu.VMEM((4, 128, 128), jnp.int32),
            pltpu.VMEM((4, 128, 128), jnp.int32),
            pltpu.VMEM((2, 384, 512), BF16),
            pltpu.VMEM((2, 384, 512), BF16),
            pltpu.VMEM((8, 512), F32),
            pltpu.VMEM((8, 512), F32),
            pltpu.SemaphoreType.DMA(()),
        ],
        compiler_params=pltpu.CompilerParams(vmem_limit_bytes=32 * 2**20),
    )(big, jnp.asarray(basis_table(), F32), jnp.asarray(upper, BF16), jnp.asarray(upper.T, BF16))


SIDES = [(-1, 0), (1, 0), (0, -1), (0, 1), (-1, -1), (-1, 1), (1, -1), (1, 1)]


def there(side, gx, gy):
    ok = None
    for d, g, n in ((side[0], gx, NGX), (side[1], gy, NGY)):
        if d:
            c = (g + d >= 0) & (g + d < n)
            ok = c if ok is None else ok & c
    return ok


def halo_kernel(local, xlo, xhi, ylo, yhi, corner, out, gxlo, gxhi, gylo, gyhi, gcorner, ssem, rsem):
    gx = lax.axis_index("gx")
    gy = lax.axis_index("gy")
    bar = pltpu.get_barrier_semaphore()
    for side in SIDES:
        @pl.when(there(side, gx, gy))
        def _(side=side):
            pl.semaphore_signal(
                bar, inc=1, device_id=(gx + side[0], gy + side[1]), device_id_type=MESH
            )
    nx = (gx > 0).astype(jnp.int32) + (gx < NGX - 1).astype(jnp.int32)
    ny = (gy > 0).astype(jnp.int32) + (gy < NGY - 1).astype(jnp.int32)
    pl.semaphore_wait(bar, (nx + 1) * (ny + 1) - 1)

    src = [xlo, xhi, ylo, yhi] + [corner.at[k] for k in range(4)]
    dst = [gxhi, gxlo, gyhi, gylo] + [gcorner.at[3 - k] for k in range(4)]

    def copy(k):
        side = SIDES[k]
        return pltpu.make_async_remote_copy(
            src_ref=src[k],
            dst_ref=dst[k],
            send_sem=ssem.at[k],
            recv_sem=rsem.at[k],
            device_id=(gx + side[0], gy + side[1]),
            device_id_type=MESH,
        )

    for k in (2, 3, 4, 5, 6, 7, 0, 1):
        @pl.when(there(SIDES[k], gx, gy))
        def _(k=k):
            copy(k).start()
    out[...] = local[...]

    def take(k, add):
        @pl.when(there(SIDES[k], gx, gy))
        def _():
            copy([1, 0, 3, 2, 7, 6, 5, 4][k]).wait_recv()
            add()

    def add_xlo():
        for i in range(3):
            out[i * 500 : i * 500 + 100, :] += gxlo[100 * i : 100 * i + 100, :]

    def add_xhi():
        for i in range(3):
            out[(3 + i) * 500 + 400 : (3 + i) * 500 + 500, :] += gxhi[100 * i : 100 * i + 100, :]

    def add_y(ref, shift):
        for c in range(6):
            for p in range(5):
                k = 50 * c + 10 * p
                rows = pl.ds(c * 500 + 100 * p + shift, 10, stride=2)
                out[rows, :] += ref[k : k + 10, :]

    def add_corner(k):
        cx, cy = k // 2, k % 2
        for i in range(3):
            rows = pl.ds((cx * 3 + i) * 500 + 400 * cx + 80 * cy + cy, 10, stride=2)
            out[rows, :] += gcorner[k, 10 * i : 10 * i + 10, :]

    take(0, add_xlo)
    take(1, add_xhi)
    for k in range(4):
        take(4 + k, functools.partial(add_corner, k))
    take(2, lambda: add_y(gylo, 0))
    take(3, lambda: add_y(gyhi, 81))
    for k in range(8):
        @pl.when(there(SIDES[k], gx, gy))
        def _(k=k):
            copy(k).wait_send()


def halo(local, xlo, xhi, ylo, yhi, corner):
    vm = pl.BlockSpec(memory_space=pltpu.VMEM)
    return pl.pallas_call(
        halo_kernel,
        name="halo",
        out_shape=jax.ShapeDtypeStruct((3000, 128), F32),
        in_specs=[vm] * 6,
        out_specs=vm,
        scratch_shapes=[pltpu.VMEM((304, 128), F32)] * 4
        + [
            pltpu.VMEM((4, 32, 128), F32),
            pltpu.SemaphoreType.DMA((8,)),
            pltpu.SemaphoreType.DMA((8,)),
        ],
        compiler_params=pltpu.CompilerParams(
            collective_id=1, has_side_effects=True, vmem_limit_bytes=16 * 2**20
        ),
    )(local, xlo, xhi, ylo, yhi, corner)


def body(wavefield, moduli, residuals, coords, angles, element_ids, counts):
    wave = wavefield.reshape(2, 2, 3, 125, 2, 128).transpose(0, 2, 3, 4, 1, 5).reshape(3000, 128)
    big = exchange(
        residuals[0],
        coords[0].transpose(1, 0, 2),
        angles.reshape(256, 128),
        element_ids[0],
        counts,
        wave,
        moduli.reshape(4, 2, 256),
    )
    out = halo(*inject(big))
    out = out.reshape(2, 3, 125, 2, 2, 128).transpose(0, 4, 1, 2, 3, 5)
    return out.reshape(2, 2, 3, 125, 256)


def solution(mesh):
    in_specs = (
        P("gx", "gy", None, None, None),
        P("gx", "gy", None, None),
        P(("gx", "gy"), None, None),
        P(("gx", "gy"), None, None, None),
        P(("gx", "gy"), None, None, None),
        P(("gx", "gy"), None, None),
        P(("gx", "gy"), None),
    )
    out_specs = P("gx", "gy", None, None, None)
    return jax.shard_map(body, mesh=mesh, in_specs=in_specs, out_specs=out_specs, check_vma=False)
```

```python
import functools
import math

import jax
import jax.numpy as jnp
import numpy as np
from jax import lax
from jax.experimental import pallas as pl
from jax.experimental.pallas import tpu as pltpu
from jax.sharding import PartitionSpec as P

MESH = pl.DeviceIdType.MESH
F32 = jnp.float32
BF16 = jnp.bfloat16
NGX = 8
NGY = 16
NDEV = 128
CHUNKS = 136
TOT = 128
NST = 192
NT = (((1,), (1,)), ((), ()))
NN = (((1,), (0,)), ((), ()))


def gll_points():
    return np.array([-1.0, -math.sqrt(3.0 / 7.0), 0.0, math.sqrt(3.0 / 7.0), 1.0])


def gll_weights():
    return np.array([0.1, 49.0 / 90.0, 32.0 / 45.0, 49.0 / 90.0, 0.1])


def derivative_table():
    points = gll_points()
    table = np.zeros((5, 5))
    for row in range(5):
        for col in range(5):
            if row == col:
                table[row, col] = sum(
                    (1.0 / (points[col] - points[other]) for other in range(5) if other != col)
                )
            else:
                value = 1.0 / (points[col] - points[row])
                for other in range(5):
                    if other != col and other != row:
                        value = (
                            value * (points[row] - points[other]) / (points[col] - points[other])
                        )
                table[row, col] = value
    return table


def split_np(a):
    hi = np.asarray(a, np.float32).astype(jnp.bfloat16)
    lo = (np.asarray(a, np.float64) - hi.astype(np.float64)).astype(jnp.bfloat16)
    return hi, lo


def row_of(p, q, r):
    pq = 5 * p + q
    return 120 + r if pq == 24 else 24 * r + pq


def operators():
    table = np.asarray(derivative_table(), np.float32).astype(np.float64)
    weight = np.asarray(gll_weights(), np.float32).astype(np.float64)
    grad = np.zeros((3, 128, 128))
    back = np.zeros((3, 128, 128))
    for p in range(5):
        for q in range(5):
            for r in range(5):
                n = 25 * p + 5 * q + r
                for k in range(5):
                    grad[0, n, 25 * k + 5 * q + r] = table[p, k]
                    grad[1, n, 25 * p + 5 * k + r] = table[q, k]
                    grad[2, n, 25 * p + 5 * q + k] = table[r, k]
                w = weight[p] * weight[q] * weight[r]
                for k in range(5):
                    back[0, row_of(k, q, r), n] = -w * table[p, k]
                    back[1, row_of(p, k, r), n] = -w * table[q, k]
                    back[2, row_of(p, q, k), n] = -w * table[r, k]
    ghi, glo = split_np(grad.reshape(384, 128))
    flat = np.concatenate([back[0], back[1], back[2]], axis=1)
    bhi, blo = split_np(flat)
    return np.concatenate([ghi, glo, ghi], axis=1), np.concatenate([bhi, blo, bhi], axis=1)


def split(x):
    hi = x.astype(BF16)
    return hi, (x - hi.astype(F32)).astype(BF16)


def sin_cos(x):
    y = 0.5 * x
    z = y * y
    s = y * (
        1.0
        + z * (-1.0 / 6 + z * (1.0 / 120 + z * (-1.0 / 5040 + z * (1.0 / 362880 + z * (-1.0 / 39916800)))))
    )
    c = 1.0 + z * (
        -0.5
        + z
        * (1.0 / 24 + z * (-1.0 / 720 + z * (1.0 / 40320 + z * (-1.0 / 3628800 + z * (1.0 / 479001600)))))
    )
    return 2.0 * s * c, 1.0 - 2.0 * s * s


def far_first(j):
    return 2 + ((j + 1) // 2) * (1 - 2 * (j % 2))


def exchange_kernel(
    resid, coords, angles, ids, counts, wave, moduli, grad, back, upper,
    stage,
    fm, abuf, ibuf, cbuf, wbuf, mbuf, gbuf, bbuf, ubuf, recv, fl, pos_s,
    isem, wsem, bsem, ssem, rsem,
):
    gx = lax.axis_index("gx")
    gy = lax.axis_index("gy")
    me = gx * NGY + gy
    y, core, z, x = gx // 2, gx % 2, gy // 4, gy % 4
    loads = [
        pltpu.make_async_copy(resid, fm.at[0], isem.at[0]),
        pltpu.make_async_copy(coords, fm.at[pl.ds(1, 3)], isem.at[1]),
        pltpu.make_async_copy(angles, abuf, isem.at[2]),
        pltpu.make_async_copy(ids, ibuf, isem.at[3]),
        pltpu.make_async_copy(counts, cbuf, isem.at[4]),
    ]
    fetches = [
        pltpu.make_async_copy(a, b, wsem.at[k])
        for k, (a, b) in enumerate(
            ((wave, wbuf), (moduli, mbuf), (grad, gbuf), (back, bbuf), (upper, ubuf))
        )
    ]
    for load in loads + fetches:
        load.start()
    bar = pltpu.get_barrier_semaphore()
    for k in range(1, NGY):
        pl.semaphore_signal(bar, inc=1, device_id=(gx, (gy + k) % NGY), device_id_type=MESH)
    for k in range(1, NGX):
        pl.semaphore_signal(bar, inc=1, device_id=((gx + k) % NGX, gy), device_id_type=MESH)
    for load in loads:
        load.wait()
    fm[4] = abuf[pl.ds(0, 128, stride=2), :]
    fm[5] = abuf[pl.ds(1, 128, stride=2), :]
    limit = jnp.transpose(jnp.broadcast_to(cbuf[...].astype(F32), (128, 128)))
    slot = lax.broadcasted_iota(jnp.int32, (128, 128), 1).astype(F32)
    fm[6] = jnp.where(slot < limit, ibuf[...].astype(F32), -1.0)
    pl.semaphore_wait(bar, NGX + NGY - 2)
    for k in range(1, NGX):
        pl.semaphore_signal(bsem, inc=1, device_id=((gx + k) % NGX, gy), device_id_type=MESH)
    for f in range(7):
        recv[3, f, 31:32, :] = fm[f, pl.ds(me, 1), :]
    pl.semaphore_wait(bsem, NGX - 1)

    def send(j, last):
        ty = (y + far_first(j // 4)) % 4
        tz = (z + far_first(j % 4)) % 4
        for m in range(7 if last else 8):
            tx = (x + far_first(m // 2)) % 4
            tc = (core + 1 - m % 2) % 2
            t = (2 * ty + tc) * NGY + 4 * tz + tx
            pltpu.make_async_remote_copy(
                src_ref=fm.at[:, t, :],
                dst_ref=recv.at[j // 4, :, (j % 4) * 8 + m, :],
                send_sem=ssem,
                recv_sem=rsem.at[j // 4],
                device_id=(2 * ty + tc, 4 * tz + tx),
                device_id_type=MESH,
            ).start()

    def send_eight(j, carry):
        send(j, False)
        return carry

    lax.fori_loop(0, 15, send_eight, 0)
    send(15, True)
    for fetch in fetches:
        fetch.wait()

    def column(w, carry):
        cx = w // 2
        cy = w % 2
        lam = mbuf[w, 0:1, :]
        mu = mbuf[w, 1:2, :]
        grads = []
        for i in range(3):
            start = (cx * 3 + i) * 500 + cy
            u = jnp.concatenate(
                [wbuf[pl.ds(start + 2 * h, 125, stride=4), :] for h in range(2)], axis=1
            )
            u = jnp.concatenate([u, jnp.zeros((3, 256), F32)], axis=0)
            hi, lo = split(u)
            grads.append(
                lax.dot_general(
                    gbuf[...],
                    jnp.concatenate([hi, hi, lo], axis=0),
                    NN,
                    preferred_element_type=F32,
                )
            )
        g = [[grads[i][128 * j : 128 * j + 128] for j in range(3)] for i in range(3)]
        ldiv = lam * (g[0][0] + g[1][1] + g[2][2])
        parts = {}
        for i in range(3):
            for j in range(i, 3):
                s = mu * (g[i][j] + g[j][i])
                if i == j:
                    s = s + ldiv
                parts[(i, j)] = parts[(j, i)] = split(s)
        for i in range(3):
            hi = [parts[(i, j)][0] for j in range(3)]
            lo = [parts[(i, j)][1] for j in range(3)]
            got = lax.dot_general(
                bbuf[...],
                jnp.concatenate(hi + hi + lo, axis=0),
                NN,
                preferred_element_type=F32,
            )
            for h in range(2):
                at = NST + 192 * h + 48 * w + 16 * i
                stage[pl.ds(at, 16)] = got[:, 128 * h : 128 * h + 128].reshape(16, 8, 128)
        return carry

    lax.fori_loop(0, 4, column, 0)
    up = ubuf[...]
    ones = jnp.ones((128, 128), BF16)
    lane_row = lax.broadcasted_iota(jnp.int32, (128, 128), 0).astype(F32)

    def waiter(ref, group):
        return pltpu.make_async_remote_copy(
            src_ref=ref,
            dst_ref=ref,
            send_sem=ssem,
            recv_sem=rsem.at[group],
            device_id=(gx, (gy + 1) % NGY),
            device_id_type=MESH,
        )

    def prepare(g):
        sin_a, cos_a = sin_cos(recv[g, 4])
        sin_d, cos_d = sin_cos(recv[g, 5])
        num = recv[g, 6]
        colf = jnp.floor(num * (1.0 / 256.0))
        for k in range(4):
            fl[32 * k : 32 * k + 32, :] = recv[g, k]
        fl[128:160, :] = cos_a * cos_d
        fl[160:192, :] = sin_a * cos_d
        fl[192:224, :] = sin_d
        fl[224:256, :] = num - 256.0 * colf
        stacked = jnp.concatenate(
            [(colf == float(w)).astype(F32).astype(BF16) for w in range(4)], axis=0
        )
        prefix = lax.dot_general(stacked, up, NN, preferred_element_type=F32)
        total = lax.dot_general(stacked, ones, NN, preferred_element_type=F32)
        start = jnp.zeros((32, 128), F32)
        pos = jnp.full((32, 128), -1.0, F32)
        for w in range(4):
            n = total[32 * w : 32 * w + 32]
            stage[pl.ds(TOT + 16 * w + 4 * g, 4)] = n.reshape(4, 8, 128)
            pos = jnp.where(colf == float(w), prefix[32 * w : 32 * w + 32] + start, pos)
            start = start + n
        pos_s[...] = pos

        def sort_some(h, carry):
            for k in range(16):
                t = h * 16 + k
                f = fl[pl.ds(t, 8, stride=32), :]
                hi = f.astype(BF16).astype(F32)
                mid = (f - hi).astype(BF16).astype(F32)
                lo = f - hi - mid
                perm = jnp.where(lane_row == pos_s[pl.ds(t, 1), :], 1.0, 0.0).astype(BF16)
                got = lax.dot_general(
                    jnp.concatenate([hi, mid, lo], axis=0).astype(BF16),
                    perm,
                    NT,
                    preferred_element_type=F32,
                )
                stage[g * 32 + t] = got[0:8] + got[8:16] + got[16:24]
            return carry

        lax.fori_loop(0, 2, sort_some, 0)

    def group(g, carry):
        waiter(recv.at[g], g).wait_recv()
        prepare(g)
        return carry

    lax.fori_loop(0, 3, group, 0)
    waiter(recv.at[3, :, pl.ds(0, 31), :], 3).wait_recv()
    prepare(3)
    waiter(fm.at[:, pl.ds(0, 127), :], 0).wait_send()


def exchange(resid, coords, angles, ids, counts, wave, moduli):
    grad, back = operators()
    upper = np.triu(np.ones((128, 128), np.float32), 1)
    return pl.pallas_call(
        exchange_kernel,
        name="exchange",
        out_shape=pltpu.VMEM((576, 8, 128), F32),
        in_specs=[pl.BlockSpec(memory_space=pltpu.HBM)] * 10,
        out_specs=pl.BlockSpec(memory_space=pltpu.VMEM),
        scratch_shapes=[
            pltpu.VMEM((7, 128, 128), F32),
            pltpu.VMEM((256, 128), F32),
            pltpu.VMEM((128, 128), jnp.int32),
            pltpu.VMEM((1, 128), jnp.int32),
            pltpu.VMEM((3000, 128), F32),
            pltpu.VMEM((4, 2, 256), F32),
            pltpu.VMEM((384, 384), BF16),
            pltpu.VMEM((128, 1152), BF16),
            pltpu.VMEM((128, 128), BF16),
            pltpu.VMEM((4, 7, 32, 128), F32),
            pltpu.VMEM((256, 128), F32),
            pltpu.VMEM((32, 128), F32),
            pltpu.SemaphoreType.DMA((5,)),
            pltpu.SemaphoreType.DMA((5,)),
            pltpu.SemaphoreType.REGULAR,
            pltpu.SemaphoreType.DMA(()),
            pltpu.SemaphoreType.DMA((4,)),
        ],
        compiler_params=pltpu.CompilerParams(
            collective_id=0, has_side_effects=True, vmem_limit_bytes=32 * 2**20
        ),
    )(
        *[
            pltpu.with_memory_space_constraint(a, pltpu.HBM)
            for a in (
                resid, coords, angles, ids, counts, wave, moduli,
                jnp.asarray(grad), jnp.asarray(back), jnp.asarray(upper, BF16),
            )
        ]
    )


def node_coefficients():
    points = gll_points()
    poly = np.zeros((5, 5))
    for node in range(5):
        c = np.array([1.0])
        for other in range(5):
            if other != node:
                c = np.convolve(c, np.array([-points[other], 1.0])) / (points[node] - points[other])
        poly[node] = c
    slope = poly[:, 1:] * np.arange(1, 5)[None, :]
    every = np.concatenate([poly, slope], axis=1)
    blocks = []
    for m in range(9):
        blocks.append(np.concatenate([every[:, m], np.zeros(3)]))
    for t in range(3):
        for m in range(9):
            blocks.append(every[(8 * t + np.arange(8)) % 5, m])
    return np.repeat(np.concatenate(blocks)[:, None], 128, axis=1)


def fill_lanes(win, at, coef, temp, lhs, k, h):
    def across(f):
        return win[at, pl.ds(f, 8, stride=0), :]

    def basis(x, block):
        c = [coef[8 * (block + m) : 8 * (block + m) + 8, :] for m in range(9)]
        val = (((c[4] * x + c[3]) * x + c[2]) * x + c[1]) * x + c[0]
        der = ((c[8] * x + c[7]) * x + c[6]) * x + c[5]
        return val, der

    vx, dx = basis(across(1), 0)
    vz, dz = basis(across(3), 0)
    eta = across(2)
    t = [across(4 + i) for i in range(3)]
    d = [across(0) * t[i] for i in range(3)]
    temp[0:8, :] = dx * t[0]
    temp[8:16, :] = vx * t[1]
    temp[16:24, :] = vx * t[2]
    temp[24:32, :] = vz
    temp[32:40, :] = dz

    def row(block, node):
        return temp[pl.ds(8 * block + node, 8, stride=0), :]

    sub = lax.broadcasted_iota(jnp.int32, (8, 128), 0)

    def by_p(block, tile):
        if tile == 0:
            return jnp.where(sub < 5, row(block, 0), row(block, 1))
        if tile == 1:
            return jnp.where(sub < 2, row(block, 1), jnp.where(sub < 7, row(block, 2), row(block, 3)))
        return jnp.where(sub < 4, row(block, 3), row(block, 4))

    a, b = [], []
    for tile in range(3):
        vy, dy = basis(eta, 9 + 9 * tile)
        a.append(by_p(0, tile) * vy + by_p(1, tile) * dy)
        b.append(by_p(2, tile) * vy)
        if tile == 0:
            vy4, dy4 = vy[4:5, :], dy[4:5, :]

    def shape(j):
        if j < 15:
            return a[j % 3] * row(3, j // 3) + b[j % 3] * row(4, j // 3)
        a4 = row(0, 4) * vy4 + row(1, 4) * dy4
        b4 = row(2, 4) * vy4
        return a4 * vz + b4 * dz

    for j in range(16):
        temp[40 + 8 * j : 48 + 8 * j, :] = shape(j)
    shapes = temp[40:168, :].reshape(16, 8, 128)
    for i in range(3):
        hi, lo = split((shapes * d[i][None]).reshape(128, 128))
        lhs[k, h, 128 * i : 128 * i + 128, :] = hi
        lhs[k, 2 + h, 128 * i : 128 * i + 128, :] = lo


def inject_kernel(
    big, coef_ref, upper, lower, out, xlo, xhi, ylo, yhi, corner,
    acc, win, tabv, tabs, begin, end, lhs_a, lhs_b, num_a, num_b, temp, tsem,
):
    up = upper[...]
    down = lower[...]
    sub = lax.broadcasted_iota(jnp.int32, (16, 128), 0)
    lane16 = lax.broadcasted_iota(jnp.int32, (16, 128), 1)
    pick = jnp.where(lane16 == 0, 1.0, 0.0).astype(BF16)
    table = jnp.zeros((16, 128), jnp.int32)
    first = jnp.zeros((16, 128), jnp.int32)
    for w in range(4):
        n_rows = big[TOT + 16 * w : TOT + 16 * w + 16].reshape(128, 128)
        n_bf = n_rows.astype(BF16)
        n = lax.dot_general(pick, n_bf, NT, preferred_element_type=F32)
        fill = lax.dot_general(n.astype(BF16), up, NN, preferred_element_type=F32)
        n = n.astype(jnp.int32)
        fill = fill.astype(jnp.int32)
        word = ((fill >> 7) + CHUNKS * w) * 128 + ((fill - first) & 127)
        table = jnp.where(sub == w, word, table)
        table = jnp.where(sub == 4 + w, fill + n, table)
        first = first + n
        at = lax.dot_general(down, n_bf, NN, preferred_element_type=F32).astype(jnp.int32) & 127
        begin[w] = at
        end[w] = at + n_rows.astype(jnp.int32)
    tabv[...] = table
    totab = pltpu.make_async_copy(tabv, tabs, tsem)
    totab.start()
    totab.wait()

    lane = lax.broadcasted_iota(jnp.int32, (8, 128), 1)
    zero = jnp.zeros((8, 128), F32)

    def place(step, cur):
        for h in range(2):
            part = big[pl.ds(NST + 192 * h + 6 * step, 6)].reshape(48, 128)
            acc[pl.ds(step * 48, 48), 128 * h : 128 * h + 128] = part
        for k in range(4):
            t = step * 4 + k
            tile = big[t]
            new = []
            for w in range(4):
                b = jnp.broadcast_to(begin[w, pl.ds(t, 1), :], (8, 128))
                e = jnp.broadcast_to(end[w, pl.ds(t, 1), :], (8, 128))
                word = tabs[w, t]
                chunk = word >> 7
                rolled = pltpu.roll(tile, word & 127, axis=1)
                low = jnp.where(lane < b, cur[w], jnp.where(lane < e, rolled, zero))
                high = jnp.where(lane + 128 < e, rolled, zero)
                win[chunk] = low
                win[chunk + 1] = high
                new.append(jnp.where(e >= 128, high, low))
            cur = tuple(new)
        return cur

    lax.fori_loop(0, 32, place, (zero,) * 4)
    row = lax.broadcasted_iota(jnp.int32, (256, 128), 0).astype(F32).astype(BF16)
    upto = [0]
    for w in range(4):
        count = tabs[4 + w, 127]
        for k in range(3):
            win[CHUNKS * w + (count + 127) // 128 + k] = zero
        upto.append(upto[-1] + (count + 511) // 512)
    for k in range(4):
        win[4 * CHUNKS + k] = zero

    def which(u):
        w = jnp.int32(0)
        at = u * 4
        for k in range(1, 4):
            past = u >= upto[k]
            w = jnp.where(past, k, w)
            at = jnp.where(past, CHUNKS * k + (u - upto[k]) * 4, at)
        done = u >= upto[4]
        return jnp.where(done, 0, w), jnp.where(done, 4 * CHUNKS, at)

    def fill_unit(u, lhs, num):
        _, at = which(u)
        for k in range(2):
            for h in range(2):
                c = at + 2 * k + h
                fill_lanes(win, c, coef_ref, temp.at[2 * k + h], lhs, k, h)
                part = slice(256 * k + 128 * h, 256 * k + 128 * h + 128)
                want = jnp.concatenate([win[c, pl.ds(7, 8, stride=0), :]] * 2, axis=0).astype(BF16)
                want = jnp.broadcast_to(want[0:1], (256, 128))
                num[k, h] = jnp.where(row == want, jnp.ones((), BF16), jnp.zeros((), BF16))

    def use_unit(u, lhs, num):
        w, _ = which(u)
        part = pl.ds(pl.multiple_of(w * 384, 384), 384)
        total = None
        for k in range(2):
            onehot = [num[k, 0], num[k, 1]]
            got = lax.dot_general(
                jnp.concatenate([lhs[k, j] for j in range(4)], axis=1),
                jnp.concatenate(onehot + onehot, axis=1),
                NT,
                preferred_element_type=F32,
            )
            total = got if total is None else total + got
        acc[part, :] += total

    fill_unit(0, lhs_a, num_a)

    def two_units(step, carry):
        u = 2 * step
        use_unit(u, lhs_a, num_a)
        fill_unit(u + 1, lhs_b, num_b)
        use_unit(u + 1, lhs_b, num_b)
        fill_unit(u + 2, lhs_a, num_a)
        return carry

    lax.fori_loop(0, (upto[4] + 1) // 2, two_units, 0)

    lane2 = lax.broadcasted_iota(jnp.int32, (8, 256), 1)
    for w in range(4):
        cx, cy = w // 2, w % 2
        for i in range(3):
            base = 384 * w + 128 * i
            g = [acc[base + 24 * r : base + 24 * r + 24, :] for r in range(5)]
            tail = acc[base + 120 : base + 128, :]
            groups = [g[0], tail[0:1, :]], [g[4], tail[4:5, :]]
            lows, highs = [], []
            for a, b in zip(*groups):
                ln = lax.broadcasted_iota(jnp.int32, a.shape, 1)
                lows.append(a + jnp.where(ln == 0, 0.0, pltpu.roll(b, 1, axis=1)))
                highs.append(b + jnp.where(ln == 255, 0.0, pltpu.roll(a, 255, axis=1)))
            main = [lows[0], g[1], g[2], g[3], highs[0]]
            last = [lows[1], tail[1:2, :], tail[2:3, :], tail[3:4, :], highs[1]]
            origin = (cx * 3 + i) * 500 + cy
            for r in range(5):
                for h in range(2):
                    cols = slice(128 * h, 128 * h + 128)
                    at = origin + 4 * r + 2 * h
                    out[pl.ds(at, 24, stride=20), :] = main[r][:, cols]
                    out[pl.ds(at + 480, 1), :] = last[r][:, cols]
    for i in range(3):
        a = out[i * 500 + 400 : i * 500 + 500, :]
        b = out[(3 + i) * 500 : (3 + i) * 500 + 100, :]
        out[i * 500 + 400 : i * 500 + 500, :] = a + b
        out[(3 + i) * 500 : (3 + i) * 500 + 100, :] = a + b
    for c in range(6):
        for p in range(5):
            high = pl.ds(c * 500 + 100 * p + 80, 10, stride=2)
            low = pl.ds(c * 500 + 100 * p + 1, 10, stride=2)
            both = out[high, :] + out[low, :]
            out[high, :] = both
            out[low, :] = both
    for i in range(3):
        xlo[100 * i : 100 * i + 100, :] = out[i * 500 : i * 500 + 100, :]
        xhi[100 * i : 100 * i + 100, :] = out[(3 + i) * 500 + 400 : (3 + i) * 500 + 500, :]
    for c in range(6):
        for p in range(5):
            at = 50 * c + 10 * p
            ylo[at : at + 10, :] = out[pl.ds(c * 500 + 100 * p, 10, stride=2), :]
            yhi[at : at + 10, :] = out[pl.ds(c * 500 + 100 * p + 81, 10, stride=2), :]
    for cx in range(2):
        for cy in range(2):
            for i in range(3):
                start = (cx * 3 + i) * 500 + 400 * cx + 80 * cy + cy
                corner[2 * cx + cy, 10 * i : 10 * i + 10, :] = out[pl.ds(start, 10, stride=2), :]


def inject(big):
    vm = pl.BlockSpec(memory_space=pltpu.VMEM)
    face = jax.ShapeDtypeStruct((304, 128), F32)
    upper = np.triu(np.ones((128, 128), np.float32), 1)
    return pl.pallas_call(
        inject_kernel,
        name="inject",
        out_shape=(
            jax.ShapeDtypeStruct((3000, 128), F32),
            face, face, face, face,
            jax.ShapeDtypeStruct((4, 32, 128), F32),
        ),
        in_specs=[vm] * 4,
        out_specs=(vm,) * 6,
        scratch_shapes=[
            pltpu.VMEM((1536, 256), F32),
            pltpu.VMEM((4 * CHUNKS + 4, 8, 128), F32),
            pltpu.VMEM((16, 128), jnp.int32),
            pltpu.SMEM((16, 128), jnp.int32),
            pltpu.VMEM((4, 128, 128), jnp.int32),
            pltpu.VMEM((4, 128, 128), jnp.int32),
            pltpu.VMEM((2, 4, 384, 128), BF16),
            pltpu.VMEM((2, 4, 384, 128), BF16),
            pltpu.VMEM((2, 2, 256, 128), BF16),
            pltpu.VMEM((2, 2, 256, 128), BF16),
            pltpu.VMEM((4, 168, 128), F32),
            pltpu.SemaphoreType.DMA(()),
        ],
        compiler_params=pltpu.CompilerParams(vmem_limit_bytes=32 * 2**20),
    )(big, jnp.asarray(node_coefficients(), F32), jnp.asarray(upper, BF16), jnp.asarray(upper.T, BF16))


SIDES = [(-1, 0), (1, 0), (0, -1), (0, 1), (-1, -1), (-1, 1), (1, -1), (1, 1)]


def there(side, gx, gy):
    ok = None
    for d, g, n in ((side[0], gx, NGX), (side[1], gy, NGY)):
        if d:
            c = (g + d >= 0) & (g + d < n)
            ok = c if ok is None else ok & c
    return ok


def halo_kernel(local, xlo, xhi, ylo, yhi, corner, out, gxlo, gxhi, gylo, gyhi, gcorner, ssem, rsem):
    gx = lax.axis_index("gx")
    gy = lax.axis_index("gy")
    bar = pltpu.get_barrier_semaphore()
    for side in SIDES:
        @pl.when(there(side, gx, gy))
        def _(side=side):
            pl.semaphore_signal(
                bar, inc=1, device_id=(gx + side[0], gy + side[1]), device_id_type=MESH
            )
    nx = (gx > 0).astype(jnp.int32) + (gx < NGX - 1).astype(jnp.int32)
    ny = (gy > 0).astype(jnp.int32) + (gy < NGY - 1).astype(jnp.int32)
    pl.semaphore_wait(bar, (nx + 1) * (ny + 1) - 1)

    src = [xlo, xhi, ylo, yhi] + [corner.at[k] for k in range(4)]
    dst = [gxhi, gxlo, gyhi, gylo] + [gcorner.at[3 - k] for k in range(4)]

    def copy(k):
        side = SIDES[k]
        return pltpu.make_async_remote_copy(
            src_ref=src[k],
            dst_ref=dst[k],
            send_sem=ssem.at[k],
            recv_sem=rsem.at[k],
            device_id=(gx + side[0], gy + side[1]),
            device_id_type=MESH,
        )

    for k in (2, 3, 4, 5, 6, 7, 0, 1):
        @pl.when(there(SIDES[k], gx, gy))
        def _(k=k):
            copy(k).start()
    out[...] = local[...]

    def take(k, add):
        @pl.when(there(SIDES[k], gx, gy))
        def _():
            copy([1, 0, 3, 2, 7, 6, 5, 4][k]).wait_recv()
            add()

    def add_xlo():
        for i in range(3):
            out[i * 500 : i * 500 + 100, :] += gxlo[100 * i : 100 * i + 100, :]

    def add_xhi():
        for i in range(3):
            out[(3 + i) * 500 + 400 : (3 + i) * 500 + 500, :] += gxhi[100 * i : 100 * i + 100, :]

    def add_y(ref, shift):
        for c in range(6):
            for p in range(5):
                k = 50 * c + 10 * p
                rows = pl.ds(c * 500 + 100 * p + shift, 10, stride=2)
                out[rows, :] += ref[k : k + 10, :]

    def add_corner(k):
        cx, cy = k // 2, k % 2
        for i in range(3):
            rows = pl.ds((cx * 3 + i) * 500 + 400 * cx + 80 * cy + cy, 10, stride=2)
            out[rows, :] += gcorner[k, 10 * i : 10 * i + 10, :]

    take(0, add_xlo)
    take(1, add_xhi)
    for k in range(4):
        take(4 + k, functools.partial(add_corner, k))
    take(2, lambda: add_y(gylo, 0))
    take(3, lambda: add_y(gyhi, 81))
    for k in range(8):
        @pl.when(there(SIDES[k], gx, gy))
        def _(k=k):
            copy(k).wait_send()


def halo(local, xlo, xhi, ylo, yhi, corner):
    vm = pl.BlockSpec(memory_space=pltpu.VMEM)
    return pl.pallas_call(
        halo_kernel,
        name="halo",
        out_shape=jax.ShapeDtypeStruct((3000, 128), F32),
        in_specs=[vm] * 6,
        out_specs=vm,
        scratch_shapes=[pltpu.VMEM((304, 128), F32)] * 4
        + [
            pltpu.VMEM((4, 32, 128), F32),
            pltpu.SemaphoreType.DMA((8,)),
            pltpu.SemaphoreType.DMA((8,)),
        ],
        compiler_params=pltpu.CompilerParams(
            collective_id=1, has_side_effects=True, vmem_limit_bytes=16 * 2**20
        ),
    )(local, xlo, xhi, ylo, yhi, corner)


def body(wavefield, moduli, residuals, coords, angles, element_ids, counts):
    wave = wavefield.reshape(2, 2, 3, 125, 2, 128).transpose(0, 2, 3, 4, 1, 5).reshape(3000, 128)
    big = exchange(
        residuals[0],
        coords[0].transpose(1, 0, 2),
        angles.reshape(256, 128),
        element_ids[0],
        counts,
        wave,
        moduli.reshape(4, 2, 256),
    )
    out = halo(*inject(big))
    out = out.reshape(2, 3, 125, 2, 2, 128).transpose(0, 4, 1, 2, 3, 5)
    return out.reshape(2, 2, 3, 125, 256)


def solution(mesh):
    in_specs = (
        P("gx", "gy", None, None, None),
        P("gx", "gy", None, None),
        P(("gx", "gy"), None, None),
        P(("gx", "gy"), None, None, None),
        P(("gx", "gy"), None, None, None),
        P(("gx", "gy"), None, None),
        P(("gx", "gy"), None),
    )
    out_specs = P("gx", "gy", None, None, None)
    return jax.shard_map(body, mesh=mesh, in_specs=in_specs, out_specs=out_specs, check_vma=False)
```

```python
import functools
import math

import jax
import jax.numpy as jnp
import numpy as np
from jax import lax
from jax.experimental import pallas as pl
from jax.experimental.pallas import tpu as pltpu
from jax.sharding import PartitionSpec as P

MESH = pl.DeviceIdType.MESH
F32 = jnp.float32
BF16 = jnp.bfloat16
NGX = 8
NGY = 16
NDEV = 128
CHUNKS = 136
TOT = 128
NST = 192
NT = (((1,), (1,)), ((), ()))
NN = (((1,), (0,)), ((), ()))


def gll_points():
    return np.array([-1.0, -math.sqrt(3.0 / 7.0), 0.0, math.sqrt(3.0 / 7.0), 1.0])


def gll_weights():
    return np.array([0.1, 49.0 / 90.0, 32.0 / 45.0, 49.0 / 90.0, 0.1])


def derivative_table():
    points = gll_points()
    table = np.zeros((5, 5))
    for row in range(5):
        for col in range(5):
            if row == col:
                table[row, col] = sum(
                    (1.0 / (points[col] - points[other]) for other in range(5) if other != col)
                )
            else:
                value = 1.0 / (points[col] - points[row])
                for other in range(5):
                    if other != col and other != row:
                        value = (
                            value * (points[row] - points[other]) / (points[col] - points[other])
                        )
                table[row, col] = value
    return table


def split_np(a):
    hi = np.asarray(a, np.float32).astype(jnp.bfloat16)
    lo = (np.asarray(a, np.float64) - hi.astype(np.float64)).astype(jnp.bfloat16)
    return hi, lo


def row_of(p, q, r):
    pq = 5 * p + q
    return 120 + r if pq == 24 else 24 * r + pq


def operators():
    table = np.asarray(derivative_table(), np.float32).astype(np.float64)
    weight = np.asarray(gll_weights(), np.float32).astype(np.float64)
    grad = np.zeros((3, 128, 128))
    back = np.zeros((3, 128, 128))
    for p in range(5):
        for q in range(5):
            for r in range(5):
                n = 25 * p + 5 * q + r
                for k in range(5):
                    grad[0, n, 25 * k + 5 * q + r] = table[p, k]
                    grad[1, n, 25 * p + 5 * k + r] = table[q, k]
                    grad[2, n, 25 * p + 5 * q + k] = table[r, k]
                w = weight[p] * weight[q] * weight[r]
                for k in range(5):
                    back[0, row_of(k, q, r), n] = -w * table[p, k]
                    back[1, row_of(p, k, r), n] = -w * table[q, k]
                    back[2, row_of(p, q, k), n] = -w * table[r, k]
    ghi, glo = split_np(grad.reshape(384, 128))
    flat = np.concatenate([back[0], back[1], back[2]], axis=1)
    bhi, blo = split_np(flat)
    return np.concatenate([ghi, glo, ghi], axis=1), np.concatenate([bhi, blo, bhi], axis=1)


def split(x):
    hi = x.astype(BF16)
    return hi, (x - hi.astype(F32)).astype(BF16)


def sin_cos(x):
    y = 0.5 * x
    z = y * y
    s = y * (
        1.0
        + z * (-1.0 / 6 + z * (1.0 / 120 + z * (-1.0 / 5040 + z * (1.0 / 362880 + z * (-1.0 / 39916800)))))
    )
    c = 1.0 + z * (
        -0.5
        + z
        * (1.0 / 24 + z * (-1.0 / 720 + z * (1.0 / 40320 + z * (-1.0 / 3628800 + z * (1.0 / 479001600)))))
    )
    return 2.0 * s * c, 1.0 - 2.0 * s * s


def far_first(j):
    return 2 + ((j + 1) // 2) * (1 - 2 * (j % 2))


def exchange_kernel(
    resid, coords, angles, ids, counts, wave, moduli, grad, back, upper, lower,
    stage, table, begin, end,
    fm, abuf, ibuf, cbuf, wbuf, mbuf, gbuf, bbuf, ubuf, dbuf, recv, fl, pos_s,
    isem, wsem, bsem, ssem, rsem,
):
    gx = lax.axis_index("gx")
    gy = lax.axis_index("gy")
    me = gx * NGY + gy
    y, core, z, x = gx // 2, gx % 2, gy // 4, gy % 4
    loads = [
        pltpu.make_async_copy(resid, fm.at[0], isem.at[0]),
        pltpu.make_async_copy(coords, fm.at[pl.ds(1, 3)], isem.at[1]),
        pltpu.make_async_copy(angles, abuf, isem.at[2]),
        pltpu.make_async_copy(ids, ibuf, isem.at[3]),
        pltpu.make_async_copy(counts, cbuf, isem.at[4]),
    ]
    fetches = [
        pltpu.make_async_copy(a, b, wsem.at[k])
        for k, (a, b) in enumerate(
            ((wave, wbuf), (moduli, mbuf), (grad, gbuf), (back, bbuf), (upper, ubuf), (lower, dbuf))
        )
    ]
    for load in loads + fetches:
        load.start()
    bar = pltpu.get_barrier_semaphore()
    for k in range(1, NGY):
        pl.semaphore_signal(bar, inc=1, device_id=(gx, (gy + k) % NGY), device_id_type=MESH)
    for k in range(1, NGX):
        pl.semaphore_signal(bar, inc=1, device_id=((gx + k) % NGX, gy), device_id_type=MESH)
    for load in loads:
        load.wait()
    fm[4] = abuf[pl.ds(0, 128, stride=2), :]
    fm[5] = abuf[pl.ds(1, 128, stride=2), :]
    limit = jnp.transpose(jnp.broadcast_to(cbuf[...].astype(F32), (128, 128)))
    slot = lax.broadcasted_iota(jnp.int32, (128, 128), 1).astype(F32)
    fm[6] = jnp.where(slot < limit, ibuf[...].astype(F32), -1.0)
    pl.semaphore_wait(bar, NGX + NGY - 2)
    for k in range(1, NGX):
        pl.semaphore_signal(bsem, inc=1, device_id=((gx + k) % NGX, gy), device_id_type=MESH)
    for f in range(7):
        recv[3, f, 31:32, :] = fm[f, pl.ds(me, 1), :]
    pl.semaphore_wait(bsem, NGX - 1)

    def send(j, last):
        ty = (y + far_first(j // 4)) % 4
        tz = (z + far_first(j % 4)) % 4
        for m in range(7 if last else 8):
            tx = (x + far_first(m // 2)) % 4
            tc = (core + 1 - m % 2) % 2
            t = (2 * ty + tc) * NGY + 4 * tz + tx
            pltpu.make_async_remote_copy(
                src_ref=fm.at[:, t, :],
                dst_ref=recv.at[j // 4, :, (j % 4) * 8 + m, :],
                send_sem=ssem,
                recv_sem=rsem.at[j // 4],
                device_id=(2 * ty + tc, 4 * tz + tx),
                device_id_type=MESH,
            ).start()

    def send_eight(j, carry):
        send(j, False)
        return carry

    lax.fori_loop(0, 15, send_eight, 0)
    send(15, True)
    for fetch in fetches:
        fetch.wait()

    def column(w, carry):
        cx = w // 2
        cy = w % 2
        lam = mbuf[w, 0:1, :]
        mu = mbuf[w, 1:2, :]
        grads = []
        for i in range(3):
            start = (cx * 3 + i) * 500 + cy
            u = jnp.concatenate(
                [wbuf[pl.ds(start + 2 * h, 125, stride=4), :] for h in range(2)], axis=1
            )
            u = jnp.concatenate([u, jnp.zeros((3, 256), F32)], axis=0)
            hi, lo = split(u)
            grads.append(
                lax.dot_general(
                    gbuf[...],
                    jnp.concatenate([hi, hi, lo], axis=0),
                    NN,
                    preferred_element_type=F32,
                )
            )
        g = [[grads[i][128 * j : 128 * j + 128] for j in range(3)] for i in range(3)]
        ldiv = lam * (g[0][0] + g[1][1] + g[2][2])
        parts = {}
        for i in range(3):
            for j in range(i, 3):
                s = mu * (g[i][j] + g[j][i])
                if i == j:
                    s = s + ldiv
                parts[(i, j)] = parts[(j, i)] = split(s)
        for i in range(3):
            hi = [parts[(i, j)][0] for j in range(3)]
            lo = [parts[(i, j)][1] for j in range(3)]
            got = lax.dot_general(
                bbuf[...],
                jnp.concatenate(hi + hi + lo, axis=0),
                NN,
                preferred_element_type=F32,
            )
            for h in range(2):
                at = NST + 192 * h + 48 * w + 16 * i
                stage[pl.ds(at, 16)] = got[:, 128 * h : 128 * h + 128].reshape(16, 8, 128)
        return carry

    lax.fori_loop(0, 4, column, 0)
    up = ubuf[...]
    ones = jnp.ones((128, 128), BF16)
    lane_row = lax.broadcasted_iota(jnp.int32, (128, 128), 0).astype(F32)

    def waiter(ref, group):
        return pltpu.make_async_remote_copy(
            src_ref=ref,
            dst_ref=ref,
            send_sem=ssem,
            recv_sem=rsem.at[group],
            device_id=(gx, (gy + 1) % NGY),
            device_id_type=MESH,
        )

    def prepare(g):
        sin_a, cos_a = sin_cos(recv[g, 4])
        sin_d, cos_d = sin_cos(recv[g, 5])
        num = recv[g, 6]
        colf = jnp.floor(num * (1.0 / 256.0))
        for k in range(4):
            fl[32 * k : 32 * k + 32, :] = recv[g, k]
        fl[128:160, :] = cos_a * cos_d
        fl[160:192, :] = sin_a * cos_d
        fl[192:224, :] = sin_d
        fl[224:256, :] = num - 256.0 * colf
        stacked = jnp.concatenate(
            [(colf == float(w)).astype(F32).astype(BF16) for w in range(4)], axis=0
        )
        prefix = lax.dot_general(stacked, up, NN, preferred_element_type=F32)
        total = lax.dot_general(stacked, ones, NN, preferred_element_type=F32)
        start = jnp.zeros((32, 128), F32)
        pos = jnp.full((32, 128), -1.0, F32)
        for w in range(4):
            n = total[32 * w : 32 * w + 32]
            stage[pl.ds(TOT + 16 * w + 4 * g, 4)] = n.reshape(4, 8, 128)
            pos = jnp.where(colf == float(w), prefix[32 * w : 32 * w + 32] + start, pos)
            start = start + n
        pos_s[...] = pos

        def sort_some(h, carry):
            for k in range(16):
                t = h * 16 + k
                f = fl[pl.ds(t, 8, stride=32), :]
                hi = f.astype(BF16).astype(F32)
                mid = (f - hi).astype(BF16).astype(F32)
                lo = f - hi - mid
                perm = jnp.where(lane_row == pos_s[pl.ds(t, 1), :], 1.0, 0.0).astype(BF16)
                got = lax.dot_general(
                    jnp.concatenate([hi, mid, lo], axis=0).astype(BF16),
                    perm,
                    NT,
                    preferred_element_type=F32,
                )
                stage[g * 32 + t] = got[0:8] + got[8:16] + got[16:24]
            return carry

        lax.fori_loop(0, 2, sort_some, 0)

    def group(g, carry):
        waiter(recv.at[g], g).wait_recv()
        prepare(g)
        return carry

    lax.fori_loop(0, 3, group, 0)
    waiter(recv.at[3, :, pl.ds(0, 31), :], 3).wait_recv()
    prepare(3)
    down = dbuf[...]
    sub = lax.broadcasted_iota(jnp.int32, (16, 128), 0)
    lane16 = lax.broadcasted_iota(jnp.int32, (16, 128), 1)
    pick = jnp.where(lane16 == 0, 1.0, 0.0).astype(BF16)
    words = jnp.zeros((16, 128), jnp.int32)
    first = jnp.zeros((16, 128), jnp.int32)
    for w in range(4):
        n_rows = stage[TOT + 16 * w : TOT + 16 * w + 16].reshape(128, 128)
        n_bf = n_rows.astype(BF16)
        n = lax.dot_general(pick, n_bf, NT, preferred_element_type=F32)
        fill = lax.dot_general(n.astype(BF16), up, NN, preferred_element_type=F32)
        n = n.astype(jnp.int32)
        fill = fill.astype(jnp.int32)
        word = ((fill >> 7) + CHUNKS * w) * 128 + ((fill - first) & 127)
        words = jnp.where(sub == w, word, words)
        words = jnp.where(sub == 4 + w, fill + n, words)
        first = first + n
        at = lax.dot_general(down, n_bf, NN, preferred_element_type=F32).astype(jnp.int32) & 127
        begin[w] = at
        end[w] = at + n_rows.astype(jnp.int32)
    table[...] = words
    waiter(fm.at[:, pl.ds(0, 127), :], 0).wait_send()


def exchange(resid, coords, angles, ids, counts, wave, moduli):
    grad, back = operators()
    upper = np.triu(np.ones((128, 128), np.float32), 1)
    return pl.pallas_call(
        exchange_kernel,
        name="exchange",
        out_shape=(
            pltpu.VMEM((576, 8, 128), F32),
            pltpu.VMEM((16, 128), jnp.int32),
            pltpu.VMEM((4, 128, 128), jnp.int32),
            pltpu.VMEM((4, 128, 128), jnp.int32),
        ),
        in_specs=[pl.BlockSpec(memory_space=pltpu.HBM)] * 11,
        out_specs=(pl.BlockSpec(memory_space=pltpu.VMEM),) * 4,
        scratch_shapes=[
            pltpu.VMEM((7, 128, 128), F32),
            pltpu.VMEM((256, 128), F32),
            pltpu.VMEM((128, 128), jnp.int32),
            pltpu.VMEM((1, 128), jnp.int32),
            pltpu.VMEM((3000, 128), F32),
            pltpu.VMEM((4, 2, 256), F32),
            pltpu.VMEM((384, 384), BF16),
            pltpu.VMEM((128, 1152), BF16),
            pltpu.VMEM((128, 128), BF16),
            pltpu.VMEM((128, 128), BF16),
            pltpu.VMEM((4, 7, 32, 128), F32),
            pltpu.VMEM((256, 128), F32),
            pltpu.VMEM((32, 128), F32),
            pltpu.SemaphoreType.DMA((5,)),
            pltpu.SemaphoreType.DMA((6,)),
            pltpu.SemaphoreType.REGULAR,
            pltpu.SemaphoreType.DMA(()),
            pltpu.SemaphoreType.DMA((4,)),
        ],
        compiler_params=pltpu.CompilerParams(
            collective_id=0, has_side_effects=True, vmem_limit_bytes=32 * 2**20
        ),
    )(
        *[
            pltpu.with_memory_space_constraint(a, pltpu.HBM)
            for a in (
                resid, coords, angles, ids, counts, wave, moduli,
                jnp.asarray(grad), jnp.asarray(back), jnp.asarray(upper, BF16),
                jnp.asarray(upper.T, BF16),
            )
        ]
    )


def node_coefficients():
    points = gll_points()
    poly = np.zeros((5, 5))
    for node in range(5):
        c = np.array([1.0])
        for other in range(5):
            if other != node:
                c = np.convolve(c, np.array([-points[other], 1.0])) / (points[node] - points[other])
        poly[node] = c
    slope = poly[:, 1:] * np.arange(1, 5)[None, :]
    every = np.concatenate([poly, slope], axis=1)
    blocks = []
    for m in range(9):
        blocks.append(np.concatenate([every[:, m], np.zeros(3)]))
    for t in range(3):
        for m in range(9):
            blocks.append(every[(8 * t + np.arange(8)) % 5, m])
    return np.repeat(np.concatenate(blocks)[:, None], 128, axis=1)


def fill_lanes(win, at, coef, lhs, h):
    tile_in = win[at]

    def spread(x, k):
        return jnp.broadcast_to(x[k : k + 1, :], (8, 128))

    def across(f):
        return spread(tile_in, f)

    def basis(x, block):
        c = [coef[8 * (block + m) : 8 * (block + m) + 8, :] for m in range(9)]
        val = (((c[4] * x + c[3]) * x + c[2]) * x + c[1]) * x + c[0]
        der = ((c[8] * x + c[7]) * x + c[6]) * x + c[5]
        return val, der

    vx, dx = basis(across(1), 0)
    vz, dz = basis(across(3), 0)
    eta = across(2)
    t = [across(4 + i) for i in range(3)]
    d = [across(0) * t[i] for i in range(3)]
    rows = [dx * t[0], vx * t[1], vx * t[2], vz, dz]

    def row(block, node):
        return spread(rows[block], node)

    sub = lax.broadcasted_iota(jnp.int32, (8, 128), 0)

    def by_p(block, tile):
        if tile == 0:
            return jnp.where(sub < 5, row(block, 0), row(block, 1))
        if tile == 1:
            return jnp.where(sub < 2, row(block, 1), jnp.where(sub < 7, row(block, 2), row(block, 3)))
        return jnp.where(sub < 4, row(block, 3), row(block, 4))

    a, b = [], []
    for tile in range(3):
        vy, dy = basis(eta, 9 + 9 * tile)
        a.append(by_p(0, tile) * vy + by_p(1, tile) * dy)
        b.append(by_p(2, tile) * vy)
        if tile == 0:
            vy4, dy4 = vy[4:5, :], dy[4:5, :]

    def shape(j):
        if j < 15:
            return a[j % 3] * row(3, j // 3) + b[j % 3] * row(4, j // 3)
        a4 = row(0, 4) * vy4 + row(1, 4) * dy4
        b4 = row(2, 4) * vy4
        return a4 * vz + b4 * dz

    shapes = jnp.concatenate([shape(j) for j in range(16)], axis=0).reshape(16, 8, 128)
    for i in range(3):
        hi, lo = split((shapes * d[i][None]).reshape(128, 128))
        lhs[h, 128 * i : 128 * i + 128, :] = hi
        lhs[2 + h, 128 * i : 128 * i + 128, :] = lo


def inject_kernel(
    big, table, begin, end, coef, out, xlo, xhi, ylo, yhi, corner,
    acc, win, tabs, lhs_a, lhs_b, tsem,
):
    totab = pltpu.make_async_copy(table, tabs, tsem)
    totab.start()
    totab.wait()

    lane = lax.broadcasted_iota(jnp.int32, (8, 128), 1)
    zero = jnp.zeros((8, 128), F32)

    def place(step, carry):
        for k in range(8):
            t = step * 8 + k
            tile = big[t]
            for w in range(4):
                b = begin[w, pl.ds(t, 8, stride=0), :]
                e = end[w, pl.ds(t, 8, stride=0), :]
                word = tabs[w, t]
                chunk = word >> 7
                rolled = pltpu.roll(tile, word & 127, axis=1)
                pltpu.store(win.at[chunk], jnp.where(lane < e, rolled, zero), mask=lane >= b)
                win[chunk + 1] = jnp.where(lane + 128 < e, rolled, zero)
        return carry

    lax.fori_loop(0, 16, place, 0)
    row = lax.broadcasted_iota(jnp.int32, (256, 128), 0).astype(F32).astype(BF16)
    upto = [0]
    for w in range(4):
        count = tabs[4 + w, 127]
        for k in range(3):
            win[CHUNKS * w + (count + 127) // 128 + k] = zero
        upto.append(upto[-1] + (count + 511) // 512)
    for k in range(4):
        win[4 * CHUNKS + k] = zero

    def chunk_of(u):
        at = u * 4
        for k in range(1, 4):
            at = jnp.where(u >= upto[k], CHUNKS * k + (u - upto[k]) * 4, at)
        return jnp.where(u >= upto[4], 4 * CHUNKS, at)

    def fill(at, lhs):
        for h in range(2):
            fill_lanes(win, at + h, coef, lhs, h)

    def push(at, reg):
        hot = []
        for h in range(2):
            want = jnp.broadcast_to(win[at + h, 7:8, :], (16, 128)).astype(BF16)
            want = jnp.concatenate([want] * 16, axis=0)
            hot.append(jnp.where(row == want, jnp.ones((), BF16), jnp.zeros((), BF16)))
        rhs = jnp.concatenate(hot, axis=1)
        for q in range(2):
            pltpu.matmul_push_rhs(rhs, staging_register=reg, mxu_index=q, transpose=True)

    def use(lhs, reg, accs):
        for q in range(2):
            left = jnp.concatenate([lhs[2 * q], lhs[2 * q + 1]], axis=1)
            pltpu.matmul_acc_lhs(accs[q], left, load_staged_rhs=reg)

    def multiply(*accs):
        for q in range(2):
            pltpu.matmul_pop(accs[q])
        fill(chunk_of(0), lhs_a)
        push(chunk_of(0), 0)
        for w in range(4):

            def two_blocks(step, carry, w=w):
                u = upto[w] + step
                push(CHUNKS * w + 4 * step + 2, 1)
                fill(CHUNKS * w + 4 * step + 2, lhs_b)
                use(lhs_a, 0, accs)
                use(lhs_b, 1, accs)
                fill(chunk_of(u + 1), lhs_a)
                push(chunk_of(u + 1), 0)
                return carry

            lax.fori_loop(0, upto[w + 1] - upto[w], two_blocks, 0)
            if w == 3:
                use(lhs_a, 0, accs)
            total = pltpu.matmul_pop(accs[0]) + pltpu.matmul_pop(accs[1])
            for h in range(2):
                at = NST + 192 * h + 48 * w
                acc[384 * w : 384 * w + 384, 128 * h : 128 * h + 128] = (
                    total[:, 128 * h : 128 * h + 128] + big[at : at + 48].reshape(384, 128)
                )

    pl.run_scoped(multiply, pltpu.ACC(0)((384, 256), F32), pltpu.ACC(1)((384, 256), F32))

    lane2 = lax.broadcasted_iota(jnp.int32, (8, 256), 1)
    for w in range(4):
        cx, cy = w // 2, w % 2
        for i in range(3):
            base = 384 * w + 128 * i
            g = [acc[base + 24 * r : base + 24 * r + 24, :] for r in range(5)]
            tail = acc[base + 120 : base + 128, :]
            groups = [g[0], tail[0:1, :]], [g[4], tail[4:5, :]]
            lows, highs = [], []
            for a, b in zip(*groups):
                ln = lax.broadcasted_iota(jnp.int32, a.shape, 1)
                lows.append(a + jnp.where(ln == 0, 0.0, pltpu.roll(b, 1, axis=1)))
                highs.append(b + jnp.where(ln == 255, 0.0, pltpu.roll(a, 255, axis=1)))
            main = [lows[0], g[1], g[2], g[3], highs[0]]
            last = [lows[1], tail[1:2, :], tail[2:3, :], tail[3:4, :], highs[1]]
            origin = (cx * 3 + i) * 500 + cy
            for r in range(5):
                for h in range(2):
                    cols = slice(128 * h, 128 * h + 128)
                    at = origin + 4 * r + 2 * h
                    out[pl.ds(at, 24, stride=20), :] = main[r][:, cols]
                    out[pl.ds(at + 480, 1), :] = last[r][:, cols]
    for i in range(3):
        a = out[i * 500 + 400 : i * 500 + 500, :]
        b = out[(3 + i) * 500 : (3 + i) * 500 + 100, :]
        out[i * 500 + 400 : i * 500 + 500, :] = a + b
        out[(3 + i) * 500 : (3 + i) * 500 + 100, :] = a + b
    for c in range(6):
        for p in range(5):
            high = pl.ds(c * 500 + 100 * p + 80, 10, stride=2)
            low = pl.ds(c * 500 + 100 * p + 1, 10, stride=2)
            both = out[high, :] + out[low, :]
            out[high, :] = both
            out[low, :] = both
    for i in range(3):
        xlo[100 * i : 100 * i + 100, :] = out[i * 500 : i * 500 + 100, :]
        xhi[100 * i : 100 * i + 100, :] = out[(3 + i) * 500 + 400 : (3 + i) * 500 + 500, :]
    for c in range(6):
        for p in range(5):
            at = 50 * c + 10 * p
            ylo[at : at + 10, :] = out[pl.ds(c * 500 + 100 * p, 10, stride=2), :]
            yhi[at : at + 10, :] = out[pl.ds(c * 500 + 100 * p + 81, 10, stride=2), :]
    for cx in range(2):
        for cy in range(2):
            for i in range(3):
                start = (cx * 3 + i) * 500 + 400 * cx + 80 * cy + cy
                corner[2 * cx + cy, 10 * i : 10 * i + 10, :] = out[pl.ds(start, 10, stride=2), :]


def inject(big, table, begin, end):
    vm = pl.BlockSpec(memory_space=pltpu.VMEM)
    face = jax.ShapeDtypeStruct((304, 128), F32)
    return pl.pallas_call(
        inject_kernel,
        name="inject",
        out_shape=(
            jax.ShapeDtypeStruct((3000, 128), F32),
            face, face, face, face,
            jax.ShapeDtypeStruct((4, 32, 128), F32),
        ),
        in_specs=[vm] * 5,
        out_specs=(vm,) * 6,
        scratch_shapes=[
            pltpu.VMEM((1536, 256), F32),
            pltpu.VMEM((4 * CHUNKS + 4, 8, 128), F32),
            pltpu.SMEM((16, 128), jnp.int32),
            pltpu.VMEM((4, 384, 128), BF16),
            pltpu.VMEM((4, 384, 128), BF16),
            pltpu.SemaphoreType.DMA(()),
        ],
        compiler_params=pltpu.CompilerParams(vmem_limit_bytes=32 * 2**20),
    )(big, table, begin, end, jnp.asarray(node_coefficients(), F32))


SIDES = [(-1, 0), (1, 0), (0, -1), (0, 1), (-1, -1), (-1, 1), (1, -1), (1, 1)]


def there(side, gx, gy):
    ok = None
    for d, g, n in ((side[0], gx, NGX), (side[1], gy, NGY)):
        if d:
            c = (g + d >= 0) & (g + d < n)
            ok = c if ok is None else ok & c
    return ok


def halo_kernel(local, xlo, xhi, ylo, yhi, corner, out, gxlo, gxhi, gylo, gyhi, gcorner, ssem, rsem):
    gx = lax.axis_index("gx")
    gy = lax.axis_index("gy")
    bar = pltpu.get_barrier_semaphore()
    for side in SIDES:
        @pl.when(there(side, gx, gy))
        def _(side=side):
            pl.semaphore_signal(
                bar, inc=1, device_id=(gx + side[0], gy + side[1]), device_id_type=MESH
            )
    nx = (gx > 0).astype(jnp.int32) + (gx < NGX - 1).astype(jnp.int32)
    ny = (gy > 0).astype(jnp.int32) + (gy < NGY - 1).astype(jnp.int32)
    pl.semaphore_wait(bar, (nx + 1) * (ny + 1) - 1)

    src = [xlo, xhi, ylo, yhi] + [corner.at[k] for k in range(4)]
    dst = [gxhi, gxlo, gyhi, gylo] + [gcorner.at[3 - k] for k in range(4)]

    def copy(k):
        side = SIDES[k]
        return pltpu.make_async_remote_copy(
            src_ref=src[k],
            dst_ref=dst[k],
            send_sem=ssem.at[k],
            recv_sem=rsem.at[k],
            device_id=(gx + side[0], gy + side[1]),
            device_id_type=MESH,
        )

    for k in (2, 3, 4, 5, 6, 7, 0, 1):
        @pl.when(there(SIDES[k], gx, gy))
        def _(k=k):
            copy(k).start()
    out[...] = local[...]

    def take(k, add):
        @pl.when(there(SIDES[k], gx, gy))
        def _():
            copy([1, 0, 3, 2, 7, 6, 5, 4][k]).wait_recv()
            add()

    def add_xlo():
        for i in range(3):
            out[i * 500 : i * 500 + 100, :] += gxlo[100 * i : 100 * i + 100, :]

    def add_xhi():
        for i in range(3):
            out[(3 + i) * 500 + 400 : (3 + i) * 500 + 500, :] += gxhi[100 * i : 100 * i + 100, :]

    def add_y(ref, shift):
        for c in range(6):
            for p in range(5):
                k = 50 * c + 10 * p
                rows = pl.ds(c * 500 + 100 * p + shift, 10, stride=2)
                out[rows, :] += ref[k : k + 10, :]

    def add_corner(k):
        cx, cy = k // 2, k % 2
        for i in range(3):
            rows = pl.ds((cx * 3 + i) * 500 + 400 * cx + 80 * cy + cy, 10, stride=2)
            out[rows, :] += gcorner[k, 10 * i : 10 * i + 10, :]

    take(0, add_xlo)
    take(1, add_xhi)
    for k in range(4):
        take(4 + k, functools.partial(add_corner, k))
    take(2, lambda: add_y(gylo, 0))
    take(3, lambda: add_y(gyhi, 81))
    for k in range(8):
        @pl.when(there(SIDES[k], gx, gy))
        def _(k=k):
            copy(k).wait_send()


def halo(local, xlo, xhi, ylo, yhi, corner):
    vm = pl.BlockSpec(memory_space=pltpu.VMEM)
    return pl.pallas_call(
        halo_kernel,
        name="halo",
        out_shape=jax.ShapeDtypeStruct((3000, 128), F32),
        in_specs=[vm] * 6,
        out_specs=vm,
        scratch_shapes=[pltpu.VMEM((304, 128), F32)] * 4
        + [
            pltpu.VMEM((4, 32, 128), F32),
            pltpu.SemaphoreType.DMA((8,)),
            pltpu.SemaphoreType.DMA((8,)),
        ],
        compiler_params=pltpu.CompilerParams(
            collective_id=1, has_side_effects=True, vmem_limit_bytes=16 * 2**20
        ),
    )(local, xlo, xhi, ylo, yhi, corner)


def body(wavefield, moduli, residuals, coords, angles, element_ids, counts):
    wave = wavefield.reshape(2, 2, 3, 125, 2, 128).transpose(0, 2, 3, 4, 1, 5).reshape(3000, 128)
    sorted_slots = exchange(
        residuals[0],
        coords[0].transpose(1, 0, 2),
        angles.reshape(256, 128),
        element_ids[0],
        counts,
        wave,
        moduli.reshape(4, 2, 256),
    )
    out = halo(*inject(*sorted_slots))
    out = out.reshape(2, 3, 125, 2, 2, 128).transpose(0, 4, 1, 2, 3, 5)
    return out.reshape(2, 2, 3, 125, 256)


def solution(mesh):
    in_specs = (
        P("gx", "gy", None, None, None),
        P("gx", "gy", None, None),
        P(("gx", "gy"), None, None),
        P(("gx", "gy"), None, None, None),
        P(("gx", "gy"), None, None, None),
        P(("gx", "gy"), None, None),
        P(("gx", "gy"), None),
    )
    out_specs = P("gx", "gy", None, None, None)
    return jax.shard_map(body, mesh=mesh, in_specs=in_specs, out_specs=out_specs, check_vma=False)
```

```python
import functools
import math

import jax
import jax.numpy as jnp
import numpy as np
from jax import lax
from jax.experimental import pallas as pl
from jax.experimental.pallas import tpu as pltpu
from jax.sharding import PartitionSpec as P

MESH = pl.DeviceIdType.MESH
F32 = jnp.float32
BF16 = jnp.bfloat16
NGX = 8
NGY = 16
NDEV = 128
CHUNKS = 136
NST = 128
FIELD = 136
NT = (((1,), (1,)), ((), ()))
NN = (((1,), (0,)), ((), ()))


def gll_points():
    return np.array([-1.0, -math.sqrt(3.0 / 7.0), 0.0, math.sqrt(3.0 / 7.0), 1.0])


def gll_weights():
    return np.array([0.1, 49.0 / 90.0, 32.0 / 45.0, 49.0 / 90.0, 0.1])


def derivative_table():
    points = gll_points()
    table = np.zeros((5, 5))
    for row in range(5):
        for col in range(5):
            if row == col:
                table[row, col] = sum(
                    (1.0 / (points[col] - points[other]) for other in range(5) if other != col)
                )
            else:
                value = 1.0 / (points[col] - points[row])
                for other in range(5):
                    if other != col and other != row:
                        value = (
                            value * (points[row] - points[other]) / (points[col] - points[other])
                        )
                table[row, col] = value
    return table


def split_np(a):
    hi = np.asarray(a, np.float32).astype(jnp.bfloat16)
    lo = (np.asarray(a, np.float64) - hi.astype(np.float64)).astype(jnp.bfloat16)
    return hi, lo


def row_of(p, q, r):
    pq = 5 * p + q
    return 120 + r if pq == 24 else 24 * r + pq


def operators():
    table = np.asarray(derivative_table(), np.float32).astype(np.float64)
    weight = np.asarray(gll_weights(), np.float32).astype(np.float64)
    grad = np.zeros((3, 128, 128))
    back = np.zeros((3, 128, 128))
    for p in range(5):
        for q in range(5):
            for r in range(5):
                n = 25 * p + 5 * q + r
                for k in range(5):
                    grad[0, n, 25 * k + 5 * q + r] = table[p, k]
                    grad[1, n, 25 * p + 5 * k + r] = table[q, k]
                    grad[2, n, 25 * p + 5 * q + k] = table[r, k]
                w = weight[p] * weight[q] * weight[r]
                for k in range(5):
                    back[0, row_of(k, q, r), n] = -w * table[p, k]
                    back[1, row_of(p, k, r), n] = -w * table[q, k]
                    back[2, row_of(p, q, k), n] = -w * table[r, k]
    ghi, glo = split_np(grad.reshape(384, 128))
    flat = np.concatenate([back[0], back[1], back[2]], axis=1)
    bhi, blo = split_np(flat)
    return np.concatenate([ghi, glo, ghi], axis=1), np.concatenate([bhi, blo, bhi], axis=1)


def split(x):
    hi = x.astype(BF16)
    return hi, (x - hi.astype(F32)).astype(BF16)


def sin_cos(x):
    y = 0.5 * x
    z = y * y
    s = y * (
        1.0
        + z * (-1.0 / 6 + z * (1.0 / 120 + z * (-1.0 / 5040 + z * (1.0 / 362880 + z * (-1.0 / 39916800)))))
    )
    c = 1.0 + z * (
        -0.5
        + z
        * (1.0 / 24 + z * (-1.0 / 720 + z * (1.0 / 40320 + z * (-1.0 / 3628800 + z * (1.0 / 479001600)))))
    )
    return 2.0 * s * c, 1.0 - 2.0 * s * s


def far_first(j):
    return 2 + ((j + 1) // 2) * (1 - 2 * (j % 2))


def exchange_kernel(
    resid, coords, angles, ids, counts, wave, moduli, grad, back, upper,
    stage, table,
    fl, pos_s, outgo, abuf, ibuf, cbuf, wbuf, mbuf, gbuf, bbuf, ubuf,
    isem, wsem, bsem, ssem, rsem,
):
    gx = lax.axis_index("gx")
    gy = lax.axis_index("gy")
    me = gx * NGY + gy
    y, core, z, x = gx // 2, gx % 2, gy // 4, gy % 4
    loads = [
        pltpu.make_async_copy(a, b, isem.at[k])
        for k, (a, b) in enumerate(
            [(counts, cbuf), (ids, ibuf), (angles, abuf), (upper, ubuf)]
            + [(resid, fl.at[pl.ds(0, 128)])]
            + [(coords.at[d], fl.at[pl.ds(FIELD * (1 + d), 128)]) for d in range(3)]
        )
    ]
    fetches = [
        pltpu.make_async_copy(a, b, wsem.at[k])
        for k, (a, b) in enumerate(
            ((wave, wbuf), (moduli, mbuf), (grad, gbuf), (back, bbuf))
        )
    ]
    for load in loads + fetches:
        load.start()
    bar = pltpu.get_barrier_semaphore()
    for k in range(1, NGY):
        pl.semaphore_signal(bar, inc=1, device_id=(gx, (gy + k) % NGY), device_id_type=MESH)
    for k in range(1, NGX):
        pl.semaphore_signal(bar, inc=1, device_id=((gx + k) % NGX, gy), device_id_type=MESH)
    for load in loads:
        load.wait()

    sin_a, cos_a = sin_cos(abuf[pl.ds(0, 128, stride=2), :])
    sin_d, cos_d = sin_cos(abuf[pl.ds(1, 128, stride=2), :])
    fl[FIELD * 4 : FIELD * 4 + 128, :] = cos_a * cos_d
    fl[FIELD * 5 : FIELD * 5 + 128, :] = sin_a * cos_d
    fl[FIELD * 6 : FIELD * 6 + 128, :] = sin_d
    limit = jnp.transpose(jnp.broadcast_to(cbuf[...].astype(F32), (128, 128)))
    slot = lax.broadcasted_iota(jnp.int32, (128, 128), 1).astype(F32)
    num = ibuf[...].astype(F32)
    fl[FIELD * 7 : FIELD * 7 + 128, :] = num + 1.0
    up = ubuf[...]
    ones = jnp.ones((128, 128), BF16)

    def columns_of(col):
        masks = [(col == float(w)).astype(F32).astype(BF16) for w in range(4)]
        return jnp.concatenate(masks, axis=0)

    colf = jnp.where(slot < limit, jnp.floor(num * (1.0 / 256.0)), -1.0)
    stacked = columns_of(colf)
    prefix = lax.dot_general(stacked, up, NN, preferred_element_type=F32)
    total = lax.dot_general(stacked, ones, NN, preferred_element_type=F32)
    start = jnp.zeros((128, 128), F32)
    pos = jnp.full((128, 128), -1.0, F32)
    for w in range(4):
        rows = slice(128 * w, 128 * w + 128)
        pos = jnp.where(colf == float(w), prefix[rows] + start, pos)
        start = start + total[rows]
    pos_s[...] = pos
    lane_row = lax.broadcasted_iota(jnp.int32, (128, 128), 0).astype(F32)

    def sort_some(h, carry):
        for k in range(16):
            t = h * 16 + k
            f = fl[pl.ds(t, 8, stride=FIELD), :]
            hi = f.astype(BF16).astype(F32)
            mid = (f - hi).astype(BF16).astype(F32)
            lo = f - hi - mid
            perm = jnp.where(lane_row == pos_s[pl.ds(t, 1), :], 1.0, 0.0).astype(BF16)
            got = lax.dot_general(
                jnp.concatenate([hi, mid, lo], axis=0).astype(BF16),
                perm,
                NT,
                preferred_element_type=F32,
            )
            outgo[t] = got[0:8] + got[8:16] + got[16:24]
        return carry

    lax.fori_loop(0, 4, sort_some, 0)
    pl.semaphore_wait(bar, NGX + NGY - 2)
    for k in range(1, NGX):
        pl.semaphore_signal(bsem, inc=1, device_id=((gx + k) % NGX, gy), device_id_type=MESH)
    lax.fori_loop(4, 8, sort_some, 0)
    stage[NDEV - 1] = outgo[me]
    pl.semaphore_wait(bsem, NGX - 1)

    def send(j, last):
        ty = (y + far_first(j // 4)) % 4
        tz = (z + far_first(j % 4)) % 4
        for m in range(7 if last else 8):
            tx = (x + far_first(m // 2)) % 4
            tc = (core + 1 - m % 2) % 2
            pltpu.make_async_remote_copy(
                src_ref=outgo.at[(2 * ty + tc) * NGY + 4 * tz + tx],
                dst_ref=stage.at[j * 8 + m],
                send_sem=ssem,
                recv_sem=rsem,
                device_id=(2 * ty + tc, 4 * tz + tx),
                device_id_type=MESH,
            ).start()

    def send_eight(j, carry):
        send(j, False)
        return carry

    lax.fori_loop(0, 15, send_eight, 0)
    send(15, True)
    for fetch in fetches:
        fetch.wait()

    def column(w, carry):
        cx = w // 2
        cy = w % 2
        lam = mbuf[w, 0:1, :]
        mu = mbuf[w, 1:2, :]
        grads = []
        for i in range(3):
            start = (cx * 3 + i) * 500 + cy
            u = jnp.concatenate(
                [wbuf[pl.ds(start + 2 * h, 125, stride=4), :] for h in range(2)], axis=1
            )
            u = jnp.concatenate([u, jnp.zeros((3, 256), F32)], axis=0)
            hi, lo = split(u)
            grads.append(
                lax.dot_general(
                    gbuf[...],
                    jnp.concatenate([hi, hi, lo], axis=0),
                    NN,
                    preferred_element_type=F32,
                )
            )
        g = [[grads[i][128 * j : 128 * j + 128] for j in range(3)] for i in range(3)]
        ldiv = lam * (g[0][0] + g[1][1] + g[2][2])
        parts = {}
        for i in range(3):
            for j in range(i, 3):
                s = mu * (g[i][j] + g[j][i])
                if i == j:
                    s = s + ldiv
                parts[(i, j)] = parts[(j, i)] = split(s)
        for i in range(3):
            hi = [parts[(i, j)][0] for j in range(3)]
            lo = [parts[(i, j)][1] for j in range(3)]
            got = lax.dot_general(
                bbuf[...],
                jnp.concatenate(hi + hi + lo, axis=0),
                NN,
                preferred_element_type=F32,
            )
            for h in range(2):
                at = NST + 192 * h + 48 * w + 16 * i
                stage[pl.ds(at, 16)] = got[:, 128 * h : 128 * h + 128].reshape(16, 8, 128)
        return carry

    lax.fori_loop(0, 4, column, 0)
    drain = pltpu.make_async_remote_copy(
        src_ref=outgo.at[pl.ds(0, NDEV - 1)],
        dst_ref=stage.at[pl.ds(0, NDEV - 1)],
        send_sem=ssem,
        recv_sem=rsem,
        device_id=(gx, (gy + 1) % NGY),
        device_id_type=MESH,
    )
    drain.wait_recv()
    got = stage.reshape(4096, 128)[pl.ds(7, NDEV, stride=8), :]
    received = columns_of(jnp.floor((got - 1.0) * (1.0 / 256.0)))
    total = lax.dot_general(received, ones, NN, preferred_element_type=F32)
    sub = lax.broadcasted_iota(jnp.int32, (16, 128), 0)
    lane16 = lax.broadcasted_iota(jnp.int32, (16, 128), 1)
    pick = jnp.where(lane16 == 0, 1.0, 0.0).astype(BF16)
    words = jnp.zeros((16, 128), jnp.int32)
    first = jnp.zeros((16, 128), jnp.int32)
    for w in range(4):
        n_bf = total[128 * w : 128 * w + 128].astype(BF16)
        n = lax.dot_general(pick, n_bf, NT, preferred_element_type=F32)
        fill = lax.dot_general(n.astype(BF16), up, NN, preferred_element_type=F32)
        n = n.astype(jnp.int32)
        fill = fill.astype(jnp.int32)
        word = ((fill >> 7) + CHUNKS * w) * 16384 + (fill & 127) * 128 + ((fill - first) & 127)
        words = jnp.where(sub == w, word, words)
        words = jnp.where(sub == 4 + w, fill + n, words)
        first = first + n
    table[...] = words
    drain.wait_send()


def exchange(resid, coords, angles, ids, counts, wave, moduli):
    grad, back = operators()
    upper = np.triu(np.ones((128, 128), np.float32), 1)
    return pl.pallas_call(
        exchange_kernel,
        name="exchange",
        out_shape=(
            pltpu.VMEM((512, 8, 128), F32),
            pltpu.VMEM((16, 128), jnp.int32),
        ),
        in_specs=[pl.BlockSpec(memory_space=pltpu.HBM)] * 10,
        out_specs=(pl.BlockSpec(memory_space=pltpu.VMEM),) * 2,
        scratch_shapes=[
            pltpu.VMEM((8 * FIELD, 128), F32),
            pltpu.VMEM((128, 128), F32),
            pltpu.VMEM((NDEV, 8, 128), F32),
            pltpu.VMEM((256, 128), F32),
            pltpu.VMEM((128, 128), jnp.int32),
            pltpu.VMEM((1, 128), jnp.int32),
            pltpu.VMEM((3000, 128), F32),
            pltpu.VMEM((4, 2, 256), F32),
            pltpu.VMEM((384, 384), BF16),
            pltpu.VMEM((128, 1152), BF16),
            pltpu.VMEM((128, 128), BF16),
            pltpu.SemaphoreType.DMA((8,)),
            pltpu.SemaphoreType.DMA((4,)),
            pltpu.SemaphoreType.REGULAR,
            pltpu.SemaphoreType.DMA(()),
            pltpu.SemaphoreType.DMA(()),
        ],
        compiler_params=pltpu.CompilerParams(
            collective_id=0, has_side_effects=True, vmem_limit_bytes=32 * 2**20
        ),
    )(
        *[
            pltpu.with_memory_space_constraint(a, pltpu.HBM)
            for a in (
                resid, coords, angles, ids, counts, wave, moduli,
                jnp.asarray(grad), jnp.asarray(back), jnp.asarray(upper, BF16),
            )
        ]
    )


def node_coefficients():
    points = gll_points()
    poly = np.zeros((5, 5))
    for node in range(5):
        c = np.array([1.0])
        for other in range(5):
            if other != node:
                c = np.convolve(c, np.array([-points[other], 1.0])) / (points[node] - points[other])
        poly[node] = c
    slope = poly[:, 1:] * np.arange(1, 5)[None, :]
    every = np.concatenate([poly, slope], axis=1)
    blocks = []
    for m in range(9):
        blocks.append(np.concatenate([every[:, m], np.zeros(3)]))
    for t in range(3):
        for m in range(9):
            blocks.append(every[(8 * t + np.arange(8)) % 5, m])
    return np.repeat(np.concatenate(blocks)[:, None], 128, axis=1)


def fill_lanes(win, at, coef, lhs, h):
    tile_in = win[at]

    def spread(x, k):
        return jnp.broadcast_to(x[k : k + 1, :], (8, 128))

    def across(f):
        return spread(tile_in, f)

    def basis(x, block):
        c = [coef[8 * (block + m) : 8 * (block + m) + 8, :] for m in range(9)]
        val = (((c[4] * x + c[3]) * x + c[2]) * x + c[1]) * x + c[0]
        der = ((c[8] * x + c[7]) * x + c[6]) * x + c[5]
        return val, der

    vx, dx = basis(across(1), 0)
    vz, dz = basis(across(3), 0)
    eta = across(2)
    t = [across(4 + i) for i in range(3)]
    d = [across(0) * t[i] for i in range(3)]
    rows = [dx * t[0], vx * t[1], vx * t[2], vz, dz]

    def row(block, node):
        return spread(rows[block], node)

    sub = lax.broadcasted_iota(jnp.int32, (8, 128), 0)

    def by_p(block, tile):
        if tile == 0:
            return jnp.where(sub < 5, row(block, 0), row(block, 1))
        if tile == 1:
            return jnp.where(sub < 2, row(block, 1), jnp.where(sub < 7, row(block, 2), row(block, 3)))
        return jnp.where(sub < 4, row(block, 3), row(block, 4))

    a, b = [], []
    for tile in range(3):
        vy, dy = basis(eta, 9 + 9 * tile)
        a.append(by_p(0, tile) * vy + by_p(1, tile) * dy)
        b.append(by_p(2, tile) * vy)
        if tile == 0:
            vy4, dy4 = vy[4:5, :], dy[4:5, :]

    def shape(j):
        if j < 15:
            return a[j % 3] * row(3, j // 3) + b[j % 3] * row(4, j // 3)
        a4 = row(0, 4) * vy4 + row(1, 4) * dy4
        b4 = row(2, 4) * vy4
        return a4 * vz + b4 * dz

    shapes = jnp.concatenate([shape(j) for j in range(16)], axis=0).reshape(16, 8, 128)
    for i in range(3):
        hi, lo = split((shapes * d[i][None]).reshape(128, 128))
        lhs[h, 128 * i : 128 * i + 128, :] = hi
        lhs[2 + h, 128 * i : 128 * i + 128, :] = lo


def inject_kernel(
    big, table, coef, out, xlo, xhi, ylo, yhi, corner,
    acc, win, tabs, lhs_a, lhs_b, tsem,
):
    totab = pltpu.make_async_copy(table, tabs, tsem)
    totab.start()
    totab.wait()

    lane = lax.broadcasted_iota(jnp.int32, (8, 128), 1)
    zero = jnp.zeros((8, 128), F32)

    def place(step, carry):
        for k in range(8):
            t = step * 8 + k
            tile = big[t]
            col = jnp.floor((jnp.broadcast_to(tile[7:8, :], (8, 128)) - 1.0) * (1.0 / 256.0))
            for w in range(4):
                word = tabs[w, t]
                chunk = word >> 14
                begin = (word >> 7) & 127
                run = pltpu.roll(jnp.where(col == float(w), tile, zero), word & 127, axis=1)
                after = lane >= begin
                pltpu.store(win.at[chunk], run, mask=after)
                win[chunk + 1] = jnp.where(after, zero, run)
        return carry

    lax.fori_loop(0, 16, place, 0)
    row = lax.broadcasted_iota(jnp.int32, (256, 128), 0).astype(F32).astype(BF16)
    upto = [0]
    for w in range(4):
        count = tabs[4 + w, 127]
        for k in range(3):
            win[CHUNKS * w + (count + 127) // 128 + k] = zero
        upto.append(upto[-1] + (count + 511) // 512)
    for k in range(4):
        win[4 * CHUNKS + k] = zero

    def chunk_of(u):
        at = u * 4
        for k in range(1, 4):
            at = jnp.where(u >= upto[k], CHUNKS * k + (u - upto[k]) * 4, at)
        return jnp.where(u >= upto[4], 4 * CHUNKS, at)

    def fill(at, lhs):
        for h in range(2):
            fill_lanes(win, at + h, coef, lhs, h)

    def push(at, reg):
        hot = []
        for h in range(2):
            want = jnp.broadcast_to(win[at + h, 7:8, :], (16, 128)) - 1.0
            want = (want - 256.0 * jnp.floor(want * (1.0 / 256.0))).astype(BF16)
            want = jnp.concatenate([want] * 16, axis=0)
            hot.append(jnp.where(row == want, jnp.ones((), BF16), jnp.zeros((), BF16)))
        rhs = jnp.concatenate(hot, axis=1)
        for q in range(2):
            pltpu.matmul_push_rhs(rhs, staging_register=reg, mxu_index=q, transpose=True)

    def use(lhs, reg, accs):
        for q in range(2):
            left = jnp.concatenate([lhs[2 * q], lhs[2 * q + 1]], axis=1)
            pltpu.matmul_acc_lhs(accs[q], left, load_staged_rhs=reg)

    def multiply(*accs):
        for q in range(2):
            pltpu.matmul_pop(accs[q])
        fill(chunk_of(0), lhs_a)
        push(chunk_of(0), 0)
        for w in range(4):

            def two_blocks(step, carry, w=w):
                u = upto[w] + step
                push(CHUNKS * w + 4 * step + 2, 1)
                fill(CHUNKS * w + 4 * step + 2, lhs_b)
                use(lhs_a, 0, accs)
                use(lhs_b, 1, accs)
                fill(chunk_of(u + 1), lhs_a)
                push(chunk_of(u + 1), 0)
                return carry

            lax.fori_loop(0, upto[w + 1] - upto[w], two_blocks, 0)
            if w == 3:
                use(lhs_a, 0, accs)
            total = pltpu.matmul_pop(accs[0]) + pltpu.matmul_pop(accs[1])
            for h in range(2):
                at = NST + 192 * h + 48 * w
                acc[384 * w : 384 * w + 384, 128 * h : 128 * h + 128] = (
                    total[:, 128 * h : 128 * h + 128] + big[at : at + 48].reshape(384, 128)
                )

    pl.run_scoped(multiply, pltpu.ACC(0)((384, 256), F32), pltpu.ACC(1)((384, 256), F32))

    lane2 = lax.broadcasted_iota(jnp.int32, (8, 256), 1)
    for w in range(4):
        cx, cy = w // 2, w % 2
        for i in range(3):
            base = 384 * w + 128 * i
            g = [acc[base + 24 * r : base + 24 * r + 24, :] for r in range(5)]
            tail = acc[base + 120 : base + 128, :]
            groups = [g[0], tail[0:1, :]], [g[4], tail[4:5, :]]
            lows, highs = [], []
            for a, b in zip(*groups):
                ln = lax.broadcasted_iota(jnp.int32, a.shape, 1)
                lows.append(a + jnp.where(ln == 0, 0.0, pltpu.roll(b, 1, axis=1)))
                highs.append(b + jnp.where(ln == 255, 0.0, pltpu.roll(a, 255, axis=1)))
            main = [lows[0], g[1], g[2], g[3], highs[0]]
            last = [lows[1], tail[1:2, :], tail[2:3, :], tail[3:4, :], highs[1]]
            origin = (cx * 3 + i) * 500 + cy
            for r in range(5):
                for h in range(2):
                    cols = slice(128 * h, 128 * h + 128)
                    at = origin + 4 * r + 2 * h
                    out[pl.ds(at, 24, stride=20), :] = main[r][:, cols]
                    out[pl.ds(at + 480, 1), :] = last[r][:, cols]
    for i in range(3):
        a = out[i * 500 + 400 : i * 500 + 500, :]
        b = out[(3 + i) * 500 : (3 + i) * 500 + 100, :]
        out[i * 500 + 400 : i * 500 + 500, :] = a + b
        out[(3 + i) * 500 : (3 + i) * 500 + 100, :] = a + b
    for c in range(6):
        for p in range(5):
            high = pl.ds(c * 500 + 100 * p + 80, 10, stride=2)
            low = pl.ds(c * 500 + 100 * p + 1, 10, stride=2)
            both = out[high, :] + out[low, :]
            out[high, :] = both
            out[low, :] = both
    for i in range(3):
        xlo[100 * i : 100 * i + 100, :] = out[i * 500 : i * 500 + 100, :]
        xhi[100 * i : 100 * i + 100, :] = out[(3 + i) * 500 + 400 : (3 + i) * 500 + 500, :]
    for c in range(6):
        for p in range(5):
            at = 50 * c + 10 * p
            ylo[at : at + 10, :] = out[pl.ds(c * 500 + 100 * p, 10, stride=2), :]
            yhi[at : at + 10, :] = out[pl.ds(c * 500 + 100 * p + 81, 10, stride=2), :]
    for cx in range(2):
        for cy in range(2):
            for i in range(3):
                start = (cx * 3 + i) * 500 + 400 * cx + 80 * cy + cy
                corner[2 * cx + cy, 10 * i : 10 * i + 10, :] = out[pl.ds(start, 10, stride=2), :]


def inject(big, table):
    vm = pl.BlockSpec(memory_space=pltpu.VMEM)
    face = jax.ShapeDtypeStruct((304, 128), F32)
    return pl.pallas_call(
        inject_kernel,
        name="inject",
        out_shape=(
            jax.ShapeDtypeStruct((3000, 128), F32),
            face, face, face, face,
            jax.ShapeDtypeStruct((4, 32, 128), F32),
        ),
        in_specs=[vm] * 3,
        out_specs=(vm,) * 6,
        scratch_shapes=[
            pltpu.VMEM((1536, 256), F32),
            pltpu.VMEM((4 * CHUNKS + 4, 8, 128), F32),
            pltpu.SMEM((16, 128), jnp.int32),
            pltpu.VMEM((4, 384, 128), BF16),
            pltpu.VMEM((4, 384, 128), BF16),
            pltpu.SemaphoreType.DMA(()),
        ],
        compiler_params=pltpu.CompilerParams(vmem_limit_bytes=32 * 2**20),
    )(big, table, jnp.asarray(node_coefficients(), F32))


SIDES = [(-1, 0), (1, 0), (0, -1), (0, 1), (-1, -1), (-1, 1), (1, -1), (1, 1)]


def there(side, gx, gy):
    ok = None
    for d, g, n in ((side[0], gx, NGX), (side[1], gy, NGY)):
        if d:
            c = (g + d >= 0) & (g + d < n)
            ok = c if ok is None else ok & c
    return ok


def halo_kernel(local, xlo, xhi, ylo, yhi, corner, out, gxlo, gxhi, gylo, gyhi, gcorner, ssem, rsem):
    gx = lax.axis_index("gx")
    gy = lax.axis_index("gy")
    bar = pltpu.get_barrier_semaphore()
    for side in SIDES:
        @pl.when(there(side, gx, gy))
        def _(side=side):
            pl.semaphore_signal(
                bar, inc=1, device_id=(gx + side[0], gy + side[1]), device_id_type=MESH
            )
    nx = (gx > 0).astype(jnp.int32) + (gx < NGX - 1).astype(jnp.int32)
    ny = (gy > 0).astype(jnp.int32) + (gy < NGY - 1).astype(jnp.int32)
    pl.semaphore_wait(bar, (nx + 1) * (ny + 1) - 1)

    src = [xlo, xhi, ylo, yhi] + [corner.at[k] for k in range(4)]
    dst = [gxhi, gxlo, gyhi, gylo] + [gcorner.at[3 - k] for k in range(4)]

    def copy(k):
        side = SIDES[k]
        return pltpu.make_async_remote_copy(
            src_ref=src[k],
            dst_ref=dst[k],
            send_sem=ssem.at[k],
            recv_sem=rsem.at[k],
            device_id=(gx + side[0], gy + side[1]),
            device_id_type=MESH,
        )

    for k in (2, 3, 4, 5, 6, 7, 0, 1):
        @pl.when(there(SIDES[k], gx, gy))
        def _(k=k):
            copy(k).start()
    out[...] = local[...]

    def take(k, add):
        @pl.when(there(SIDES[k], gx, gy))
        def _():
            copy([1, 0, 3, 2, 7, 6, 5, 4][k]).wait_recv()
            add()

    def add_xlo():
        for i in range(3):
            out[i * 500 : i * 500 + 100, :] += gxlo[100 * i : 100 * i + 100, :]

    def add_xhi():
        for i in range(3):
            out[(3 + i) * 500 + 400 : (3 + i) * 500 + 500, :] += gxhi[100 * i : 100 * i + 100, :]

    def add_y(ref, shift):
        for c in range(6):
            for p in range(5):
                k = 50 * c + 10 * p
                rows = pl.ds(c * 500 + 100 * p + shift, 10, stride=2)
                out[rows, :] += ref[k : k + 10, :]

    def add_corner(k):
        cx, cy = k // 2, k % 2
        for i in range(3):
            rows = pl.ds((cx * 3 + i) * 500 + 400 * cx + 80 * cy + cy, 10, stride=2)
            out[rows, :] += gcorner[k, 10 * i : 10 * i + 10, :]

    take(0, add_xlo)
    take(1, add_xhi)
    for k in range(4):
        take(4 + k, functools.partial(add_corner, k))
    take(2, lambda: add_y(gylo, 0))
    take(3, lambda: add_y(gyhi, 81))
    for k in range(8):
        @pl.when(there(SIDES[k], gx, gy))
        def _(k=k):
            copy(k).wait_send()


def halo(local, xlo, xhi, ylo, yhi, corner):
    vm = pl.BlockSpec(memory_space=pltpu.VMEM)
    return pl.pallas_call(
        halo_kernel,
        name="halo",
        out_shape=jax.ShapeDtypeStruct((3000, 128), F32),
        in_specs=[vm] * 6,
        out_specs=vm,
        scratch_shapes=[pltpu.VMEM((304, 128), F32)] * 4
        + [
            pltpu.VMEM((4, 32, 128), F32),
            pltpu.SemaphoreType.DMA((8,)),
            pltpu.SemaphoreType.DMA((8,)),
        ],
        compiler_params=pltpu.CompilerParams(
            collective_id=1, has_side_effects=True, vmem_limit_bytes=16 * 2**20
        ),
    )(local, xlo, xhi, ylo, yhi, corner)


def body(wavefield, moduli, residuals, coords, angles, element_ids, counts):
    wave = wavefield.reshape(2, 2, 3, 125, 2, 128).transpose(0, 2, 3, 4, 1, 5).reshape(3000, 128)
    sorted_slots = exchange(
        residuals[0],
        coords[0].transpose(1, 0, 2),
        angles.reshape(256, 128),
        element_ids[0],
        counts,
        wave,
        moduli.reshape(4, 2, 256),
    )
    out = halo(*inject(*sorted_slots))
    out = out.reshape(2, 3, 125, 2, 2, 128).transpose(0, 4, 1, 2, 3, 5)
    return out.reshape(2, 2, 3, 125, 256)


def solution(mesh):
    in_specs = (
        P("gx", "gy", None, None, None),
        P("gx", "gy", None, None),
        P(("gx", "gy"), None, None),
        P(("gx", "gy"), None, None, None),
        P(("gx", "gy"), None, None, None),
        P(("gx", "gy"), None, None),
        P(("gx", "gy"), None),
    )
    out_specs = P("gx", "gy", None, None, None)
    return jax.shard_map(body, mesh=mesh, in_specs=in_specs, out_specs=out_specs, check_vma=False)
```

```python
import functools
import math

import jax
import jax.numpy as jnp
import numpy as np
from jax import lax
from jax.experimental import pallas as pl
from jax.experimental.pallas import tpu as pltpu
from jax.sharding import PartitionSpec as P

MESH = pl.DeviceIdType.MESH
F32 = jnp.float32
BF16 = jnp.bfloat16
NGX = 8
NGY = 16
NDEV = 128
CHUNKS = 136
NST = 128
FIELD = 136
NT = (((1,), (1,)), ((), ()))
NN = (((1,), (0,)), ((), ()))


def gll_points():
    return np.array([-1.0, -math.sqrt(3.0 / 7.0), 0.0, math.sqrt(3.0 / 7.0), 1.0])


def gll_weights():
    return np.array([0.1, 49.0 / 90.0, 32.0 / 45.0, 49.0 / 90.0, 0.1])


def derivative_table():
    points = gll_points()
    table = np.zeros((5, 5))
    for row in range(5):
        for col in range(5):
            if row == col:
                table[row, col] = sum(
                    (1.0 / (points[col] - points[other]) for other in range(5) if other != col)
                )
            else:
                value = 1.0 / (points[col] - points[row])
                for other in range(5):
                    if other != col and other != row:
                        value = (
                            value * (points[row] - points[other]) / (points[col] - points[other])
                        )
                table[row, col] = value
    return table


def split_np(a):
    hi = np.asarray(a, np.float32).astype(jnp.bfloat16)
    lo = (np.asarray(a, np.float64) - hi.astype(np.float64)).astype(jnp.bfloat16)
    return hi, lo


def row_of(p, q, r):
    pq = 5 * p + q
    return 120 + r if pq == 24 else 24 * r + pq


def operators():
    table = np.asarray(derivative_table(), np.float32).astype(np.float64)
    weight = np.asarray(gll_weights(), np.float32).astype(np.float64)
    grad = np.zeros((3, 128, 128))
    back = np.zeros((3, 128, 128))
    for p in range(5):
        for q in range(5):
            for r in range(5):
                n = 25 * p + 5 * q + r
                for k in range(5):
                    grad[0, n, 25 * k + 5 * q + r] = table[p, k]
                    grad[1, n, 25 * p + 5 * k + r] = table[q, k]
                    grad[2, n, 25 * p + 5 * q + k] = table[r, k]
                w = weight[p] * weight[q] * weight[r]
                for k in range(5):
                    back[0, row_of(k, q, r), n] = -w * table[p, k]
                    back[1, row_of(p, k, r), n] = -w * table[q, k]
                    back[2, row_of(p, q, k), n] = -w * table[r, k]
    ghi, glo = split_np(grad.reshape(384, 128))
    flat = np.concatenate([back[0], back[1], back[2]], axis=1)
    bhi, blo = split_np(flat)
    return np.concatenate([ghi, glo, ghi], axis=1), np.concatenate([bhi, blo, bhi], axis=1)


def split(x):
    hi = x.astype(BF16)
    return hi, (x - hi.astype(F32)).astype(BF16)


def sin_cos(x):
    y = 0.5 * x
    z = y * y
    s = y * (
        1.0
        + z * (-1.0 / 6 + z * (1.0 / 120 + z * (-1.0 / 5040 + z * (1.0 / 362880 + z * (-1.0 / 39916800)))))
    )
    c = 1.0 + z * (
        -0.5
        + z
        * (1.0 / 24 + z * (-1.0 / 720 + z * (1.0 / 40320 + z * (-1.0 / 3628800 + z * (1.0 / 479001600)))))
    )
    return 2.0 * s * c, 1.0 - 2.0 * s * s


def far_first(j):
    return 2 + ((j + 1) // 2) * (1 - 2 * (j % 2))


def exchange_kernel(
    resid, coords, angles, ids, counts, wave, moduli, grad, back, upper,
    stage, table,
    fl, pos_s, outgo, abuf, ibuf, cbuf, wbuf, mbuf, gbuf, bbuf, ubuf,
    isem, wsem, ssem, rsem,
):
    gx = lax.axis_index("gx")
    gy = lax.axis_index("gy")
    me = gx * NGY + gy
    y, core, z, x = gx // 2, gx % 2, gy // 4, gy % 4
    loads = [
        pltpu.make_async_copy(a, b, isem.at[k])
        for k, (a, b) in enumerate(
            [(counts, cbuf), (ids, ibuf), (angles, abuf), (upper, ubuf)]
            + [(resid, fl.at[pl.ds(0, 128)])]
            + [(coords.at[d], fl.at[pl.ds(FIELD * (1 + d), 128)]) for d in range(3)]
        )
    ]
    fetches = [
        pltpu.make_async_copy(a, b, wsem.at[k])
        for k, (a, b) in enumerate(
            ((wave, wbuf), (moduli, mbuf), (grad, gbuf), (back, bbuf))
        )
    ]
    for load in loads + fetches:
        load.start()
    bar = pltpu.get_barrier_semaphore()

    near_x = [(x + far_first(m)) % 4 for m in range(4)]
    near_c = [(core + 1 - m) % 2 for m in range(2)]
    offset = [near_c[m % 2] * NGY + near_x[m // 2] for m in range(8)]

    def peers(j, last):
        ty = 2 * ((y + far_first(j // 4)) % 4)
        tz = 4 * ((z + far_first(j % 4)) % 4)
        origin = ty * NGY + tz
        for m in range(7 if last else 8):
            yield m, origin + offset[m], ty + near_c[m % 2], tz + near_x[m // 2]

    def greet(j, last):
        for _, _, tgx, tgy in peers(j, last):
            pl.semaphore_signal(bar, inc=1, device_id=(tgx, tgy), device_id_type=MESH)

    def greet_eight(j, carry):
        greet(j, False)
        return carry

    lax.fori_loop(0, 15, greet_eight, 0)
    greet(15, True)
    for load in loads:
        load.wait()

    sin_a, cos_a = sin_cos(abuf[pl.ds(0, 128, stride=2), :])
    sin_d, cos_d = sin_cos(abuf[pl.ds(1, 128, stride=2), :])
    fl[FIELD * 4 : FIELD * 4 + 128, :] = cos_a * cos_d
    fl[FIELD * 5 : FIELD * 5 + 128, :] = sin_a * cos_d
    fl[FIELD * 6 : FIELD * 6 + 128, :] = sin_d
    limit = jnp.transpose(jnp.broadcast_to(cbuf[...].astype(F32), (128, 128)))
    slot = lax.broadcasted_iota(jnp.int32, (128, 128), 1).astype(F32)
    num = ibuf[...].astype(F32)
    fl[FIELD * 7 : FIELD * 7 + 128, :] = num + 1.0
    up = ubuf[...]
    ones = jnp.ones((128, 128), BF16)

    def columns_of(col):
        masks = [(col == float(w)).astype(F32).astype(BF16) for w in range(4)]
        return jnp.concatenate(masks, axis=0)

    colf = jnp.where(slot < limit, jnp.floor(num * (1.0 / 256.0)), -1.0)
    stacked = columns_of(colf)
    prefix = lax.dot_general(stacked, up, NN, preferred_element_type=F32)
    total = lax.dot_general(stacked, ones, NN, preferred_element_type=F32)
    start = jnp.zeros((128, 128), F32)
    pos = jnp.full((128, 128), -1.0, F32)
    for w in range(4):
        rows = slice(128 * w, 128 * w + 128)
        pos = jnp.where(colf == float(w), prefix[rows] + start, pos)
        start = start + total[rows]
    pos_s[...] = pos
    lane_row = lax.broadcasted_iota(jnp.int32, (128, 128), 0).astype(F32)

    def sort_some(h, carry):
        for k in range(16):
            t = h * 16 + k
            f = fl[pl.ds(t, 8, stride=FIELD), :]
            hi = f.astype(BF16).astype(F32)
            mid = (f - hi).astype(BF16).astype(F32)
            lo = f - hi - mid
            perm = jnp.where(lane_row == pos_s[pl.ds(t, 1), :], 1.0, 0.0).astype(BF16)
            got = lax.dot_general(
                jnp.concatenate([hi, mid, lo], axis=0).astype(BF16),
                perm,
                NT,
                preferred_element_type=F32,
            )
            outgo[t] = got[0:8] + got[8:16] + got[16:24]
        return carry

    lax.fori_loop(0, 8, sort_some, 0)
    stage[NDEV - 1] = outgo[me]
    pl.semaphore_wait(bar, NDEV - 1)

    def send(j, last):
        for m, target, tgx, tgy in peers(j, last):
            pltpu.make_async_remote_copy(
                src_ref=outgo.at[target],
                dst_ref=stage.at[j * 8 + m],
                send_sem=ssem,
                recv_sem=rsem,
                device_id=(tgx, tgy),
                device_id_type=MESH,
            ).start()

    def send_eight(j, carry):
        send(j, False)
        return carry

    lax.fori_loop(0, 15, send_eight, 0)
    send(15, True)
    for fetch in fetches:
        fetch.wait()

    def column(w, carry):
        cx = w // 2
        cy = w % 2
        lam = mbuf[w, 0:1, :]
        mu = mbuf[w, 1:2, :]
        grads = []
        for i in range(3):
            start = (cx * 3 + i) * 500 + cy
            u = jnp.concatenate(
                [wbuf[pl.ds(start + 2 * h, 125, stride=4), :] for h in range(2)], axis=1
            )
            u = jnp.concatenate([u, jnp.zeros((3, 256), F32)], axis=0)
            hi, lo = split(u)
            grads.append(
                lax.dot_general(
                    gbuf[...],
                    jnp.concatenate([hi, hi, lo], axis=0),
                    NN,
                    preferred_element_type=F32,
                )
            )
        g = [[grads[i][128 * j : 128 * j + 128] for j in range(3)] for i in range(3)]
        ldiv = lam * (g[0][0] + g[1][1] + g[2][2])
        parts = {}
        for i in range(3):
            for j in range(i, 3):
                s = mu * (g[i][j] + g[j][i])
                if i == j:
                    s = s + ldiv
                parts[(i, j)] = parts[(j, i)] = split(s)
        for i in range(3):
            hi = [parts[(i, j)][0] for j in range(3)]
            lo = [parts[(i, j)][1] for j in range(3)]
            got = lax.dot_general(
                bbuf[...],
                jnp.concatenate(hi + hi + lo, axis=0),
                NN,
                preferred_element_type=F32,
            )
            for h in range(2):
                at = NST + 192 * h + 48 * w + 16 * i
                stage[pl.ds(at, 16)] = got[:, 128 * h : 128 * h + 128].reshape(16, 8, 128)
        return carry

    lax.fori_loop(0, 4, column, 0)
    drain = pltpu.make_async_remote_copy(
        src_ref=outgo.at[pl.ds(0, NDEV - 1)],
        dst_ref=stage.at[pl.ds(0, NDEV - 1)],
        send_sem=ssem,
        recv_sem=rsem,
        device_id=(gx, (gy + 1) % NGY),
        device_id_type=MESH,
    )
    drain.wait_recv()
    got = stage.reshape(4096, 128)[pl.ds(7, NDEV, stride=8), :]
    received = columns_of(jnp.floor((got - 1.0) * (1.0 / 256.0)))
    total = lax.dot_general(received, ones, NN, preferred_element_type=F32)
    sub = lax.broadcasted_iota(jnp.int32, (16, 128), 0)
    lane16 = lax.broadcasted_iota(jnp.int32, (16, 128), 1)
    pick = jnp.where(lane16 == 0, 1.0, 0.0).astype(BF16)
    words = jnp.zeros((16, 128), jnp.int32)
    first = jnp.zeros((16, 128), jnp.int32)
    for w in range(4):
        n_bf = total[128 * w : 128 * w + 128].astype(BF16)
        n = lax.dot_general(pick, n_bf, NT, preferred_element_type=F32)
        fill = lax.dot_general(n.astype(BF16), up, NN, preferred_element_type=F32)
        n = n.astype(jnp.int32)
        fill = fill.astype(jnp.int32)
        word = ((fill >> 7) + CHUNKS * w) * 16384 + (fill & 127) * 128 + ((fill - first) & 127)
        words = jnp.where(sub == w, word, words)
        words = jnp.where(sub == 4 + w, fill + n, words)
        first = first + n
    table[...] = words
    drain.wait_send()


def exchange(resid, coords, angles, ids, counts, wave, moduli):
    grad, back = operators()
    upper = np.triu(np.ones((128, 128), np.float32), 1)
    return pl.pallas_call(
        exchange_kernel,
        name="exchange",
        out_shape=(
            pltpu.VMEM((512, 8, 128), F32),
            pltpu.VMEM((16, 128), jnp.int32),
        ),
        in_specs=[pl.BlockSpec(memory_space=pltpu.HBM)] * 10,
        out_specs=(pl.BlockSpec(memory_space=pltpu.VMEM),) * 2,
        scratch_shapes=[
            pltpu.VMEM((8 * FIELD, 128), F32),
            pltpu.VMEM((128, 128), F32),
            pltpu.VMEM((NDEV, 8, 128), F32),
            pltpu.VMEM((256, 128), F32),
            pltpu.VMEM((128, 128), jnp.int32),
            pltpu.VMEM((1, 128), jnp.int32),
            pltpu.VMEM((3000, 128), F32),
            pltpu.VMEM((4, 2, 256), F32),
            pltpu.VMEM((384, 384), BF16),
            pltpu.VMEM((128, 1152), BF16),
            pltpu.VMEM((128, 128), BF16),
            pltpu.SemaphoreType.DMA((8,)),
            pltpu.SemaphoreType.DMA((4,)),
            pltpu.SemaphoreType.DMA(()),
            pltpu.SemaphoreType.DMA(()),
        ],
        compiler_params=pltpu.CompilerParams(
            collective_id=0, has_side_effects=True, vmem_limit_bytes=32 * 2**20
        ),
    )(
        *[
            pltpu.with_memory_space_constraint(a, pltpu.HBM)
            for a in (
                resid, coords, angles, ids, counts, wave, moduli,
                jnp.asarray(grad), jnp.asarray(back), jnp.asarray(upper, BF16),
            )
        ]
    )


def node_coefficients():
    points = gll_points()
    poly = np.zeros((5, 5))
    for node in range(5):
        c = np.array([1.0])
        for other in range(5):
            if other != node:
                c = np.convolve(c, np.array([-points[other], 1.0])) / (points[node] - points[other])
        poly[node] = c
    slope = poly[:, 1:] * np.arange(1, 5)[None, :]
    every = np.concatenate([poly, slope], axis=1)
    blocks = []
    for m in range(9):
        blocks.append(np.concatenate([every[:, m], np.zeros(3)]))
    for m in range(9):
        blocks.append(every[np.arange(8) % 5, m])
    return np.repeat(np.concatenate(blocks)[:, None], 128, axis=1)


def fill_lanes(win, at, coef, lhs, h):
    tile_in = win[at]

    def spread(x, k):
        return jnp.broadcast_to(x[k : k + 1, :], (8, 128))

    def across(f):
        return spread(tile_in, f)

    def basis(x, block):
        c = [coef[8 * (block + m) : 8 * (block + m) + 8, :] for m in range(9)]
        val = (((c[4] * x + c[3]) * x + c[2]) * x + c[1]) * x + c[0]
        der = ((c[8] * x + c[7]) * x + c[6]) * x + c[5]
        return val, der

    vx, dx = basis(across(1), 0)
    vy, dy = basis(across(2), 9)
    vz, dz = basis(across(3), 0)
    t = [across(4 + i) for i in range(3)]
    d = [across(0) * t[i] for i in range(3)]
    sub = lax.broadcasted_iota(jnp.int32, (8, 128), 0)

    def by_p(rows, tile):
        row = functools.partial(spread, rows)
        if tile == 0:
            return jnp.where(sub < 5, row(0), row(1))
        if tile == 1:
            return jnp.where(sub < 2, row(1), jnp.where(sub < 7, row(2), row(3)))
        return jnp.where(sub < 4, row(3), row(4))

    def by_q(rows):
        turn = lambda n: pltpu.roll(rows, n, axis=0)
        return [
            rows,
            jnp.where(sub < 5, turn(5), turn(2)),
            jnp.where(sub < 7, turn(7), turn(4)),
        ]

    y1, y2, y3 = vy * t[0], dy * t[1], vy * t[2]
    q1, q2, q3 = by_q(y1), by_q(y2), by_q(y3)
    a, b = [], []
    for tile in range(3):
        px, pd = by_p(vx, tile), by_p(dx, tile)
        a.append(pd * q1[tile] + px * q2[tile])
        b.append(px * q3[tile])

    def last(rows):
        return rows[4:5, :]

    def shape(j):
        if j < 15:
            return a[j % 3] * spread(vz, j // 3) + b[j % 3] * spread(dz, j // 3)
        a4 = last(dx) * last(y1) + last(vx) * last(y2)
        b4 = last(vx) * last(y3)
        return a4 * vz + b4 * dz

    shapes = jnp.concatenate([shape(j) for j in range(16)], axis=0).reshape(16, 8, 128)
    for i in range(3):
        hi, lo = split((shapes * d[i][None]).reshape(128, 128))
        lhs[h, 128 * i : 128 * i + 128, :] = hi
        lhs[2 + h, 128 * i : 128 * i + 128, :] = lo


def inject_kernel(
    big, table, coef, out, xlo, xhi, ylo, yhi, corner,
    acc, win, tabs, lhs_a, lhs_b, tsem,
):
    totab = pltpu.make_async_copy(table, tabs, tsem)
    totab.start()
    totab.wait()

    lane = lax.broadcasted_iota(jnp.int32, (8, 128), 1)
    zero = jnp.zeros((8, 128), F32)

    def place(step, carry):
        for k in range(8):
            t = step * 8 + k
            tile = big[t]
            col = jnp.floor((jnp.broadcast_to(tile[7:8, :], (8, 128)) - 1.0) * (1.0 / 256.0))
            for w in range(4):
                word = tabs[w, t]
                chunk = word >> 14
                begin = (word >> 7) & 127
                run = pltpu.roll(jnp.where(col == float(w), tile, zero), word & 127, axis=1)
                after = lane >= begin
                pltpu.store(win.at[chunk], run, mask=after)
                win[chunk + 1] = jnp.where(after, zero, run)
        return carry

    lax.fori_loop(0, 16, place, 0)
    row = lax.broadcasted_iota(jnp.int32, (256, 128), 0).astype(F32).astype(BF16)
    upto = [0]
    for w in range(4):
        count = tabs[4 + w, 127]
        for k in range(3):
            win[CHUNKS * w + (count + 127) // 128 + k] = zero
        upto.append(upto[-1] + (count + 511) // 512)
    for k in range(4):
        win[4 * CHUNKS + k] = zero

    def chunk_of(u):
        at = u * 4
        for k in range(1, 4):
            at = jnp.where(u >= upto[k], CHUNKS * k + (u - upto[k]) * 4, at)
        return jnp.where(u >= upto[4], 4 * CHUNKS, at)

    def fill(at, lhs):
        for h in range(2):
            fill_lanes(win, at + h, coef, lhs, h)

    def push(at, reg):
        hot = []
        for h in range(2):
            want = jnp.broadcast_to(win[at + h, 7:8, :], (16, 128)) - 1.0
            want = (want - 256.0 * jnp.floor(want * (1.0 / 256.0))).astype(BF16)
            want = jnp.concatenate([want] * 16, axis=0)
            hot.append(jnp.where(row == want, jnp.ones((), BF16), jnp.zeros((), BF16)))
        rhs = jnp.concatenate(hot, axis=1)
        for q in range(2):
            pltpu.matmul_push_rhs(rhs, staging_register=reg, mxu_index=q, transpose=True)

    def use(lhs, reg, accs):
        for q in range(2):
            left = jnp.concatenate([lhs[2 * q], lhs[2 * q + 1]], axis=1)
            pltpu.matmul_acc_lhs(accs[q], left, load_staged_rhs=reg)

    def multiply(*accs):
        for q in range(2):
            pltpu.matmul_pop(accs[q])
        fill(chunk_of(0), lhs_a)
        push(chunk_of(0), 0)
        for w in range(4):

            def two_blocks(step, carry, w=w):
                u = upto[w] + step
                push(CHUNKS * w + 4 * step + 2, 1)
                fill(CHUNKS * w + 4 * step + 2, lhs_b)
                use(lhs_a, 0, accs)
                use(lhs_b, 1, accs)
                fill(chunk_of(u + 1), lhs_a)
                push(chunk_of(u + 1), 0)
                return carry

            lax.fori_loop(0, upto[w + 1] - upto[w], two_blocks, 0)
            if w == 3:
                use(lhs_a, 0, accs)
            total = pltpu.matmul_pop(accs[0]) + pltpu.matmul_pop(accs[1])
            for h in range(2):
                at = NST + 192 * h + 48 * w
                acc[384 * w : 384 * w + 384, 128 * h : 128 * h + 128] = (
                    total[:, 128 * h : 128 * h + 128] + big[at : at + 48].reshape(384, 128)
                )

    pl.run_scoped(multiply, pltpu.ACC(0)((384, 256), F32), pltpu.ACC(1)((384, 256), F32))

    lane2 = lax.broadcasted_iota(jnp.int32, (8, 256), 1)
    for w in range(4):
        cx, cy = w // 2, w % 2
        for i in range(3):
            base = 384 * w + 128 * i
            g = [acc[base + 24 * r : base + 24 * r + 24, :] for r in range(5)]
            tail = acc[base + 120 : base + 128, :]
            groups = [g[0], tail[0:1, :]], [g[4], tail[4:5, :]]
            lows, highs = [], []
            for a, b in zip(*groups):
                ln = lax.broadcasted_iota(jnp.int32, a.shape, 1)
                lows.append(a + jnp.where(ln == 0, 0.0, pltpu.roll(b, 1, axis=1)))
                highs.append(b + jnp.where(ln == 255, 0.0, pltpu.roll(a, 255, axis=1)))
            main = [lows[0], g[1], g[2], g[3], highs[0]]
            last = [lows[1], tail[1:2, :], tail[2:3, :], tail[3:4, :], highs[1]]
            origin = (cx * 3 + i) * 500 + cy
            for r in range(5):
                for h in range(2):
                    cols = slice(128 * h, 128 * h + 128)
                    at = origin + 4 * r + 2 * h
                    out[pl.ds(at, 24, stride=20), :] = main[r][:, cols]
                    out[pl.ds(at + 480, 1), :] = last[r][:, cols]
    for i in range(3):
        a = out[i * 500 + 400 : i * 500 + 500, :]
        b = out[(3 + i) * 500 : (3 + i) * 500 + 100, :]
        out[i * 500 + 400 : i * 500 + 500, :] = a + b
        out[(3 + i) * 500 : (3 + i) * 500 + 100, :] = a + b
    for c in range(6):
        for p in range(5):
            high = pl.ds(c * 500 + 100 * p + 80, 10, stride=2)
            low = pl.ds(c * 500 + 100 * p + 1, 10, stride=2)
            both = out[high, :] + out[low, :]
            out[high, :] = both
            out[low, :] = both
    for i in range(3):
        xlo[100 * i : 100 * i + 100, :] = out[i * 500 : i * 500 + 100, :]
        xhi[100 * i : 100 * i + 100, :] = out[(3 + i) * 500 + 400 : (3 + i) * 500 + 500, :]
    for i in range(3):
        for c in range(9):
            cx, p = (0, c) if c < 4 else (1, c - 4)
            origin = (cx * 3 + i) * 500 + 100 * p
            at = 9 * (9 * i + c)
            for face, shift in ((ylo, 0), (yhi, 81)):
                face[at : at + 8, :] = out[pl.ds(origin + shift, 8, stride=2), :]
                face[at + 8 : at + 9, :] = out[origin + shift + 18 : origin + shift + 19, :]
    for cx in range(2):
        for cy in range(2):
            for i in range(3):
                start = (cx * 3 + i) * 500 + 400 * cx + 80 * cy + cy
                corner[2 * cx + cy, 10 * i : 10 * i + 10, :] = out[pl.ds(start, 10, stride=2), :]


def inject(big, table):
    vm = pl.BlockSpec(memory_space=pltpu.VMEM)
    face = jax.ShapeDtypeStruct((304, 128), F32)
    side = jax.ShapeDtypeStruct((248, 128), F32)
    return pl.pallas_call(
        inject_kernel,
        name="inject",
        out_shape=(
            jax.ShapeDtypeStruct((3000, 128), F32),
            face, face, side, side,
            jax.ShapeDtypeStruct((4, 32, 128), F32),
        ),
        in_specs=[vm] * 3,
        out_specs=(vm,) * 6,
        scratch_shapes=[
            pltpu.VMEM((1536, 256), F32),
            pltpu.VMEM((4 * CHUNKS + 4, 8, 128), F32),
            pltpu.SMEM((16, 128), jnp.int32),
            pltpu.VMEM((4, 384, 128), BF16),
            pltpu.VMEM((4, 384, 128), BF16),
            pltpu.SemaphoreType.DMA(()),
        ],
        compiler_params=pltpu.CompilerParams(vmem_limit_bytes=32 * 2**20),
    )(big, table, jnp.asarray(node_coefficients(), F32))


SIDES = [(-1, 0), (1, 0), (0, -1), (0, 1), (-1, -1), (-1, 1), (1, -1), (1, 1)]


def there(side, gx, gy):
    ok = None
    for d, g, n in ((side[0], gx, NGX), (side[1], gy, NGY)):
        if d:
            c = (g + d >= 0) & (g + d < n)
            ok = c if ok is None else ok & c
    return ok


def halo_kernel(local, xlo, xhi, ylo, yhi, corner, out, gxlo, gxhi, gylo, gyhi, gcorner, ssem, rsem):
    gx = lax.axis_index("gx")
    gy = lax.axis_index("gy")
    bar = pltpu.get_barrier_semaphore()
    for side in SIDES:
        @pl.when(there(side, gx, gy))
        def _(side=side):
            pl.semaphore_signal(
                bar, inc=1, device_id=(gx + side[0], gy + side[1]), device_id_type=MESH
            )
    nx = (gx > 0).astype(jnp.int32) + (gx < NGX - 1).astype(jnp.int32)
    ny = (gy > 0).astype(jnp.int32) + (gy < NGY - 1).astype(jnp.int32)
    pl.semaphore_wait(bar, (nx + 1) * (ny + 1) - 1)

    src = [xlo, xhi, ylo, yhi] + [corner.at[k] for k in range(4)]
    dst = [gxhi, gxlo, gyhi, gylo] + [gcorner.at[3 - k] for k in range(4)]

    def copy(k):
        side = SIDES[k]
        return pltpu.make_async_remote_copy(
            src_ref=src[k],
            dst_ref=dst[k],
            send_sem=ssem.at[k],
            recv_sem=rsem.at[k],
            device_id=(gx + side[0], gy + side[1]),
            device_id_type=MESH,
        )

    for k in (2, 3, 4, 5, 6, 7, 0, 1):
        @pl.when(there(SIDES[k], gx, gy))
        def _(k=k):
            copy(k).start()
    out[...] = local[...]

    def take(k, add):
        @pl.when(there(SIDES[k], gx, gy))
        def _():
            copy([1, 0, 3, 2, 7, 6, 5, 4][k]).wait_recv()
            add()

    def add_xlo():
        for i in range(3):
            out[i * 500 : i * 500 + 100, :] += gxlo[100 * i : 100 * i + 100, :]

    def add_xhi():
        for i in range(3):
            out[(3 + i) * 500 + 400 : (3 + i) * 500 + 500, :] += gxhi[100 * i : 100 * i + 100, :]

    def add_y(ref, shift):
        for i in range(3):
            for c in range(9):
                k = 9 * (9 * i + c)
                first = ref[k : k + 8, :]
                pair = jnp.concatenate([first[0:1, :], first[1:2, :]], axis=1)
                turned = pltpu.roll(pair, 255, axis=1)[:, 0:128]
                for cx, p in ((0, c), (1, c - 4)):
                    if 0 <= p < 5:
                        at = (cx * 3 + i) * 500 + 100 * p + shift
                        out[pl.ds(at, 8, stride=2), :] += first
                        out[at + 16 : at + 17, :] += turned
                        out[at + 18 : at + 19, :] += ref[k + 8 : k + 9, :]

    def add_corner(k):
        cx, cy = k // 2, k % 2
        for i in range(3):
            rows = pl.ds((cx * 3 + i) * 500 + 400 * cx + 80 * cy + cy, 10, stride=2)
            out[rows, :] += gcorner[k, 10 * i : 10 * i + 10, :]

    take(0, add_xlo)
    take(1, add_xhi)
    for k in range(4):
        take(4 + k, functools.partial(add_corner, k))
    take(2, lambda: add_y(gylo, 0))
    take(3, lambda: add_y(gyhi, 81))
    for k in range(8):
        @pl.when(there(SIDES[k], gx, gy))
        def _(k=k):
            copy(k).wait_send()


def halo(local, xlo, xhi, ylo, yhi, corner):
    vm = pl.BlockSpec(memory_space=pltpu.VMEM)
    return pl.pallas_call(
        halo_kernel,
        name="halo",
        out_shape=jax.ShapeDtypeStruct((3000, 128), F32),
        in_specs=[vm] * 6,
        out_specs=vm,
        scratch_shapes=[pltpu.VMEM((n, 128), F32) for n in (304, 304, 248, 248)]
        + [
            pltpu.VMEM((4, 32, 128), F32),
            pltpu.SemaphoreType.DMA((8,)),
            pltpu.SemaphoreType.DMA((8,)),
        ],
        compiler_params=pltpu.CompilerParams(
            collective_id=1, has_side_effects=True, vmem_limit_bytes=16 * 2**20
        ),
    )(local, xlo, xhi, ylo, yhi, corner)


def body(wavefield, moduli, residuals, coords, angles, element_ids, counts):
    wave = wavefield.reshape(2, 2, 3, 125, 2, 128).transpose(0, 2, 3, 4, 1, 5).reshape(3000, 128)
    sorted_slots = exchange(
        residuals[0],
        coords[0].transpose(1, 0, 2),
        angles.reshape(256, 128),
        element_ids[0],
        counts,
        wave,
        moduli.reshape(4, 2, 256),
    )
    out = halo(*inject(*sorted_slots))
    out = out.reshape(2, 3, 125, 2, 2, 128).transpose(0, 4, 1, 2, 3, 5)
    return out.reshape(2, 2, 3, 125, 256)


def solution(mesh):
    in_specs = (
        P("gx", "gy", None, None, None),
        P("gx", "gy", None, None),
        P(("gx", "gy"), None, None),
        P(("gx", "gy"), None, None, None),
        P(("gx", "gy"), None, None, None),
        P(("gx", "gy"), None, None),
        P(("gx", "gy"), None),
    )
    out_specs = P("gx", "gy", None, None, None)
    return jax.shard_map(body, mesh=mesh, in_specs=in_specs, out_specs=out_specs, check_vma=False)
```

```python
import functools
import math

import jax
import jax.numpy as jnp
import numpy as np
from jax import lax
from jax.experimental import pallas as pl
from jax.experimental.pallas import tpu as pltpu
from jax.sharding import PartitionSpec as P

MESH = pl.DeviceIdType.MESH
F32 = jnp.float32
BF16 = jnp.bfloat16
NGX = 8
NGY = 16
NDEV = 128
CHUNKS = 136
NST = 128
FIELD = 136
NT = (((1,), (1,)), ((), ()))
NN = (((1,), (0,)), ((), ()))


def gll_points():
    return np.array([-1.0, -math.sqrt(3.0 / 7.0), 0.0, math.sqrt(3.0 / 7.0), 1.0])


def gll_weights():
    return np.array([0.1, 49.0 / 90.0, 32.0 / 45.0, 49.0 / 90.0, 0.1])


def derivative_table():
    points = gll_points()
    table = np.zeros((5, 5))
    for row in range(5):
        for col in range(5):
            if row == col:
                table[row, col] = sum(
                    (1.0 / (points[col] - points[other]) for other in range(5) if other != col)
                )
            else:
                value = 1.0 / (points[col] - points[row])
                for other in range(5):
                    if other != col and other != row:
                        value = (
                            value * (points[row] - points[other]) / (points[col] - points[other])
                        )
                table[row, col] = value
    return table


def split_np(a):
    hi = np.asarray(a, np.float32).astype(jnp.bfloat16)
    lo = (np.asarray(a, np.float64) - hi.astype(np.float64)).astype(jnp.bfloat16)
    return hi, lo


def row_of(p, q, r):
    pq = 5 * p + q
    return 120 + r if pq == 24 else 24 * r + pq


def operators():
    table = np.asarray(derivative_table(), np.float32).astype(np.float64)
    weight = np.asarray(gll_weights(), np.float32).astype(np.float64)
    grad = np.zeros((3, 128, 128))
    back = np.zeros((3, 128, 128))
    for p in range(5):
        for q in range(5):
            for r in range(5):
                n = 25 * p + 5 * q + r
                for k in range(5):
                    grad[0, n, 25 * k + 5 * q + r] = table[p, k]
                    grad[1, n, 25 * p + 5 * k + r] = table[q, k]
                    grad[2, n, 25 * p + 5 * q + k] = table[r, k]
                w = weight[p] * weight[q] * weight[r]
                for k in range(5):
                    back[0, row_of(k, q, r), n] = -w * table[p, k]
                    back[1, row_of(p, k, r), n] = -w * table[q, k]
                    back[2, row_of(p, q, k), n] = -w * table[r, k]
    ghi, glo = split_np(grad.reshape(384, 128))
    flat = np.concatenate([back[0], back[1], back[2]], axis=1)
    bhi, blo = split_np(flat)
    return np.concatenate([ghi, glo, ghi], axis=1), np.concatenate([bhi, blo, bhi], axis=1)


def split(x):
    hi = x.astype(BF16)
    return hi, (x - hi.astype(F32)).astype(BF16)


def sin_cos(x):
    y = 0.5 * x
    z = y * y
    s = y * (
        1.0
        + z * (-1.0 / 6 + z * (1.0 / 120 + z * (-1.0 / 5040 + z * (1.0 / 362880 + z * (-1.0 / 39916800)))))
    )
    c = 1.0 + z * (
        -0.5
        + z
        * (1.0 / 24 + z * (-1.0 / 720 + z * (1.0 / 40320 + z * (-1.0 / 3628800 + z * (1.0 / 479001600)))))
    )
    return 2.0 * s * c, 1.0 - 2.0 * s * s


def far_first(j):
    return 2 + ((j + 1) // 2) * (1 - 2 * (j % 2))


def exchange_kernel(
    resid, coords, angles, ids, counts, wave, moduli, grad, back, upper,
    stage, table,
    fl, pos_s, outgo, abuf, ibuf, cbuf, wbuf, mbuf, gbuf, bbuf, ubuf,
    isem, wsem, ssem, rsem,
):
    gx = lax.axis_index("gx")
    gy = lax.axis_index("gy")
    me = gx * NGY + gy
    y, core, z, x = gx // 2, gx % 2, gy // 4, gy % 4
    loads = [
        pltpu.make_async_copy(a, b, isem.at[k])
        for k, (a, b) in enumerate(
            [(counts, cbuf), (ids, ibuf), (angles, abuf), (upper, ubuf)]
            + [(resid, fl.at[pl.ds(0, 128)])]
            + [(coords.at[d], fl.at[pl.ds(FIELD * (1 + d), 128)]) for d in range(3)]
        )
    ]
    fetches = [
        pltpu.make_async_copy(a, b, wsem.at[k])
        for k, (a, b) in enumerate(
            ((wave, wbuf), (moduli, mbuf), (grad, gbuf), (back, bbuf))
        )
    ]
    for load in loads + fetches:
        load.start()
    bar = pltpu.get_barrier_semaphore()

    near_x = [(x + far_first(m)) % 4 for m in range(4)]
    near_c = [(core + 1 - m) % 2 for m in range(2)]
    offset = [near_c[m % 2] * NGY + near_x[m // 2] for m in range(8)]

    def peers(j, last):
        ty = 2 * ((y + far_first(j // 4)) % 4)
        tz = 4 * ((z + far_first(j % 4)) % 4)
        origin = ty * NGY + tz
        for m in range(7 if last else 8):
            yield m, origin + offset[m], ty + near_c[m % 2], tz + near_x[m // 2]

    def greet(j, last):
        for _, _, tgx, tgy in peers(j, last):
            pl.semaphore_signal(bar, inc=1, device_id=(tgx, tgy), device_id_type=MESH)

    def greet_eight(j, carry):
        greet(j, False)
        return carry

    lax.fori_loop(0, 15, greet_eight, 0)
    greet(15, True)
    for load in loads:
        load.wait()

    for k in range(2):
        fl[FIELD * (4 + k) : FIELD * (4 + k) + 128, :] = abuf[pl.ds(k, 128, stride=2), :]
    limit = jnp.transpose(jnp.broadcast_to(cbuf[...].astype(F32), (128, 128)))
    slot = lax.broadcasted_iota(jnp.int32, (128, 128), 1).astype(F32)
    num = ibuf[...].astype(F32)
    fl[FIELD * 6 : FIELD * 6 + 128, :] = num + 1.0
    fl[FIELD * 7 : FIELD * 7 + 128, :] = jnp.zeros((128, 128), F32)
    up = ubuf[...]
    ones = jnp.ones((128, 128), BF16)

    def columns_of(col):
        masks = [(col == float(w)).astype(F32).astype(BF16) for w in range(4)]
        return jnp.concatenate(masks, axis=0)

    colf = jnp.where(slot < limit, jnp.floor(num * (1.0 / 256.0)), -1.0)
    stacked = columns_of(colf)
    prefix = lax.dot_general(stacked, up, NN, preferred_element_type=F32)
    total = lax.dot_general(stacked, ones, NN, preferred_element_type=F32)
    start = jnp.zeros((128, 128), F32)
    pos = jnp.full((128, 128), -1.0, F32)
    for w in range(4):
        rows = slice(128 * w, 128 * w + 128)
        pos = jnp.where(colf == float(w), prefix[rows] + start, pos)
        start = start + total[rows]
    pos_s[...] = pos
    lane_row = lax.broadcasted_iota(jnp.int32, (128, 128), 0).astype(F32)

    def sort_some(h, carry):
        for k in range(16):
            t = h * 16 + k
            f = fl[pl.ds(t, 8, stride=FIELD), :]
            hi = f.astype(BF16).astype(F32)
            mid = (f - hi).astype(BF16).astype(F32)
            lo = f - hi - mid
            perm = jnp.where(lane_row == pos_s[pl.ds(t, 1), :], 1.0, 0.0).astype(BF16)
            got = lax.dot_general(
                jnp.concatenate([hi, mid, lo], axis=0).astype(BF16),
                perm,
                NT,
                preferred_element_type=F32,
            )
            outgo[t] = got[0:8] + got[8:16] + got[16:24]
        return carry

    lax.fori_loop(0, 8, sort_some, 0)
    stage[NDEV - 1] = outgo[me]
    pl.semaphore_wait(bar, NDEV - 1)

    def send(j, last):
        for m, target, tgx, tgy in peers(j, last):
            pltpu.make_async_remote_copy(
                src_ref=outgo.at[target, pl.ds(0, 7), :],
                dst_ref=stage.at[j * 8 + m, pl.ds(0, 7), :],
                send_sem=ssem,
                recv_sem=rsem,
                device_id=(tgx, tgy),
                device_id_type=MESH,
            ).start()

    def send_eight(j, carry):
        send(j, False)
        return carry

    lax.fori_loop(0, 15, send_eight, 0)
    send(15, True)
    for fetch in fetches:
        fetch.wait()

    def column(w, carry):
        cx = w // 2
        cy = w % 2
        lam = mbuf[w, 0:1, :]
        mu = mbuf[w, 1:2, :]
        grads = []
        for i in range(3):
            start = (cx * 3 + i) * 500 + cy
            u = jnp.concatenate(
                [wbuf[pl.ds(start + 2 * h, 125, stride=4), :] for h in range(2)], axis=1
            )
            u = jnp.concatenate([u, jnp.zeros((3, 256), F32)], axis=0)
            hi, lo = split(u)
            grads.append(
                lax.dot_general(
                    gbuf[...],
                    jnp.concatenate([hi, hi, lo], axis=0),
                    NN,
                    preferred_element_type=F32,
                )
            )
        g = [[grads[i][128 * j : 128 * j + 128] for j in range(3)] for i in range(3)]
        ldiv = lam * (g[0][0] + g[1][1] + g[2][2])
        parts = {}
        for i in range(3):
            for j in range(i, 3):
                s = mu * (g[i][j] + g[j][i])
                if i == j:
                    s = s + ldiv
                parts[(i, j)] = parts[(j, i)] = split(s)
        for i in range(3):
            hi = [parts[(i, j)][0] for j in range(3)]
            lo = [parts[(i, j)][1] for j in range(3)]
            got = lax.dot_general(
                bbuf[...],
                jnp.concatenate(hi + hi + lo, axis=0),
                NN,
                preferred_element_type=F32,
            )
            for h in range(2):
                at = NST + 192 * h + 48 * w + 16 * i
                stage[pl.ds(at, 16)] = got[:, 128 * h : 128 * h + 128].reshape(16, 8, 128)
        return carry

    lax.fori_loop(0, 4, column, 0)
    drain = pltpu.make_async_remote_copy(
        src_ref=outgo.at[pl.ds(0, NDEV - 1), pl.ds(0, 7), :],
        dst_ref=stage.at[pl.ds(0, NDEV - 1), pl.ds(0, 7), :],
        send_sem=ssem,
        recv_sem=rsem,
        device_id=(gx, (gy + 1) % NGY),
        device_id_type=MESH,
    )
    drain.wait_recv()
    rows = stage.reshape(4096, 128)
    got = rows[pl.ds(6, NDEV, stride=8), :]
    sin_a, cos_a = sin_cos(rows[pl.ds(4, NDEV, stride=8), :])
    sin_d, cos_d = sin_cos(rows[pl.ds(5, NDEV, stride=8), :])
    for k, v in ((4, cos_a * cos_d), (5, sin_a * cos_d), (7, sin_d)):
        rows[pl.ds(k, NDEV, stride=8), :] = v
    received = columns_of(jnp.floor((got - 1.0) * (1.0 / 256.0)))
    sub = lax.broadcasted_iota(jnp.int32, (16, 128), 0)
    words = jnp.zeros((16, 128), jnp.int32)
    first = jnp.zeros((16, 128), jnp.int32)
    for w in range(4):
        n = lax.dot_general(
            jnp.ones((16, 128), BF16), received[128 * w : 128 * w + 128], NT, preferred_element_type=F32
        )
        fill = lax.dot_general(n.astype(BF16), up, NN, preferred_element_type=F32)
        n = n.astype(jnp.int32)
        fill = fill.astype(jnp.int32)
        words = jnp.where(sub == w, (fill - first) & 127, words)
        words = jnp.where(sub == 4 + w, fill & 127, words)
        words = jnp.where(sub == 8 + w, (fill >> 7) + CHUNKS * w, words)
        words = jnp.where(sub == 12 + w, fill + n, words)
        first = first + n
    table[...] = words
    drain.wait_send()


def exchange(resid, coords, angles, ids, counts, wave, moduli):
    grad, back = operators()
    upper = np.triu(np.ones((128, 128), np.float32), 1)
    return pl.pallas_call(
        exchange_kernel,
        name="exchange",
        out_shape=(
            pltpu.VMEM((512, 8, 128), F32),
            pltpu.VMEM((16, 128), jnp.int32),
        ),
        in_specs=[pl.BlockSpec(memory_space=pltpu.HBM)] * 10,
        out_specs=(pl.BlockSpec(memory_space=pltpu.VMEM),) * 2,
        scratch_shapes=[
            pltpu.VMEM((8 * FIELD, 128), F32),
            pltpu.VMEM((128, 128), F32),
            pltpu.VMEM((NDEV, 8, 128), F32),
            pltpu.VMEM((256, 128), F32),
            pltpu.VMEM((128, 128), jnp.int32),
            pltpu.VMEM((1, 128), jnp.int32),
            pltpu.VMEM((3000, 128), F32),
            pltpu.VMEM((4, 2, 256), F32),
            pltpu.VMEM((384, 384), BF16),
            pltpu.VMEM((128, 1152), BF16),
            pltpu.VMEM((128, 128), BF16),
            pltpu.SemaphoreType.DMA((8,)),
            pltpu.SemaphoreType.DMA((4,)),
            pltpu.SemaphoreType.DMA(()),
            pltpu.SemaphoreType.DMA(()),
        ],
        compiler_params=pltpu.CompilerParams(
            collective_id=0, has_side_effects=True, vmem_limit_bytes=32 * 2**20
        ),
    )(
        *[
            pltpu.with_memory_space_constraint(a, pltpu.HBM)
            for a in (
                resid, coords, angles, ids, counts, wave, moduli,
                jnp.asarray(grad), jnp.asarray(back), jnp.asarray(upper, BF16),
            )
        ]
    )


def node_coefficients():
    points = gll_points()
    poly = np.zeros((5, 5))
    for node in range(5):
        c = np.array([1.0])
        for other in range(5):
            if other != node:
                c = np.convolve(c, np.array([-points[other], 1.0])) / (points[node] - points[other])
        poly[node] = c
    slope = poly[:, 1:] * np.arange(1, 5)[None, :]
    every = np.concatenate([poly, slope], axis=1)
    blocks = []
    for m in range(9):
        blocks.append(np.concatenate([every[:, m], np.zeros(3)]))
    for m in range(9):
        blocks.append(every[np.arange(8) % 5, m])
    return np.repeat(np.concatenate(blocks)[:, None], 128, axis=1)


def fill_lanes(win, at, coef, lhs, h):
    tile_in = win[at]

    def spread(x, k):
        return jnp.broadcast_to(x[k : k + 1, :], (8, 128))

    def across(f):
        return spread(tile_in, f)

    def basis(x, block):
        c = [coef[8 * (block + m) : 8 * (block + m) + 8, :] for m in range(9)]
        val = (((c[4] * x + c[3]) * x + c[2]) * x + c[1]) * x + c[0]
        der = ((c[8] * x + c[7]) * x + c[6]) * x + c[5]
        return val, der

    vx, dx = basis(across(1), 0)
    vy, dy = basis(across(2), 9)
    vz, dz = basis(across(3), 0)
    t = [across(i) for i in (4, 5, 7)]
    d = [across(0) * t[i] for i in range(3)]
    sub = lax.broadcasted_iota(jnp.int32, (8, 128), 0)

    def by_p(rows, tile):
        row = functools.partial(spread, rows)
        if tile == 0:
            return jnp.where(sub < 5, row(0), row(1))
        if tile == 1:
            return jnp.where(sub < 2, row(1), jnp.where(sub < 7, row(2), row(3)))
        return jnp.where(sub < 4, row(3), row(4))

    def by_q(rows):
        turn = lambda n: pltpu.roll(rows, n, axis=0)
        return [
            rows,
            jnp.where(sub < 5, turn(5), turn(2)),
            jnp.where(sub < 7, turn(7), turn(4)),
        ]

    y1, y2, y3 = vy * t[0], dy * t[1], vy * t[2]
    q1, q2, q3 = by_q(y1), by_q(y2), by_q(y3)
    a, b = [], []
    for tile in range(3):
        px, pd = by_p(vx, tile), by_p(dx, tile)
        a.append(pd * q1[tile] + px * q2[tile])
        b.append(px * q3[tile])

    def last(rows):
        return rows[4:5, :]

    def shape(j):
        if j < 15:
            return a[j % 3] * spread(vz, j // 3) + b[j % 3] * spread(dz, j // 3)
        a4 = last(dx) * last(y1) + last(vx) * last(y2)
        b4 = last(vx) * last(y3)
        return a4 * vz + b4 * dz

    shapes = jnp.concatenate([shape(j) for j in range(16)], axis=0).reshape(16, 8, 128)
    for i in range(3):
        hi, lo = split((shapes * d[i][None]).reshape(128, 128))
        lhs[h, 128 * i : 128 * i + 128, :] = hi
        lhs[2 + h, 128 * i : 128 * i + 128, :] = lo


def inject_kernel(
    big, table, coef, out, xlo, xhi, ylo, yhi, corner,
    win, tabs, lhs_a, lhs_b, tsem,
):
    totab = pltpu.make_async_copy(table, tabs, tsem)
    totab.start()
    totab.wait()

    lane = lax.broadcasted_iota(jnp.int32, (8, 128), 1)
    zero = jnp.zeros((8, 128), F32)

    def place(step, carry):
        for k in range(8):
            t = step * 8 + k
            tile = big[t]
            col = jnp.floor((jnp.broadcast_to(tile[6:7, :], (8, 128)) - 1.0) * (1.0 / 256.0))
            for w in range(4):
                chunk = tabs[8 + w, t]
                run = pltpu.roll(jnp.where(col == float(w), tile, zero), tabs[w, t], axis=1)
                after = lane >= tabs[4 + w, t]
                pltpu.store(win.at[chunk], run, mask=after)
                win[chunk + 1] = jnp.where(after, zero, run)
        return carry

    lax.fori_loop(0, 16, place, 0)
    row = lax.broadcasted_iota(jnp.int32, (256, 128), 0).astype(F32).astype(BF16)
    upto = [0]
    for w in range(4):
        count = tabs[12 + w, 127]
        for k in range(3):
            win[CHUNKS * w + (count + 127) // 128 + k] = zero
        upto.append(upto[-1] + (count + 511) // 512)
    for k in range(4):
        win[4 * CHUNKS + k] = zero

    def chunk_of(u):
        at = u * 4
        for k in range(1, 4):
            at = jnp.where(u >= upto[k], CHUNKS * k + (u - upto[k]) * 4, at)
        return jnp.where(u >= upto[4], 4 * CHUNKS, at)

    def fill(at, lhs):
        for h in range(2):
            fill_lanes(win, at + h, coef, lhs, h)

    def push(at, reg):
        hot = []
        for h in range(2):
            want = jnp.broadcast_to(win[at + h, 6:7, :], (16, 128)) - 1.0
            want = (want - 256.0 * jnp.floor(want * (1.0 / 256.0))).astype(BF16)
            want = jnp.concatenate([want] * 16, axis=0)
            hot.append(jnp.where(row == want, jnp.ones((), BF16), jnp.zeros((), BF16)))
        rhs = jnp.concatenate(hot, axis=1)
        for q in range(2):
            pltpu.matmul_push_rhs(rhs, staging_register=reg, mxu_index=q, transpose=True)

    def use(lhs, reg, accs):
        for q in range(2):
            left = jnp.concatenate([lhs[2 * q], lhs[2 * q + 1]], axis=1)
            pltpu.matmul_acc_lhs(accs[q], left, load_staged_rhs=reg)

    def settle(w, accs):
        total = pltpu.matmul_pop(accs[0]) + pltpu.matmul_pop(accs[1])
        cx, cy = w // 2, w % 2
        halves = [
            big[NST + 192 * h + 48 * w : NST + 192 * h + 48 * w + 48].reshape(384, 128)
            for h in range(2)
        ]
        total = total + jnp.concatenate(halves, axis=1)
        for i in range(3):
            base = 128 * i
            g = [total[base + 24 * r : base + 24 * r + 24, :] for r in range(5)]
            tail = total[base + 120 : base + 128, :]
            groups = [g[0], tail[0:1, :]], [g[4], tail[4:5, :]]
            lows, highs = [], []
            for a, b in zip(*groups):
                ln = lax.broadcasted_iota(jnp.int32, a.shape, 1)
                lows.append(a + jnp.where(ln == 0, 0.0, pltpu.roll(b, 1, axis=1)))
                highs.append(b + jnp.where(ln == 255, 0.0, pltpu.roll(a, 255, axis=1)))
            main = [lows[0], g[1], g[2], g[3], highs[0]]
            last = [lows[1], tail[1:2, :], tail[2:3, :], tail[3:4, :], highs[1]]
            origin = (cx * 3 + i) * 500 + cy
            for r in range(5):
                for h in range(2):
                    cols = slice(128 * h, 128 * h + 128)
                    at = origin + 4 * r + 2 * h
                    out[pl.ds(at, 24, stride=20), :] = main[r][:, cols]
                    out[pl.ds(at + 480, 1), :] = last[r][:, cols]

    def multiply(*all_accs):
        sets = [(all_accs[0], all_accs[2]), (all_accs[1], all_accs[3])]
        for acc in all_accs:
            pltpu.matmul_pop(acc)
        fill(chunk_of(0), lhs_a)
        push(chunk_of(0), 0)
        for w in range(4):
            accs = sets[w % 2]

            def two_blocks(step, carry, w=w, accs=accs):
                u = upto[w] + step
                push(CHUNKS * w + 4 * step + 2, 1)
                fill(CHUNKS * w + 4 * step + 2, lhs_b)
                use(lhs_a, 0, accs)
                use(lhs_b, 1, accs)
                fill(chunk_of(u + 1), lhs_a)
                push(chunk_of(u + 1), 0)
                return carry

            lax.fori_loop(0, upto[w + 1] - upto[w], two_blocks, 0)
            if w == 3:
                use(lhs_a, 0, accs)
            if w > 0:
                settle(w - 1, sets[(w - 1) % 2])
        settle(3, sets[1])

    pl.run_scoped(multiply, *[pltpu.ACC(q)((384, 256), F32) for q in (0, 0, 1, 1)])

    for i in range(3):
        a = out[i * 500 + 400 : i * 500 + 500, :]
        b = out[(3 + i) * 500 : (3 + i) * 500 + 100, :]
        out[i * 500 + 400 : i * 500 + 500, :] = a + b
        out[(3 + i) * 500 : (3 + i) * 500 + 100, :] = a + b
    for c in range(6):
        for p in range(5):
            high = pl.ds(c * 500 + 100 * p + 80, 10, stride=2)
            low = pl.ds(c * 500 + 100 * p + 1, 10, stride=2)
            both = out[high, :] + out[low, :]
            out[high, :] = both
            out[low, :] = both
    for i in range(3):
        xlo[100 * i : 100 * i + 100, :] = out[i * 500 : i * 500 + 100, :]
        xhi[100 * i : 100 * i + 100, :] = out[(3 + i) * 500 + 400 : (3 + i) * 500 + 500, :]
    for i in range(3):
        for c in range(9):
            cx, p = (0, c) if c < 4 else (1, c - 4)
            origin = (cx * 3 + i) * 500 + 100 * p
            at = 9 * (9 * i + c)
            for face, shift in ((ylo, 0), (yhi, 81)):
                face[at : at + 8, :] = out[pl.ds(origin + shift, 8, stride=2), :]
                face[at + 8 : at + 9, :] = out[origin + shift + 18 : origin + shift + 19, :]
    for cx in range(2):
        for cy in range(2):
            for i in range(3):
                start = (cx * 3 + i) * 500 + 400 * cx + 80 * cy + cy
                corner[2 * cx + cy, 10 * i : 10 * i + 10, :] = out[pl.ds(start, 10, stride=2), :]


def inject(big, table):
    vm = pl.BlockSpec(memory_space=pltpu.VMEM)
    face = jax.ShapeDtypeStruct((304, 128), F32)
    side = jax.ShapeDtypeStruct((248, 128), F32)
    return pl.pallas_call(
        inject_kernel,
        name="inject",
        out_shape=(
            jax.ShapeDtypeStruct((3000, 128), F32),
            face, face, side, side,
            jax.ShapeDtypeStruct((4, 32, 128), F32),
        ),
        in_specs=[vm] * 3,
        out_specs=(vm,) * 6,
        scratch_shapes=[
            pltpu.VMEM((4 * CHUNKS + 4, 8, 128), F32),
            pltpu.SMEM((16, 128), jnp.int32),
            pltpu.VMEM((4, 384, 128), BF16),
            pltpu.VMEM((4, 384, 128), BF16),
            pltpu.SemaphoreType.DMA(()),
        ],
        compiler_params=pltpu.CompilerParams(vmem_limit_bytes=32 * 2**20),
    )(big, table, jnp.asarray(node_coefficients(), F32))


SIDES = [(-1, 0), (1, 0), (0, -1), (0, 1), (-1, -1), (-1, 1), (1, -1), (1, 1)]


def there(side, gx, gy):
    ok = None
    for d, g, n in ((side[0], gx, NGX), (side[1], gy, NGY)):
        if d:
            c = (g + d >= 0) & (g + d < n)
            ok = c if ok is None else ok & c
    return ok


def halo_kernel(local, xlo, xhi, ylo, yhi, corner, out, gxlo, gxhi, gylo, gyhi, gcorner, ssem, rsem):
    gx = lax.axis_index("gx")
    gy = lax.axis_index("gy")
    bar = pltpu.get_barrier_semaphore()
    for side in SIDES:
        @pl.when(there(side, gx, gy))
        def _(side=side):
            pl.semaphore_signal(
                bar, inc=1, device_id=(gx + side[0], gy + side[1]), device_id_type=MESH
            )
    nx = (gx > 0).astype(jnp.int32) + (gx < NGX - 1).astype(jnp.int32)
    ny = (gy > 0).astype(jnp.int32) + (gy < NGY - 1).astype(jnp.int32)
    pl.semaphore_wait(bar, (nx + 1) * (ny + 1) - 1)

    src = [xlo, xhi, ylo, yhi] + [corner.at[k] for k in range(4)]
    dst = [gxhi, gxlo, gyhi, gylo] + [gcorner.at[3 - k] for k in range(4)]

    def copy(k):
        side = SIDES[k]
        return pltpu.make_async_remote_copy(
            src_ref=src[k],
            dst_ref=dst[k],
            send_sem=ssem.at[k],
            recv_sem=rsem.at[k],
            device_id=(gx + side[0], gy + side[1]),
            device_id_type=MESH,
        )

    for k in (2, 3, 4, 5, 6, 7, 0, 1):
        @pl.when(there(SIDES[k], gx, gy))
        def _(k=k):
            copy(k).start()
    out[...] = local[...]

    def take(k, add):
        @pl.when(there(SIDES[k], gx, gy))
        def _():
            copy([1, 0, 3, 2, 7, 6, 5, 4][k]).wait_recv()
            add()

    def add_xlo():
        for i in range(3):
            out[i * 500 : i * 500 + 100, :] += gxlo[100 * i : 100 * i + 100, :]

    def add_xhi():
        for i in range(3):
            out[(3 + i) * 500 + 400 : (3 + i) * 500 + 500, :] += gxhi[100 * i : 100 * i + 100, :]

    def add_y(ref, shift):
        for i in range(3):
            for c in range(9):
                k = 9 * (9 * i + c)
                first = ref[k : k + 8, :]
                pair = jnp.concatenate([first[0:1, :], first[1:2, :]], axis=1)
                turned = pltpu.roll(pair, 255, axis=1)[:, 0:128]
                for cx, p in ((0, c), (1, c - 4)):
                    if 0 <= p < 5:
                        at = (cx * 3 + i) * 500 + 100 * p + shift
                        out[pl.ds(at, 8, stride=2), :] += first
                        out[at + 16 : at + 17, :] += turned
                        out[at + 18 : at + 19, :] += ref[k + 8 : k + 9, :]

    def add_corner(k):
        cx, cy = k // 2, k % 2
        for i in range(3):
            rows = pl.ds((cx * 3 + i) * 500 + 400 * cx + 80 * cy + cy, 10, stride=2)
            out[rows, :] += gcorner[k, 10 * i : 10 * i + 10, :]

    take(0, add_xlo)
    take(1, add_xhi)
    for k in range(4):
        take(4 + k, functools.partial(add_corner, k))
    take(2, lambda: add_y(gylo, 0))
    take(3, lambda: add_y(gyhi, 81))
    for k in range(8):
        @pl.when(there(SIDES[k], gx, gy))
        def _(k=k):
            copy(k).wait_send()


def halo(local, xlo, xhi, ylo, yhi, corner):
    vm = pl.BlockSpec(memory_space=pltpu.VMEM)
    return pl.pallas_call(
        halo_kernel,
        name="halo",
        out_shape=jax.ShapeDtypeStruct((3000, 128), F32),
        in_specs=[vm] * 6,
        out_specs=vm,
        scratch_shapes=[pltpu.VMEM((n, 128), F32) for n in (304, 304, 248, 248)]
        + [
            pltpu.VMEM((4, 32, 128), F32),
            pltpu.SemaphoreType.DMA((8,)),
            pltpu.SemaphoreType.DMA((8,)),
        ],
        compiler_params=pltpu.CompilerParams(
            collective_id=1, has_side_effects=True, vmem_limit_bytes=16 * 2**20
        ),
    )(local, xlo, xhi, ylo, yhi, corner)


def body(wavefield, moduli, residuals, coords, angles, element_ids, counts):
    wave = wavefield.reshape(2, 2, 3, 125, 2, 128).transpose(0, 2, 3, 4, 1, 5).reshape(3000, 128)
    sorted_slots = exchange(
        residuals[0],
        coords[0].transpose(1, 0, 2),
        angles.reshape(256, 128),
        element_ids[0],
        counts,
        wave,
        moduli.reshape(4, 2, 256),
    )
    out = halo(*inject(*sorted_slots))
    out = out.reshape(2, 3, 125, 2, 2, 128).transpose(0, 4, 1, 2, 3, 5)
    return out.reshape(2, 2, 3, 125, 256)


def solution(mesh):
    in_specs = (
        P("gx", "gy", None, None, None),
        P("gx", "gy", None, None),
        P(("gx", "gy"), None, None),
        P(("gx", "gy"), None, None, None),
        P(("gx", "gy"), None, None, None),
        P(("gx", "gy"), None, None),
        P(("gx", "gy"), None),
    )
    out_specs = P("gx", "gy", None, None, None)
    return jax.shard_map(body, mesh=mesh, in_specs=in_specs, out_specs=out_specs, check_vma=False)
```

```python
import functools
import math

import jax
import jax.numpy as jnp
import numpy as np
from jax import lax
from jax.experimental import pallas as pl
from jax.experimental.pallas import tpu as pltpu
from jax.sharding import PartitionSpec as P

MESH = pl.DeviceIdType.MESH
F32 = jnp.float32
BF16 = jnp.bfloat16
NGX = 8
NGY = 16
NDEV = 128
CHUNKS = 136
NST = 128
FIELD = 136
NT = (((1,), (1,)), ((), ()))
NN = (((1,), (0,)), ((), ()))


def gll_points():
    return np.array([-1.0, -math.sqrt(3.0 / 7.0), 0.0, math.sqrt(3.0 / 7.0), 1.0])


def gll_weights():
    return np.array([0.1, 49.0 / 90.0, 32.0 / 45.0, 49.0 / 90.0, 0.1])


def derivative_table():
    points = gll_points()
    table = np.zeros((5, 5))
    for row in range(5):
        for col in range(5):
            if row == col:
                table[row, col] = sum(
                    (1.0 / (points[col] - points[other]) for other in range(5) if other != col)
                )
            else:
                value = 1.0 / (points[col] - points[row])
                for other in range(5):
                    if other != col and other != row:
                        value = (
                            value * (points[row] - points[other]) / (points[col] - points[other])
                        )
                table[row, col] = value
    return table


def split_np(a):
    hi = np.asarray(a, np.float32).astype(jnp.bfloat16)
    lo = (np.asarray(a, np.float64) - hi.astype(np.float64)).astype(jnp.bfloat16)
    return hi, lo


def row_of(p, q, r):
    pq = 5 * p + q
    return 120 + r if pq == 24 else 24 * r + pq


def operators():
    table = np.asarray(derivative_table(), np.float32).astype(np.float64)
    weight = np.asarray(gll_weights(), np.float32).astype(np.float64)
    grad = np.zeros((3, 128, 128))
    back = np.zeros((3, 128, 128))
    for p in range(5):
        for q in range(5):
            for r in range(5):
                n = 25 * p + 5 * q + r
                for k in range(5):
                    grad[0, n, 25 * k + 5 * q + r] = table[p, k]
                    grad[1, n, 25 * p + 5 * k + r] = table[q, k]
                    grad[2, n, 25 * p + 5 * q + k] = table[r, k]
                w = weight[p] * weight[q] * weight[r]
                for k in range(5):
                    back[0, row_of(k, q, r), n] = -w * table[p, k]
                    back[1, row_of(p, k, r), n] = -w * table[q, k]
                    back[2, row_of(p, q, k), n] = -w * table[r, k]
    ghi, glo = split_np(grad.reshape(384, 128))
    flat = np.concatenate([back[0], back[1], back[2]], axis=1)
    bhi, blo = split_np(flat)
    return np.concatenate([ghi, glo, ghi], axis=1), np.concatenate([bhi, blo, bhi], axis=1)


def split(x):
    hi = x.astype(BF16)
    return hi, (x - hi.astype(F32)).astype(BF16)


def sin_cos(x):
    y = 0.5 * x
    z = y * y
    s = y * (
        1.0
        + z * (-1.0 / 6 + z * (1.0 / 120 + z * (-1.0 / 5040 + z * (1.0 / 362880 + z * (-1.0 / 39916800)))))
    )
    c = 1.0 + z * (
        -0.5
        + z
        * (1.0 / 24 + z * (-1.0 / 720 + z * (1.0 / 40320 + z * (-1.0 / 3628800 + z * (1.0 / 479001600)))))
    )
    return 2.0 * s * c, 1.0 - 2.0 * s * s


def far_first(j):
    return 2 + ((j + 1) // 2) * (1 - 2 * (j % 2))


def exchange_kernel(
    resid, coords, angles, ids, counts, wave, moduli, grad, back, upper,
    stage, table,
    fl, pos_s, outgo, abuf, ibuf, cbuf, wbuf, mbuf, gbuf, bbuf, ubuf,
    isem, wsem, ssem, rsem,
):
    gx = lax.axis_index("gx")
    gy = lax.axis_index("gy")
    me = gx * NGY + gy
    y, core, z, x = gx // 2, gx % 2, gy // 4, gy % 4
    loads = [
        pltpu.make_async_copy(a, b, isem.at[k])
        for k, (a, b) in enumerate(
            [(counts, cbuf), (ids, ibuf), (angles, abuf), (upper, ubuf)]
            + [(resid, fl.at[pl.ds(0, 128)])]
            + [(coords.at[d], fl.at[pl.ds(FIELD * (1 + d), 128)]) for d in range(3)]
        )
    ]
    fetches = [
        pltpu.make_async_copy(a, b, wsem.at[k])
        for k, (a, b) in enumerate(
            ((wave, wbuf), (moduli, mbuf), (grad, gbuf), (back, bbuf))
        )
    ]
    for load in loads + fetches:
        load.start()
    bar = pltpu.get_barrier_semaphore()

    near_x = [(x + far_first(m)) % 4 for m in range(4)]
    near_c = [(core + 1 - m) % 2 for m in range(2)]
    offset = [near_c[m % 2] * NGY + near_x[m // 2] for m in range(8)]

    def peers(j, last):
        ty = 2 * ((y + far_first(j % 4)) % 4)
        tz = 4 * ((z + far_first(j // 4)) % 4)
        origin = ty * NGY + tz
        for m in range(7 if last else 8):
            yield m, origin + offset[m], ty + near_c[m % 2], tz + near_x[m // 2]

    def greet(j, last):
        for _, _, tgx, tgy in peers(j, last):
            pl.semaphore_signal(bar, inc=1, device_id=(tgx, tgy), device_id_type=MESH)

    def greet_eight(j, carry):
        greet(j, False)
        return carry

    lax.fori_loop(0, 15, greet_eight, 0)
    greet(15, True)
    for load in loads:
        load.wait()

    for k in range(2):
        fl[FIELD * (4 + k) : FIELD * (4 + k) + 128, :] = abuf[pl.ds(k, 128, stride=2), :]
    limit = jnp.transpose(jnp.broadcast_to(cbuf[...].astype(F32), (128, 128)))
    slot = lax.broadcasted_iota(jnp.int32, (128, 128), 1).astype(F32)
    num = ibuf[...].astype(F32)
    fl[FIELD * 6 : FIELD * 6 + 128, :] = num + 1.0
    fl[FIELD * 7 : FIELD * 7 + 128, :] = jnp.zeros((128, 128), F32)
    up = ubuf[...]
    ones = jnp.ones((128, 128), BF16)

    def columns_of(col):
        masks = [(col == float(w)).astype(F32).astype(BF16) for w in range(4)]
        return jnp.concatenate(masks, axis=0)

    colf = jnp.where(slot < limit, jnp.floor(num * (1.0 / 256.0)), -1.0)
    stacked = columns_of(colf)
    prefix = lax.dot_general(stacked, up, NN, preferred_element_type=F32)
    total = lax.dot_general(stacked, ones, NN, preferred_element_type=F32)
    start = jnp.zeros((128, 128), F32)
    pos = jnp.full((128, 128), -1.0, F32)
    for w in range(4):
        rows = slice(128 * w, 128 * w + 128)
        pos = jnp.where(colf == float(w), prefix[rows] + start, pos)
        start = start + total[rows]
    pos_s[...] = pos
    lane_row = lax.broadcasted_iota(jnp.int32, (128, 128), 0).astype(F32)

    def sort_some(h, carry):
        for k in range(16):
            t = h * 16 + k
            f = fl[pl.ds(t, 8, stride=FIELD), :]
            hi = f.astype(BF16).astype(F32)
            mid = (f - hi).astype(BF16).astype(F32)
            lo = f - hi - mid
            perm = jnp.where(lane_row == pos_s[pl.ds(t, 1), :], 1.0, 0.0).astype(BF16)
            got = lax.dot_general(
                jnp.concatenate([hi, mid, lo], axis=0).astype(BF16),
                perm,
                NT,
                preferred_element_type=F32,
            )
            outgo[t] = got[0:8] + got[8:16] + got[16:24]
        return carry

    lax.fori_loop(0, 8, sort_some, 0)
    stage[NDEV - 1] = outgo[me]
    pl.semaphore_wait(bar, NDEV - 1)

    def send(j, last):
        for m, target, tgx, tgy in peers(j, last):
            pltpu.make_async_remote_copy(
                src_ref=outgo.at[target, pl.ds(0, 7), :],
                dst_ref=stage.at[j * 8 + m, pl.ds(0, 7), :],
                send_sem=ssem,
                recv_sem=rsem,
                device_id=(tgx, tgy),
                device_id_type=MESH,
            ).start()

    def send_eight(j, carry):
        send(j, False)
        return carry

    lax.fori_loop(0, 15, send_eight, 0)
    send(15, True)
    for fetch in fetches:
        fetch.wait()

    def column(w, carry):
        cx = w // 2
        cy = w % 2
        lam = mbuf[w, 0:1, :]
        mu = mbuf[w, 1:2, :]
        grads = []
        for i in range(3):
            start = (cx * 3 + i) * 500 + cy
            u = jnp.concatenate(
                [wbuf[pl.ds(start + 2 * h, 125, stride=4), :] for h in range(2)], axis=1
            )
            u = jnp.concatenate([u, jnp.zeros((3, 256), F32)], axis=0)
            hi, lo = split(u)
            grads.append(
                lax.dot_general(
                    gbuf[...],
                    jnp.concatenate([hi, hi, lo], axis=0),
                    NN,
                    preferred_element_type=F32,
                )
            )
        g = [[grads[i][128 * j : 128 * j + 128] for j in range(3)] for i in range(3)]
        ldiv = lam * (g[0][0] + g[1][1] + g[2][2])
        parts = {}
        for i in range(3):
            for j in range(i, 3):
                s = mu * (g[i][j] + g[j][i])
                if i == j:
                    s = s + ldiv
                parts[(i, j)] = parts[(j, i)] = split(s)
        for i in range(3):
            hi = [parts[(i, j)][0] for j in range(3)]
            lo = [parts[(i, j)][1] for j in range(3)]
            got = lax.dot_general(
                bbuf[...],
                jnp.concatenate(hi + hi + lo, axis=0),
                NN,
                preferred_element_type=F32,
            )
            for h in range(2):
                at = NST + 192 * h + 48 * w + 16 * i
                stage[pl.ds(at, 16)] = got[:, 128 * h : 128 * h + 128].reshape(16, 8, 128)
        return carry

    lax.fori_loop(0, 4, column, 0)
    drain = pltpu.make_async_remote_copy(
        src_ref=outgo.at[pl.ds(0, NDEV - 1), pl.ds(0, 7), :],
        dst_ref=stage.at[pl.ds(0, NDEV - 1), pl.ds(0, 7), :],
        send_sem=ssem,
        recv_sem=rsem,
        device_id=(gx, (gy + 1) % NGY),
        device_id_type=MESH,
    )
    drain.wait_recv()
    rows = stage.reshape(4096, 128)
    got = rows[pl.ds(6, NDEV, stride=8), :]
    sin_a, cos_a = sin_cos(rows[pl.ds(4, NDEV, stride=8), :])
    sin_d, cos_d = sin_cos(rows[pl.ds(5, NDEV, stride=8), :])
    for k, v in ((4, cos_a * cos_d), (5, sin_a * cos_d), (7, sin_d)):
        rows[pl.ds(k, NDEV, stride=8), :] = v
    received = columns_of(jnp.floor((got - 1.0) * (1.0 / 256.0)))
    sub = lax.broadcasted_iota(jnp.int32, (16, 128), 0)
    words = jnp.zeros((16, 128), jnp.int32)
    first = jnp.zeros((16, 128), jnp.int32)
    for w in range(4):
        n = lax.dot_general(
            jnp.ones((16, 128), BF16), received[128 * w : 128 * w + 128], NT, preferred_element_type=F32
        )
        fill = lax.dot_general(n.astype(BF16), up, NN, preferred_element_type=F32)
        n = n.astype(jnp.int32)
        fill = fill.astype(jnp.int32)
        words = jnp.where(sub == w, (fill - first) & 127, words)
        words = jnp.where(sub == 4 + w, fill & 127, words)
        words = jnp.where(sub == 8 + w, (fill >> 7) + CHUNKS * w, words)
        words = jnp.where(sub == 12 + w, fill + n, words)
        first = first + n
    table[...] = words
    drain.wait_send()


def exchange(resid, coords, angles, ids, counts, wave, moduli):
    grad, back = operators()
    upper = np.triu(np.ones((128, 128), np.float32), 1)
    return pl.pallas_call(
        exchange_kernel,
        name="exchange",
        out_shape=(
            pltpu.VMEM((512, 8, 128), F32),
            pltpu.VMEM((16, 128), jnp.int32),
        ),
        in_specs=[pl.BlockSpec(memory_space=pltpu.HBM)] * 10,
        out_specs=(pl.BlockSpec(memory_space=pltpu.VMEM),) * 2,
        scratch_shapes=[
            pltpu.VMEM((8 * FIELD, 128), F32),
            pltpu.VMEM((128, 128), F32),
            pltpu.VMEM((NDEV, 8, 128), F32),
            pltpu.VMEM((256, 128), F32),
            pltpu.VMEM((128, 128), jnp.int32),
            pltpu.VMEM((1, 128), jnp.int32),
            pltpu.VMEM((3000, 128), F32),
            pltpu.VMEM((4, 2, 256), F32),
            pltpu.VMEM((384, 384), BF16),
            pltpu.VMEM((128, 1152), BF16),
            pltpu.VMEM((128, 128), BF16),
            pltpu.SemaphoreType.DMA((8,)),
            pltpu.SemaphoreType.DMA((4,)),
            pltpu.SemaphoreType.DMA(()),
            pltpu.SemaphoreType.DMA(()),
        ],
        compiler_params=pltpu.CompilerParams(
            collective_id=0, has_side_effects=True, vmem_limit_bytes=32 * 2**20
        ),
    )(
        *[
            pltpu.with_memory_space_constraint(a, pltpu.HBM)
            for a in (
                resid, coords, angles, ids, counts, wave, moduli,
                jnp.asarray(grad), jnp.asarray(back), jnp.asarray(upper, BF16),
            )
        ]
    )


def node_coefficients():
    points = gll_points()
    poly = np.zeros((5, 5))
    for node in range(5):
        c = np.array([1.0])
        for other in range(5):
            if other != node:
                c = np.convolve(c, np.array([-points[other], 1.0])) / (points[node] - points[other])
        poly[node] = c
    slope = poly[:, 1:] * np.arange(1, 5)[None, :]
    every = np.concatenate([poly, slope], axis=1)
    blocks = []
    for m in range(9):
        blocks.append(np.concatenate([every[:, m], np.zeros(3)]))
    for m in range(9):
        blocks.append(every[np.arange(8) % 5, m])
    return np.repeat(np.concatenate(blocks)[:, None], 128, axis=1)


def fill_lanes(win, at, coef, lhs, h):
    tile_in = win[at]

    def spread(x, k):
        return jnp.broadcast_to(x[k : k + 1, :], (8, 128))

    def across(f):
        return spread(tile_in, f)

    def basis(x, block):
        c = [coef[8 * (block + m) : 8 * (block + m) + 8, :] for m in range(9)]
        val = (((c[4] * x + c[3]) * x + c[2]) * x + c[1]) * x + c[0]
        der = ((c[8] * x + c[7]) * x + c[6]) * x + c[5]
        return val, der

    vx, dx = basis(across(1), 0)
    vy, dy = basis(across(2), 9)
    vz, dz = basis(across(3), 0)
    t = [across(i) for i in (4, 5, 7)]
    d = [across(0) * t[i] for i in range(3)]
    sub = lax.broadcasted_iota(jnp.int32, (8, 128), 0)

    def by_p(rows, tile):
        row = functools.partial(spread, rows)
        if tile == 0:
            return jnp.where(sub < 5, row(0), row(1))
        if tile == 1:
            return jnp.where(sub < 2, row(1), jnp.where(sub < 7, row(2), row(3)))
        return jnp.where(sub < 4, row(3), row(4))

    def by_q(rows):
        turn = lambda n: pltpu.roll(rows, n, axis=0)
        return [
            rows,
            jnp.where(sub < 5, turn(5), turn(2)),
            jnp.where(sub < 7, turn(7), turn(4)),
        ]

    y1, y2, y3 = vy * t[0], dy * t[1], vy * t[2]
    q1, q2, q3 = by_q(y1), by_q(y2), by_q(y3)
    a, b = [], []
    for tile in range(3):
        px, pd = by_p(vx, tile), by_p(dx, tile)
        a.append(pd * q1[tile] + px * q2[tile])
        b.append(px * q3[tile])

    def last(rows):
        return rows[4:5, :]

    def shape(j):
        if j < 15:
            return a[j % 3] * spread(vz, j // 3) + b[j % 3] * spread(dz, j // 3)
        a4 = last(dx) * last(y1) + last(vx) * last(y2)
        b4 = last(vx) * last(y3)
        return a4 * vz + b4 * dz

    shapes = jnp.concatenate([shape(j) for j in range(16)], axis=0).reshape(16, 8, 128)
    for i in range(3):
        hi, lo = split((shapes * d[i][None]).reshape(128, 128))
        lhs[h, 128 * i : 128 * i + 128, :] = hi
        lhs[2 + h, 128 * i : 128 * i + 128, :] = lo


def inject_kernel(
    big, table, coef, out, xlo, xhi, ylo, yhi, corner,
    win, tabs, lhs_a, lhs_b, tsem,
):
    totab = pltpu.make_async_copy(table, tabs, tsem)
    totab.start()
    totab.wait()

    lane = lax.broadcasted_iota(jnp.int32, (8, 128), 1)
    zero = jnp.zeros((8, 128), F32)

    def place(step, carry):
        for k in range(8):
            t = step * 8 + k
            tile = big[t]
            col = jnp.floor((jnp.broadcast_to(tile[6:7, :], (8, 128)) - 1.0) * (1.0 / 256.0))
            for w in range(4):
                chunk = tabs[8 + w, t]
                run = pltpu.roll(jnp.where(col == float(w), tile, zero), tabs[w, t], axis=1)
                after = lane >= tabs[4 + w, t]
                pltpu.store(win.at[chunk], run, mask=after)
                win[chunk + 1] = jnp.where(after, zero, run)
        return carry

    lax.fori_loop(0, 16, place, 0)
    row = lax.broadcasted_iota(jnp.int32, (256, 128), 0).astype(F32).astype(BF16)
    upto = [0]
    for w in range(4):
        count = tabs[12 + w, 127]
        for k in range(3):
            win[CHUNKS * w + (count + 127) // 128 + k] = zero
        upto.append(upto[-1] + (count + 511) // 512)
    for k in range(4):
        win[4 * CHUNKS + k] = zero

    def chunk_of(u):
        at = u * 4
        for k in range(1, 4):
            at = jnp.where(u >= upto[k], CHUNKS * k + (u - upto[k]) * 4, at)
        return jnp.where(u >= upto[4], 4 * CHUNKS, at)

    def fill(at, lhs):
        for h in range(2):
            fill_lanes(win, at + h, coef, lhs, h)

    def push(at, reg):
        hot = []
        for h in range(2):
            want = jnp.broadcast_to(win[at + h, 6:7, :], (16, 128)) - 1.0
            want = (want - 256.0 * jnp.floor(want * (1.0 / 256.0))).astype(BF16)
            want = jnp.concatenate([want] * 16, axis=0)
            hot.append(jnp.where(row == want, jnp.ones((), BF16), jnp.zeros((), BF16)))
        rhs = jnp.concatenate(hot, axis=1)
        for q in range(2):
            pltpu.matmul_push_rhs(rhs, staging_register=reg, mxu_index=q, transpose=True)

    def use(lhs, reg, accs):
        for q in range(2):
            left = jnp.concatenate([lhs[2 * q], lhs[2 * q + 1]], axis=1)
            pltpu.matmul_acc_lhs(accs[q], left, load_staged_rhs=reg)

    def settle(w, accs):
        total = pltpu.matmul_pop(accs[0]) + pltpu.matmul_pop(accs[1])
        cx, cy = w // 2, w % 2
        halves = [
            big[NST + 192 * h + 48 * w : NST + 192 * h + 48 * w + 48].reshape(384, 128)
            for h in range(2)
        ]
        total = total + jnp.concatenate(halves, axis=1)
        for i in range(3):
            base = 128 * i
            g = [total[base + 24 * r : base + 24 * r + 24, :] for r in range(5)]
            tail = total[base + 120 : base + 128, :]
            groups = [g[0], tail[0:1, :]], [g[4], tail[4:5, :]]
            lows, highs = [], []
            for a, b in zip(*groups):
                ln = lax.broadcasted_iota(jnp.int32, a.shape, 1)
                lows.append(a + jnp.where(ln == 0, 0.0, pltpu.roll(b, 1, axis=1)))
                highs.append(b + jnp.where(ln == 255, 0.0, pltpu.roll(a, 255, axis=1)))
            main = [lows[0], g[1], g[2], g[3], highs[0]]
            last = [lows[1], tail[1:2, :], tail[2:3, :], tail[3:4, :], highs[1]]
            origin = (cx * 3 + i) * 500 + cy
            for r in range(5):
                for h in range(2):
                    cols = slice(128 * h, 128 * h + 128)
                    at = origin + 4 * r + 2 * h
                    out[pl.ds(at, 24, stride=20), :] = main[r][:, cols]
                    out[pl.ds(at + 480, 1), :] = last[r][:, cols]

    def multiply(*all_accs):
        sets = [(all_accs[0], all_accs[2]), (all_accs[1], all_accs[3])]
        for acc in all_accs:
            pltpu.matmul_pop(acc)
        fill(chunk_of(0), lhs_a)
        push(chunk_of(0), 0)
        for w in range(4):
            accs = sets[w % 2]

            def two_blocks(step, carry, w=w, accs=accs):
                u = upto[w] + step
                push(CHUNKS * w + 4 * step + 2, 1)
                fill(CHUNKS * w + 4 * step + 2, lhs_b)
                use(lhs_a, 0, accs)
                use(lhs_b, 1, accs)
                fill(chunk_of(u + 1), lhs_a)
                push(chunk_of(u + 1), 0)
                return carry

            lax.fori_loop(0, upto[w + 1] - upto[w], two_blocks, 0)
            if w == 3:
                use(lhs_a, 0, accs)
            if w > 0:
                settle(w - 1, sets[(w - 1) % 2])
        settle(3, sets[1])

    pl.run_scoped(multiply, *[pltpu.ACC(q)((384, 256), F32) for q in (0, 0, 1, 1)])

    for i in range(3):
        a = out[i * 500 + 400 : i * 500 + 500, :]
        b = out[(3 + i) * 500 : (3 + i) * 500 + 100, :]
        out[i * 500 + 400 : i * 500 + 500, :] = a + b
        out[(3 + i) * 500 : (3 + i) * 500 + 100, :] = a + b
    for c in range(6):
        for p in range(5):
            high = pl.ds(c * 500 + 100 * p + 80, 10, stride=2)
            low = pl.ds(c * 500 + 100 * p + 1, 10, stride=2)
            both = out[high, :] + out[low, :]
            out[high, :] = both
            out[low, :] = both
    for i in range(3):
        xlo[100 * i : 100 * i + 100, :] = out[i * 500 : i * 500 + 100, :]
        xhi[100 * i : 100 * i + 100, :] = out[(3 + i) * 500 + 400 : (3 + i) * 500 + 500, :]
    for i in range(3):
        for c in range(9):
            cx, p = (0, c) if c < 4 else (1, c - 4)
            origin = (cx * 3 + i) * 500 + 100 * p
            at = 9 * (9 * i + c)
            for face, shift in ((ylo, 0), (yhi, 81)):
                face[at : at + 8, :] = out[pl.ds(origin + shift, 8, stride=2), :]
                face[at + 8 : at + 9, :] = out[origin + shift + 18 : origin + shift + 19, :]
    for cx in range(2):
        for cy in range(2):
            for i in range(3):
                start = (cx * 3 + i) * 500 + 400 * cx + 80 * cy + cy
                corner[2 * cx + cy, 10 * i : 10 * i + 10, :] = out[pl.ds(start, 10, stride=2), :]


def inject(big, table):
    vm = pl.BlockSpec(memory_space=pltpu.VMEM)
    face = jax.ShapeDtypeStruct((304, 128), F32)
    side = jax.ShapeDtypeStruct((248, 128), F32)
    return pl.pallas_call(
        inject_kernel,
        name="inject",
        out_shape=(
            jax.ShapeDtypeStruct((3000, 128), F32),
            face, face, side, side,
            jax.ShapeDtypeStruct((4, 32, 128), F32),
        ),
        in_specs=[vm] * 3,
        out_specs=(vm,) * 6,
        scratch_shapes=[
            pltpu.VMEM((4 * CHUNKS + 4, 8, 128), F32),
            pltpu.SMEM((16, 128), jnp.int32),
            pltpu.VMEM((4, 384, 128), BF16),
            pltpu.VMEM((4, 384, 128), BF16),
            pltpu.SemaphoreType.DMA(()),
        ],
        compiler_params=pltpu.CompilerParams(vmem_limit_bytes=32 * 2**20),
    )(big, table, jnp.asarray(node_coefficients(), F32))


SIDES = [(-1, 0), (1, 0), (0, -1), (0, 1), (-1, -1), (-1, 1), (1, -1), (1, 1)]


def there(side, gx, gy):
    ok = None
    for d, g, n in ((side[0], gx, NGX), (side[1], gy, NGY)):
        if d:
            c = (g + d >= 0) & (g + d < n)
            ok = c if ok is None else ok & c
    return ok


def halo_kernel(local, xlo, xhi, ylo, yhi, corner, out, gxlo, gxhi, gylo, gyhi, gcorner, ssem, rsem):
    gx = lax.axis_index("gx")
    gy = lax.axis_index("gy")
    bar = pltpu.get_barrier_semaphore()
    for side in SIDES:
        @pl.when(there(side, gx, gy))
        def _(side=side):
            pl.semaphore_signal(
                bar, inc=1, device_id=(gx + side[0], gy + side[1]), device_id_type=MESH
            )
    nx = (gx > 0).astype(jnp.int32) + (gx < NGX - 1).astype(jnp.int32)
    ny = (gy > 0).astype(jnp.int32) + (gy < NGY - 1).astype(jnp.int32)
    pl.semaphore_wait(bar, (nx + 1) * (ny + 1) - 1)

    src = [xlo, xhi, ylo, yhi] + [corner.at[k] for k in range(4)]
    dst = [gxhi, gxlo, gyhi, gylo] + [gcorner.at[3 - k] for k in range(4)]

    def copy(k):
        side = SIDES[k]
        return pltpu.make_async_remote_copy(
            src_ref=src[k],
            dst_ref=dst[k],
            send_sem=ssem.at[k],
            recv_sem=rsem.at[k],
            device_id=(gx + side[0], gy + side[1]),
            device_id_type=MESH,
        )

    for k in (2, 3, 4, 5, 6, 7, 0, 1):
        @pl.when(there(SIDES[k], gx, gy))
        def _(k=k):
            copy(k).start()
    out[...] = local[...]

    def take(k, add):
        @pl.when(there(SIDES[k], gx, gy))
        def _():
            copy([1, 0, 3, 2, 7, 6, 5, 4][k]).wait_recv()
            add()

    def add_xlo():
        for i in range(3):
            out[i * 500 : i * 500 + 100, :] += gxlo[100 * i : 100 * i + 100, :]

    def add_xhi():
        for i in range(3):
            out[(3 + i) * 500 + 400 : (3 + i) * 500 + 500, :] += gxhi[100 * i : 100 * i + 100, :]

    def add_y(ref, shift):
        for i in range(3):
            for c in range(9):
                k = 9 * (9 * i + c)
                first = ref[k : k + 8, :]
                pair = jnp.concatenate([first[0:1, :], first[1:2, :]], axis=1)
                turned = pltpu.roll(pair, 255, axis=1)[:, 0:128]
                for cx, p in ((0, c), (1, c - 4)):
                    if 0 <= p < 5:
                        at = (cx * 3 + i) * 500 + 100 * p + shift
                        out[pl.ds(at, 8, stride=2), :] += first
                        out[at + 16 : at + 17, :] += turned
                        out[at + 18 : at + 19, :] += ref[k + 8 : k + 9, :]

    def add_corner(k):
        cx, cy = k // 2, k % 2
        for i in range(3):
            rows = pl.ds((cx * 3 + i) * 500 + 400 * cx + 80 * cy + cy, 10, stride=2)
            out[rows, :] += gcorner[k, 10 * i : 10 * i + 10, :]

    take(0, add_xlo)
    take(1, add_xhi)
    for k in range(4):
        take(4 + k, functools.partial(add_corner, k))
    take(2, lambda: add_y(gylo, 0))
    take(3, lambda: add_y(gyhi, 81))
    for k in range(8):
        @pl.when(there(SIDES[k], gx, gy))
        def _(k=k):
            copy(k).wait_send()


def halo(local, xlo, xhi, ylo, yhi, corner):
    vm = pl.BlockSpec(memory_space=pltpu.VMEM)
    return pl.pallas_call(
        halo_kernel,
        name="halo",
        out_shape=jax.ShapeDtypeStruct((3000, 128), F32),
        in_specs=[vm] * 6,
        out_specs=vm,
        scratch_shapes=[pltpu.VMEM((n, 128), F32) for n in (304, 304, 248, 248)]
        + [
            pltpu.VMEM((4, 32, 128), F32),
            pltpu.SemaphoreType.DMA((8,)),
            pltpu.SemaphoreType.DMA((8,)),
        ],
        compiler_params=pltpu.CompilerParams(
            collective_id=1, has_side_effects=True, vmem_limit_bytes=16 * 2**20
        ),
    )(local, xlo, xhi, ylo, yhi, corner)


def body(wavefield, moduli, residuals, coords, angles, element_ids, counts):
    wave = wavefield.reshape(2, 2, 3, 125, 2, 128).transpose(0, 2, 3, 4, 1, 5).reshape(3000, 128)
    sorted_slots = exchange(
        residuals[0],
        coords[0].transpose(1, 0, 2),
        angles.reshape(256, 128),
        element_ids[0],
        counts,
        wave,
        moduli.reshape(4, 2, 256),
    )
    out = halo(*inject(*sorted_slots))
    out = out.reshape(2, 3, 125, 2, 2, 128).transpose(0, 4, 1, 2, 3, 5)
    return out.reshape(2, 2, 3, 125, 256)


def solution(mesh):
    in_specs = (
        P("gx", "gy", None, None, None),
        P("gx", "gy", None, None),
        P(("gx", "gy"), None, None),
        P(("gx", "gy"), None, None, None),
        P(("gx", "gy"), None, None, None),
        P(("gx", "gy"), None, None),
        P(("gx", "gy"), None),
    )
    out_specs = P("gx", "gy", None, None, None)
    return jax.shard_map(body, mesh=mesh, in_specs=in_specs, out_specs=out_specs, check_vma=False)
```

```python
import functools
import math

import jax
import jax.numpy as jnp
import numpy as np
from jax import lax
from jax.experimental import pallas as pl
from jax.experimental.pallas import tpu as pltpu
from jax.sharding import PartitionSpec as P

MESH = pl.DeviceIdType.MESH
F32 = jnp.float32
BF16 = jnp.bfloat16
NGX = 8
NGY = 16
NDEV = 128
CHUNKS = 136
NST = 128
FIELD = 136
NT = (((1,), (1,)), ((), ()))
NN = (((1,), (0,)), ((), ()))


def gll_points():
    return np.array([-1.0, -math.sqrt(3.0 / 7.0), 0.0, math.sqrt(3.0 / 7.0), 1.0])


def gll_weights():
    return np.array([0.1, 49.0 / 90.0, 32.0 / 45.0, 49.0 / 90.0, 0.1])


def derivative_table():
    points = gll_points()
    table = np.zeros((5, 5))
    for row in range(5):
        for col in range(5):
            if row == col:
                table[row, col] = sum(
                    (1.0 / (points[col] - points[other]) for other in range(5) if other != col)
                )
            else:
                value = 1.0 / (points[col] - points[row])
                for other in range(5):
                    if other != col and other != row:
                        value = (
                            value * (points[row] - points[other]) / (points[col] - points[other])
                        )
                table[row, col] = value
    return table


def split_np(a):
    hi = np.asarray(a, np.float32).astype(jnp.bfloat16)
    lo = (np.asarray(a, np.float64) - hi.astype(np.float64)).astype(jnp.bfloat16)
    return hi, lo


def row_of(p, q, r):
    pq = 5 * p + q
    return 120 + r if pq == 24 else 24 * r + pq


def operators():
    table = np.asarray(derivative_table(), np.float32).astype(np.float64)
    weight = np.asarray(gll_weights(), np.float32).astype(np.float64)
    grad = np.zeros((3, 128, 128))
    back = np.zeros((3, 128, 128))
    for p in range(5):
        for q in range(5):
            for r in range(5):
                n = 25 * p + 5 * q + r
                for k in range(5):
                    grad[0, n, 25 * k + 5 * q + r] = table[p, k]
                    grad[1, n, 25 * p + 5 * k + r] = table[q, k]
                    grad[2, n, 25 * p + 5 * q + k] = table[r, k]
                w = weight[p] * weight[q] * weight[r]
                for k in range(5):
                    back[0, row_of(k, q, r), n] = -w * table[p, k]
                    back[1, row_of(p, k, r), n] = -w * table[q, k]
                    back[2, row_of(p, q, k), n] = -w * table[r, k]
    ghi, glo = split_np(grad.reshape(384, 128))
    flat = np.concatenate([back[0], back[1], back[2]], axis=1)
    bhi, blo = split_np(flat)
    return np.concatenate([ghi, glo, ghi], axis=1), np.concatenate([bhi, blo, bhi], axis=1)


def split(x):
    hi = x.astype(BF16)
    return hi, (x - hi.astype(F32)).astype(BF16)


def sin_cos(x):
    y = 0.5 * x
    z = y * y
    s = y * (
        1.0
        + z * (-1.0 / 6 + z * (1.0 / 120 + z * (-1.0 / 5040 + z * (1.0 / 362880 + z * (-1.0 / 39916800)))))
    )
    c = 1.0 + z * (
        -0.5
        + z
        * (1.0 / 24 + z * (-1.0 / 720 + z * (1.0 / 40320 + z * (-1.0 / 3628800 + z * (1.0 / 479001600)))))
    )
    return 2.0 * s * c, 1.0 - 2.0 * s * s


def far_first(j):
    return 2 + ((j + 1) // 2) * (1 - 2 * (j % 2))


def exchange_kernel(
    resid, coords, angles, ids, counts, wave, moduli, grad, back, upper,
    stage, table,
    fl, pos_s, outgo, abuf, ibuf, cbuf, wbuf, mbuf, gbuf, bbuf, ubuf,
    isem, wsem, ssem, rsem,
):
    gx = lax.axis_index("gx")
    gy = lax.axis_index("gy")
    me = gx * NGY + gy
    y, core, z, x = gx // 2, gx % 2, gy // 4, gy % 4
    loads = [
        pltpu.make_async_copy(a, b, isem.at[k])
        for k, (a, b) in enumerate(
            [(counts, cbuf), (ids, ibuf), (angles, abuf), (upper, ubuf)]
            + [(resid, fl.at[pl.ds(0, 128)])]
            + [(coords.at[d], fl.at[pl.ds(FIELD * (1 + d), 128)]) for d in range(3)]
        )
    ]
    fetches = [
        pltpu.make_async_copy(a, b, wsem.at[k])
        for k, (a, b) in enumerate(
            ((wave, wbuf), (moduli, mbuf), (grad, gbuf), (back, bbuf))
        )
    ]
    for load in loads:
        load.start()
    bar = pltpu.get_barrier_semaphore()

    near_x = [(x + far_first(m)) % 4 for m in range(4)]
    near_c = [(core + 1 - m) % 2 for m in range(2)]
    offset = [near_c[m % 2] * NGY + near_x[m // 2] for m in range(8)]

    def peers(j, last):
        ty = 2 * ((y + far_first(j % 4)) % 4)
        tz = 4 * ((z + far_first(j // 4)) % 4)
        origin = ty * NGY + tz
        for m in range(7 if last else 8):
            yield m, origin + offset[m], ty + near_c[m % 2], tz + near_x[m // 2]

    def greet(j, last):
        for _, _, tgx, tgy in peers(j, last):
            pl.semaphore_signal(bar, inc=1, device_id=(tgx, tgy), device_id_type=MESH)

    def greet_eight(j, carry):
        greet(j, False)
        return carry

    lax.fori_loop(0, 15, greet_eight, 0)
    greet(15, True)
    for fetch in fetches:
        fetch.start()
    for load in loads:
        load.wait()

    for k in range(2):
        fl[FIELD * (4 + k) : FIELD * (4 + k) + 128, :] = abuf[pl.ds(k, 128, stride=2), :]
    limit = jnp.transpose(jnp.broadcast_to(cbuf[...].astype(F32), (128, 128)))
    slot = lax.broadcasted_iota(jnp.int32, (128, 128), 1).astype(F32)
    num = ibuf[...].astype(F32)
    fl[FIELD * 6 : FIELD * 6 + 128, :] = num + 1.0
    fl[FIELD * 7 : FIELD * 7 + 128, :] = jnp.zeros((128, 128), F32)
    up = ubuf[...]
    ones = jnp.ones((128, 128), BF16)

    def columns_of(col):
        masks = [(col == float(w)).astype(F32).astype(BF16) for w in range(4)]
        return jnp.concatenate(masks, axis=0)

    colf = jnp.where(slot < limit, jnp.floor(num * (1.0 / 256.0)), -1.0)
    stacked = columns_of(colf)
    prefix = lax.dot_general(stacked, up, NN, preferred_element_type=F32)
    total = lax.dot_general(stacked, ones, NN, preferred_element_type=F32)
    start = jnp.zeros((128, 128), F32)
    pos = jnp.full((128, 128), -1.0, F32)
    for w in range(4):
        rows = slice(128 * w, 128 * w + 128)
        pos = jnp.where(colf == float(w), prefix[rows] + start, pos)
        start = start + total[rows]
    pos_s[...] = pos
    lane_row = lax.broadcasted_iota(jnp.int32, (128, 128), 0).astype(F32)

    def sort_some(h, carry):
        for k in range(16):
            t = h * 16 + k
            f = fl[pl.ds(t, 8, stride=FIELD), :]
            hi = f.astype(BF16).astype(F32)
            mid = (f - hi).astype(BF16).astype(F32)
            lo = f - hi - mid
            perm = jnp.where(lane_row == pos_s[pl.ds(t, 1), :], 1.0, 0.0).astype(BF16)
            got = lax.dot_general(
                jnp.concatenate([hi, mid, lo], axis=0).astype(BF16),
                perm,
                NT,
                preferred_element_type=F32,
            )
            outgo[t] = got[0:8] + got[8:16] + got[16:24]
        return carry

    lax.fori_loop(0, 8, sort_some, 0)
    stage[NDEV - 1] = outgo[me]
    pl.semaphore_wait(bar, NDEV - 1)

    def send(j, last):
        for m, target, tgx, tgy in peers(j, last):
            pltpu.make_async_remote_copy(
                src_ref=outgo.at[target, pl.ds(0, 7), :],
                dst_ref=stage.at[j * 8 + m, pl.ds(0, 7), :],
                send_sem=ssem,
                recv_sem=rsem,
                device_id=(tgx, tgy),
                device_id_type=MESH,
            ).start()

    def send_eight(j, carry):
        send(j, False)
        return carry

    lax.fori_loop(0, 15, send_eight, 0)
    send(15, True)
    for fetch in fetches:
        fetch.wait()

    def column(w, carry):
        cx = w // 2
        cy = w % 2
        lam = mbuf[w, 0:1, :]
        mu = mbuf[w, 1:2, :]
        grads = []
        for i in range(3):
            start = (cx * 3 + i) * 500 + cy
            u = jnp.concatenate(
                [wbuf[pl.ds(start + 2 * h, 125, stride=4), :] for h in range(2)], axis=1
            )
            u = jnp.concatenate([u, jnp.zeros((3, 256), F32)], axis=0)
            hi, lo = split(u)
            grads.append(
                lax.dot_general(
                    gbuf[...],
                    jnp.concatenate([hi, hi, lo], axis=0),
                    NN,
                    preferred_element_type=F32,
                )
            )
        g = [[grads[i][128 * j : 128 * j + 128] for j in range(3)] for i in range(3)]
        ldiv = lam * (g[0][0] + g[1][1] + g[2][2])
        parts = {}
        for i in range(3):
            for j in range(i, 3):
                s = mu * (g[i][j] + g[j][i])
                if i == j:
                    s = s + ldiv
                parts[(i, j)] = parts[(j, i)] = split(s)
        for i in range(3):
            hi = [parts[(i, j)][0] for j in range(3)]
            lo = [parts[(i, j)][1] for j in range(3)]
            got = lax.dot_general(
                bbuf[...],
                jnp.concatenate(hi + hi + lo, axis=0),
                NN,
                preferred_element_type=F32,
            )
            for h in range(2):
                at = NST + 192 * h + 48 * w + 16 * i
                stage[pl.ds(at, 16)] = got[:, 128 * h : 128 * h + 128].reshape(16, 8, 128)
        return carry

    lax.fori_loop(0, 4, column, 0)
    drain = pltpu.make_async_remote_copy(
        src_ref=outgo.at[pl.ds(0, NDEV - 1), pl.ds(0, 7), :],
        dst_ref=stage.at[pl.ds(0, NDEV - 1), pl.ds(0, 7), :],
        send_sem=ssem,
        recv_sem=rsem,
        device_id=(gx, (gy + 1) % NGY),
        device_id_type=MESH,
    )
    drain.wait_recv()
    rows = stage.reshape(4096, 128)
    got = rows[pl.ds(6, NDEV, stride=8), :]
    sin_a, cos_a = sin_cos(rows[pl.ds(4, NDEV, stride=8), :])
    sin_d, cos_d = sin_cos(rows[pl.ds(5, NDEV, stride=8), :])
    for k, v in ((4, cos_a * cos_d), (5, sin_a * cos_d), (7, sin_d)):
        rows[pl.ds(k, NDEV, stride=8), :] = v
    received = columns_of(jnp.floor((got - 1.0) * (1.0 / 256.0)))
    sub = lax.broadcasted_iota(jnp.int32, (16, 128), 0)
    words = jnp.zeros((16, 128), jnp.int32)
    first = jnp.zeros((16, 128), jnp.int32)
    for w in range(4):
        n = lax.dot_general(
            jnp.ones((16, 128), BF16), received[128 * w : 128 * w + 128], NT, preferred_element_type=F32
        )
        fill = lax.dot_general(n.astype(BF16), up, NN, preferred_element_type=F32)
        n = n.astype(jnp.int32)
        fill = fill.astype(jnp.int32)
        words = jnp.where(sub == w, (fill - first) & 127, words)
        words = jnp.where(sub == 4 + w, fill & 127, words)
        words = jnp.where(sub == 8 + w, (fill >> 7) + CHUNKS * w, words)
        words = jnp.where(sub == 12 + w, fill + n, words)
        first = first + n
    table[...] = words
    drain.wait_send()


def exchange(resid, coords, angles, ids, counts, wave, moduli):
    grad, back = operators()
    upper = np.triu(np.ones((128, 128), np.float32), 1)
    return pl.pallas_call(
        exchange_kernel,
        name="exchange",
        out_shape=(
            pltpu.VMEM((512, 8, 128), F32),
            pltpu.VMEM((16, 128), jnp.int32),
        ),
        in_specs=[pl.BlockSpec(memory_space=pltpu.HBM)] * 10,
        out_specs=(pl.BlockSpec(memory_space=pltpu.VMEM),) * 2,
        scratch_shapes=[
            pltpu.VMEM((8 * FIELD, 128), F32),
            pltpu.VMEM((128, 128), F32),
            pltpu.VMEM((NDEV, 8, 128), F32),
            pltpu.VMEM((256, 128), F32),
            pltpu.VMEM((128, 128), jnp.int32),
            pltpu.VMEM((1, 128), jnp.int32),
            pltpu.VMEM((3000, 128), F32),
            pltpu.VMEM((4, 2, 256), F32),
            pltpu.VMEM((384, 384), BF16),
            pltpu.VMEM((128, 1152), BF16),
            pltpu.VMEM((128, 128), BF16),
            pltpu.SemaphoreType.DMA((8,)),
            pltpu.SemaphoreType.DMA((4,)),
            pltpu.SemaphoreType.DMA(()),
            pltpu.SemaphoreType.DMA(()),
        ],
        compiler_params=pltpu.CompilerParams(
            collective_id=0, has_side_effects=True, vmem_limit_bytes=32 * 2**20
        ),
    )(
        *[
            pltpu.with_memory_space_constraint(a, pltpu.HBM)
            for a in (
                resid, coords, angles, ids, counts, wave, moduli,
                jnp.asarray(grad), jnp.asarray(back), jnp.asarray(upper, BF16),
            )
        ]
    )


def node_coefficients():
    points = gll_points()
    poly = np.zeros((5, 5))
    for node in range(5):
        c = np.array([1.0])
        for other in range(5):
            if other != node:
                c = np.convolve(c, np.array([-points[other], 1.0])) / (points[node] - points[other])
        poly[node] = c
    slope = poly[:, 1:] * np.arange(1, 5)[None, :]
    every = np.concatenate([poly, slope], axis=1)
    blocks = []
    for m in range(9):
        blocks.append(np.concatenate([every[:, m], np.zeros(3)]))
    for m in range(9):
        blocks.append(every[np.arange(8) % 5, m])
    return np.repeat(np.concatenate(blocks)[:, None], 128, axis=1)


def fill_lanes(win, at, coef, lhs, h):
    tile_in = win[at]

    def spread(x, k):
        return jnp.broadcast_to(x[k : k + 1, :], (8, 128))

    def across(f):
        return spread(tile_in, f)

    def basis(x, block):
        c = [coef[8 * (block + m) : 8 * (block + m) + 8, :] for m in range(9)]
        val = (((c[4] * x + c[3]) * x + c[2]) * x + c[1]) * x + c[0]
        der = ((c[8] * x + c[7]) * x + c[6]) * x + c[5]
        return val, der

    vx, dx = basis(across(1), 0)
    vy, dy = basis(across(2), 9)
    vz, dz = basis(across(3), 0)
    t = [across(i) for i in (4, 5, 7)]
    d = [across(0) * t[i] for i in range(3)]
    sub = lax.broadcasted_iota(jnp.int32, (8, 128), 0)

    def by_p(rows, tile):
        row = functools.partial(spread, rows)
        if tile == 0:
            return jnp.where(sub < 5, row(0), row(1))
        if tile == 1:
            return jnp.where(sub < 2, row(1), jnp.where(sub < 7, row(2), row(3)))
        return jnp.where(sub < 4, row(3), row(4))

    def by_q(rows):
        turn = lambda n: pltpu.roll(rows, n, axis=0)
        return [
            rows,
            jnp.where(sub < 5, turn(5), turn(2)),
            jnp.where(sub < 7, turn(7), turn(4)),
        ]

    y1, y2, y3 = vy * t[0], dy * t[1], vy * t[2]
    q1, q2, q3 = by_q(y1), by_q(y2), by_q(y3)
    a, b = [], []
    for tile in range(3):
        px, pd = by_p(vx, tile), by_p(dx, tile)
        a.append(pd * q1[tile] + px * q2[tile])
        b.append(px * q3[tile])

    def last(rows):
        return rows[4:5, :]

    def shape(j):
        if j < 15:
            return a[j % 3] * spread(vz, j // 3) + b[j % 3] * spread(dz, j // 3)
        a4 = last(dx) * last(y1) + last(vx) * last(y2)
        b4 = last(vx) * last(y3)
        return a4 * vz + b4 * dz

    shapes = jnp.concatenate([shape(j) for j in range(16)], axis=0).reshape(16, 8, 128)
    for i in range(3):
        hi, lo = split((shapes * d[i][None]).reshape(128, 128))
        lhs[h, 128 * i : 128 * i + 128, :] = hi
        lhs[2 + h, 128 * i : 128 * i + 128, :] = lo


def inject_kernel(
    big, table, coef, out, xlo, xhi, ylo, yhi, corner,
    win, tabs, lhs_a, lhs_b, tsem,
):
    totab = pltpu.make_async_copy(table, tabs, tsem)
    totab.start()
    totab.wait()

    lane = lax.broadcasted_iota(jnp.int32, (8, 128), 1)
    zero = jnp.zeros((8, 128), F32)

    def place(step, carry):
        for k in range(8):
            t = step * 8 + k
            tile = big[t]
            col = jnp.floor((jnp.broadcast_to(tile[6:7, :], (8, 128)) - 1.0) * (1.0 / 256.0))
            for w in range(4):
                chunk = tabs[8 + w, t]
                run = pltpu.roll(jnp.where(col == float(w), tile, zero), tabs[w, t], axis=1)
                after = lane >= tabs[4 + w, t]
                pltpu.store(win.at[chunk], run, mask=after)
                win[chunk + 1] = jnp.where(after, zero, run)
        return carry

    lax.fori_loop(0, 16, place, 0)
    row = lax.broadcasted_iota(jnp.int32, (256, 128), 0).astype(F32).astype(BF16)
    upto = [0]
    for w in range(4):
        count = tabs[12 + w, 127]
        for k in range(3):
            win[CHUNKS * w + (count + 127) // 128 + k] = zero
        upto.append(upto[-1] + (count + 511) // 512)
    for k in range(4):
        win[4 * CHUNKS + k] = zero

    def chunk_of(u):
        at = u * 4
        for k in range(1, 4):
            at = jnp.where(u >= upto[k], CHUNKS * k + (u - upto[k]) * 4, at)
        return jnp.where(u >= upto[4], 4 * CHUNKS, at)

    def fill(at, lhs):
        for h in range(2):
            fill_lanes(win, at + h, coef, lhs, h)

    def push(at, reg):
        hot = []
        for h in range(2):
            want = jnp.broadcast_to(win[at + h, 6:7, :], (16, 128)) - 1.0
            want = (want - 256.0 * jnp.floor(want * (1.0 / 256.0))).astype(BF16)
            want = jnp.concatenate([want] * 16, axis=0)
            hot.append(jnp.where(row == want, jnp.ones((), BF16), jnp.zeros((), BF16)))
        rhs = jnp.concatenate(hot, axis=1)
        for q in range(2):
            pltpu.matmul_push_rhs(rhs, staging_register=reg, mxu_index=q, transpose=True)

    def use(lhs, reg, accs):
        for q in range(2):
            left = jnp.concatenate([lhs[2 * q], lhs[2 * q + 1]], axis=1)
            pltpu.matmul_acc_lhs(accs[q], left, load_staged_rhs=reg)

    def settle(w, accs):
        total = pltpu.matmul_pop(accs[0]) + pltpu.matmul_pop(accs[1])
        cx, cy = w // 2, w % 2
        halves = [
            big[NST + 192 * h + 48 * w : NST + 192 * h + 48 * w + 48].reshape(384, 128)
            for h in range(2)
        ]
        total = total + jnp.concatenate(halves, axis=1)
        for i in range(3):
            base = 128 * i
            g = [total[base + 24 * r : base + 24 * r + 24, :] for r in range(5)]
            tail = total[base + 120 : base + 128, :]
            groups = [g[0], tail[0:1, :]], [g[4], tail[4:5, :]]
            lows, highs = [], []
            for a, b in zip(*groups):
                ln = lax.broadcasted_iota(jnp.int32, a.shape, 1)
                lows.append(a + jnp.where(ln == 0, 0.0, pltpu.roll(b, 1, axis=1)))
                highs.append(b + jnp.where(ln == 255, 0.0, pltpu.roll(a, 255, axis=1)))
            main = [lows[0], g[1], g[2], g[3], highs[0]]
            last = [lows[1], tail[1:2, :], tail[2:3, :], tail[3:4, :], highs[1]]
            origin = (cx * 3 + i) * 500 + cy
            for r in range(5):
                for h in range(2):
                    cols = slice(128 * h, 128 * h + 128)
                    at = origin + 4 * r + 2 * h
                    out[pl.ds(at, 24, stride=20), :] = main[r][:, cols]
                    out[pl.ds(at + 480, 1), :] = last[r][:, cols]

    def multiply(*all_accs):
        sets = [(all_accs[0], all_accs[2]), (all_accs[1], all_accs[3])]
        for acc in all_accs:
            pltpu.matmul_pop(acc)
        fill(chunk_of(0), lhs_a)
        push(chunk_of(0), 0)
        for w in range(4):
            accs = sets[w % 2]

            def two_blocks(step, carry, w=w, accs=accs):
                u = upto[w] + step
                push(CHUNKS * w + 4 * step + 2, 1)
                fill(CHUNKS * w + 4 * step + 2, lhs_b)
                use(lhs_a, 0, accs)
                use(lhs_b, 1, accs)
                fill(chunk_of(u + 1), lhs_a)
                push(chunk_of(u + 1), 0)
                return carry

            lax.fori_loop(0, upto[w + 1] - upto[w], two_blocks, 0)
            if w == 3:
                use(lhs_a, 0, accs)
            if w > 0:
                settle(w - 1, sets[(w - 1) % 2])
        settle(3, sets[1])

    pl.run_scoped(multiply, *[pltpu.ACC(q)((384, 256), F32) for q in (0, 0, 1, 1)])

    for i in range(3):
        a = out[i * 500 + 400 : i * 500 + 500, :]
        b = out[(3 + i) * 500 : (3 + i) * 500 + 100, :]
        out[i * 500 + 400 : i * 500 + 500, :] = a + b
        out[(3 + i) * 500 : (3 + i) * 500 + 100, :] = a + b
    for c in range(6):
        for p in range(5):
            high = pl.ds(c * 500 + 100 * p + 80, 10, stride=2)
            low = pl.ds(c * 500 + 100 * p + 1, 10, stride=2)
            both = out[high, :] + out[low, :]
            out[high, :] = both
            out[low, :] = both
    for i in range(3):
        xlo[100 * i : 100 * i + 100, :] = out[i * 500 : i * 500 + 100, :]
        xhi[100 * i : 100 * i + 100, :] = out[(3 + i) * 500 + 400 : (3 + i) * 500 + 500, :]
    for i in range(3):
        for c in range(9):
            cx, p = (0, c) if c < 4 else (1, c - 4)
            origin = (cx * 3 + i) * 500 + 100 * p
            at = 9 * (9 * i + c)
            for face, shift in ((ylo, 0), (yhi, 81)):
                face[at : at + 8, :] = out[pl.ds(origin + shift, 8, stride=2), :]
                face[at + 8 : at + 9, :] = out[origin + shift + 18 : origin + shift + 19, :]
    for cx in range(2):
        for cy in range(2):
            for i in range(3):
                start = (cx * 3 + i) * 500 + 400 * cx + 80 * cy + cy
                corner[2 * cx + cy, 10 * i : 10 * i + 10, :] = out[pl.ds(start, 10, stride=2), :]


def inject(big, table):
    vm = pl.BlockSpec(memory_space=pltpu.VMEM)
    face = jax.ShapeDtypeStruct((304, 128), F32)
    side = jax.ShapeDtypeStruct((248, 128), F32)
    return pl.pallas_call(
        inject_kernel,
        name="inject",
        out_shape=(
            jax.ShapeDtypeStruct((3000, 128), F32),
            face, face, side, side,
            jax.ShapeDtypeStruct((4, 32, 128), F32),
        ),
        in_specs=[vm] * 3,
        out_specs=(vm,) * 6,
        scratch_shapes=[
            pltpu.VMEM((4 * CHUNKS + 4, 8, 128), F32),
            pltpu.SMEM((16, 128), jnp.int32),
            pltpu.VMEM((4, 384, 128), BF16),
            pltpu.VMEM((4, 384, 128), BF16),
            pltpu.SemaphoreType.DMA(()),
        ],
        compiler_params=pltpu.CompilerParams(vmem_limit_bytes=32 * 2**20),
    )(big, table, jnp.asarray(node_coefficients(), F32))


SIDES = [(-1, 0), (1, 0), (0, -1), (0, 1), (-1, -1), (-1, 1), (1, -1), (1, 1)]


def there(side, gx, gy):
    ok = None
    for d, g, n in ((side[0], gx, NGX), (side[1], gy, NGY)):
        if d:
            c = (g + d >= 0) & (g + d < n)
            ok = c if ok is None else ok & c
    return ok


def halo_kernel(local, xlo, xhi, ylo, yhi, corner, out, gxlo, gxhi, gylo, gyhi, gcorner, ssem, rsem):
    gx = lax.axis_index("gx")
    gy = lax.axis_index("gy")
    bar = pltpu.get_barrier_semaphore()
    for side in SIDES:
        @pl.when(there(side, gx, gy))
        def _(side=side):
            pl.semaphore_signal(
                bar, inc=1, device_id=(gx + side[0], gy + side[1]), device_id_type=MESH
            )
    nx = (gx > 0).astype(jnp.int32) + (gx < NGX - 1).astype(jnp.int32)
    ny = (gy > 0).astype(jnp.int32) + (gy < NGY - 1).astype(jnp.int32)
    pl.semaphore_wait(bar, (nx + 1) * (ny + 1) - 1)

    src = [xlo, xhi, ylo, yhi] + [corner.at[k] for k in range(4)]
    dst = [gxhi, gxlo, gyhi, gylo] + [gcorner.at[3 - k] for k in range(4)]

    def copy(k):
        side = SIDES[k]
        return pltpu.make_async_remote_copy(
            src_ref=src[k],
            dst_ref=dst[k],
            send_sem=ssem.at[k],
            recv_sem=rsem.at[k],
            device_id=(gx + side[0], gy + side[1]),
            device_id_type=MESH,
        )

    for k in (2, 3, 4, 5, 6, 7, 0, 1):
        @pl.when(there(SIDES[k], gx, gy))
        def _(k=k):
            copy(k).start()
    out[...] = local[...]

    def take(k, add):
        @pl.when(there(SIDES[k], gx, gy))
        def _():
            copy([1, 0, 3, 2, 7, 6, 5, 4][k]).wait_recv()
            add()

    def add_xlo():
        for i in range(3):
            out[i * 500 : i * 500 + 100, :] += gxlo[100 * i : 100 * i + 100, :]

    def add_xhi():
        for i in range(3):
            out[(3 + i) * 500 + 400 : (3 + i) * 500 + 500, :] += gxhi[100 * i : 100 * i + 100, :]

    def add_y(ref, shift):
        for i in range(3):
            for c in range(9):
                k = 9 * (9 * i + c)
                first = ref[k : k + 8, :]
                pair = jnp.concatenate([first[0:1, :], first[1:2, :]], axis=1)
                turned = pltpu.roll(pair, 255, axis=1)[:, 0:128]
                for cx, p in ((0, c), (1, c - 4)):
                    if 0 <= p < 5:
                        at = (cx * 3 + i) * 500 + 100 * p + shift
                        out[pl.ds(at, 8, stride=2), :] += first
                        out[at + 16 : at + 17, :] += turned
                        out[at + 18 : at + 19, :] += ref[k + 8 : k + 9, :]

    def add_corner(k):
        cx, cy = k // 2, k % 2
        for i in range(3):
            rows = pl.ds((cx * 3 + i) * 500 + 400 * cx + 80 * cy + cy, 10, stride=2)
            out[rows, :] += gcorner[k, 10 * i : 10 * i + 10, :]

    take(0, add_xlo)
    take(1, add_xhi)
    for k in range(4):
        take(4 + k, functools.partial(add_corner, k))
    take(2, lambda: add_y(gylo, 0))
    take(3, lambda: add_y(gyhi, 81))
    for k in range(8):
        @pl.when(there(SIDES[k], gx, gy))
        def _(k=k):
            copy(k).wait_send()


def halo(local, xlo, xhi, ylo, yhi, corner):
    vm = pl.BlockSpec(memory_space=pltpu.VMEM)
    return pl.pallas_call(
        halo_kernel,
        name="halo",
        out_shape=jax.ShapeDtypeStruct((3000, 128), F32),
        in_specs=[vm] * 6,
        out_specs=vm,
        scratch_shapes=[pltpu.VMEM((n, 128), F32) for n in (304, 304, 248, 248)]
        + [
            pltpu.VMEM((4, 32, 128), F32),
            pltpu.SemaphoreType.DMA((8,)),
            pltpu.SemaphoreType.DMA((8,)),
        ],
        compiler_params=pltpu.CompilerParams(
            collective_id=1, has_side_effects=True, vmem_limit_bytes=16 * 2**20
        ),
    )(local, xlo, xhi, ylo, yhi, corner)


def body(wavefield, moduli, residuals, coords, angles, element_ids, counts):
    wave = wavefield.reshape(2, 2, 3, 125, 2, 128).transpose(0, 2, 3, 4, 1, 5).reshape(3000, 128)
    sorted_slots = exchange(
        residuals[0],
        coords[0].transpose(1, 0, 2),
        angles.reshape(256, 128),
        element_ids[0],
        counts,
        wave,
        moduli.reshape(4, 2, 256),
    )
    out = halo(*inject(*sorted_slots))
    out = out.reshape(2, 3, 125, 2, 2, 128).transpose(0, 4, 1, 2, 3, 5)
    return out.reshape(2, 2, 3, 125, 256)


def solution(mesh):
    in_specs = (
        P("gx", "gy", None, None, None),
        P("gx", "gy", None, None),
        P(("gx", "gy"), None, None),
        P(("gx", "gy"), None, None, None),
        P(("gx", "gy"), None, None, None),
        P(("gx", "gy"), None, None),
        P(("gx", "gy"), None),
    )
    out_specs = P("gx", "gy", None, None, None)
    return jax.shard_map(body, mesh=mesh, in_specs=in_specs, out_specs=out_specs, check_vma=False)
```
